32 devices in a mesh: gx: 4 (over z), gy: 8 (over y, x, core).
Axes of the slice: x: 2, y: 2, z: 4, core: 2. Of those that a mesh axis runs over, the one named last changes fastest.
Arguments:
- splats: float32 [1024, 55, 128], P(('gx', 'gy')), as said below
- moment_one: float32 [1024, 55, 128], P(('gx', 'gy')), may hold values from -0.3 to 0.3
- moment_two: float32 [1024, 55, 128], P(('gx', 'gy')), may hold values from 0.001 to 1
- target: float32 [512, 3, 256], P(('gx', 'gy')), may hold values from 0 to 1
- tile_place: int32 [512], P(('gx', 'gy')), may hold values from 0 to 511, as said below
- pairs: int32 [512, 8], P(('gx', 'gy')), may hold values from -1 to 63, as said below
- fetch: int32 [32, 32, 2], P(('gx', 'gy')), may hold values from -1 to 31, as said below
Outputs:
- image: float32 [512, 3, 256], P(('gx', 'gy'))
- splat_grad: float32 [1024, 55, 128], P(('gx', 'gy'))
- adam_step: float32 [1024, 55, 128], P(('gx', 'gy'))
The draws below stay inside these ranges and needn't reach their ends.
Inputs may be any that keep to these rules, and one draw needn't show every extreme that they name: fetch[d, o] lists up to 2 distinct blocks of owner o (indices among the owner's 32 blocks, owner o holding global blocks o * 32 to o * 32 + 31) that device d fetches; -1 marks an empty place; every device fetches 2 blocks from some owner. pairs[r] names distinct fetched places s = o * 2 + i of the device that holds row r, each with fetch[that device, o, i] >= 0; -1 marks empty places, which come last; on every device some row has all 8 places live. `tile_place`: a permutation of the view tiles; view tiles are numbered row by row, 16 to a row. z = splats[:, 2] lies between 2 and 12.
All inputs are finite; a program needn't handle non-finite values.
Results may differ from the reference program's by a relative error of at most 0.0003.
Values sent between devices are 32-bit elements; how exact they have to be, the bound alone decides.
A program may use at most 128 MiB of HBM per device.

```python
import math
import jax
import jax.numpy as jnp
from jax import lax

NP = 55
BS = 128
CAP = 2
DEPTH = 8
TILES_DEV = 16
TX = 16
BLK_DEV = 32
BLOCKS = 1024
TILES = 512
N_GX = 4
N_GY = 8


def layout(key):
    devices = N_GX * N_GY
    classes = TILES_DEV
    members = devices // TILES_DEV
    band_rows = devices // TX
    slots = devices * CAP
    keys = jax.random.split(jax.random.fold_in(key, 7), 6)
    index = jnp.arange(devices, dtype=jnp.int32)
    band_index = jnp.arange(classes, dtype=jnp.int32)
    corner_score = jax.random.randint(keys[0], (classes, devices), 0, 1 << 16) * devices + index[None, :]
    corner_owner = jnp.argsort(corner_score, axis=1).astype(jnp.int32)
    owner_corner = jnp.argsort(corner_owner, axis=1).astype(jnp.int32)
    local_score = jax.random.randint(keys[1], (devices, BLK_DEV), 0, 1 << 16) * BLK_DEV + jnp.arange(BLK_DEV, dtype=jnp.int32)[None, :]
    local_order = jnp.argsort(local_score, axis=1).astype(jnp.int32)
    local_rank = jnp.argsort(local_order, axis=1).astype(jnp.int32)
    tile_row = index // TX
    tile_col = index % TX
    inner = (tile_row >= 1) & (tile_col >= 1)
    first_score = jax.random.randint(keys[2], (classes, devices), 0, 1 << 16) * devices + index[None, :] + jnp.where(inner, 0, 1 << 24)[None, :]
    first_rank = jnp.argsort(jnp.argsort(first_score, axis=1), axis=1)
    later = jax.random.randint(keys[3], (classes, devices), 0, 1 << 16) * devices + index[None, :]
    second_score = jnp.where(first_rank < members, first_rank, members + later)
    order = jnp.argsort(second_score, axis=1).astype(jnp.int32)
    group_member = jnp.arange(members, dtype=jnp.int32)
    turn = jnp.arange(TILES_DEV, dtype=jnp.int32)
    position = jnp.where(turn[None, :] == 0, group_member[:, None], members + group_member[:, None] * (TILES_DEV - 1) + turn[None, :] - 1).reshape(-1)
    band_tiles = order[:, position]
    tile_place = (band_index[:, None] * devices + band_tiles).reshape(-1).astype(jnp.int32)
    corner_table = jnp.stack([jnp.where(inner, (tile_row - 1) * TX + tile_col - 1, -1), jnp.where(tile_row >= 1, (tile_row - 1) * TX + tile_col, -1), jnp.where(tile_col >= 1, tile_row * TX + tile_col - 1, -1), index], axis=1)
    first_corners = corner_table[order[:, :members]].reshape(classes, members * 4)
    hit_first = jnp.any(first_corners[:, :, None] == index[None, None, :], axis=1)
    full = (jax.random.randint(keys[4], (classes, devices), 0, 100) < 80) | hit_first
    live_block = (jnp.arange(CAP)[None, None, :] == 0) | full[:, :, None]
    row_corners = corner_table[band_tiles]
    device_corners = row_corners.reshape(classes, members, TILES_DEV * 4)
    need = jnp.any(device_corners[:, :, :, None] == index[None, None, None, :], axis=2)
    need_owner = jnp.take_along_axis(need, jnp.broadcast_to(owner_corner[:, None, :], need.shape), axis=2)
    live_owner = jnp.take_along_axis(live_block, jnp.broadcast_to(owner_corner[:, :, None], (classes, devices, CAP)), axis=1)
    chosen = local_order[index[None, :, None], band_index[:, None, None] * CAP + jnp.arange(CAP, dtype=jnp.int32)[None, None, :]]
    fetch = jnp.where(need_owner[:, :, :, None] & live_owner[:, None, :, :], chosen[:, None, :, :], -1)
    fetch = fetch.reshape(devices, devices, CAP).astype(jnp.int32)
    valid = row_corners >= 0
    safe = jnp.maximum(row_corners, 0)
    entry = (safe[:, :, :, None] * CAP + jnp.arange(CAP)[None, None, None, :]).reshape(classes, devices * 4 * CAP)
    entry_live = jnp.take_along_axis(live_block.reshape(classes, slots), entry, axis=1).reshape(classes, devices, 4 * CAP)
    entry_live = entry_live & jnp.repeat(valid, CAP, axis=2)
    owners = jnp.take_along_axis(corner_owner, safe.reshape(classes, -1), axis=1).reshape(classes, devices, 4)
    places = (owners[:, :, :, None] * CAP + jnp.arange(CAP)[None, None, None, :]).reshape(classes, devices, 4 * CAP)
    depth_key = jax.random.randint(keys[5], (classes, slots), 0, 1 << 12) * slots + jnp.arange(slots)[None, :]
    entry_sort_key = jnp.take_along_axis(depth_key, entry, axis=1).reshape(classes, devices, 4 * CAP)
    spare = jnp.arange(4 * CAP)[None, None, :]
    score = jnp.where(entry_live, (1 << 30) - entry_sort_key, -1 - spare)
    best, taken = lax.top_k(score, DEPTH)
    picked = jnp.take_along_axis(places, taken, axis=2)
    pairs = jnp.where(best >= 0, picked, -1).reshape(TILES, DEPTH).astype(jnp.int32)
    block_owner = jnp.repeat(index, BLK_DEV)
    block_local = jnp.tile(jnp.arange(BLK_DEV, dtype=jnp.int32), devices)
    rank = local_rank[block_owner, block_local]
    band = rank // CAP
    which = rank % CAP
    corner = owner_corner[band, block_owner]
    centre_x = (16 * (corner % TX + 1)).astype(jnp.float32)
    centre_y = (16 * (band * band_rows + corner // TX + 1)).astype(jnp.float32)
    near = 2.0 + 9.0 * depth_key[band, corner * CAP + which].astype(jnp.float32) / float((1 << 12) * slots)
    return (fetch, pairs, tile_place, centre_x, centre_y, near)


def draw_fetch(key, part):
    return layout(key)[0]


def draw_pairs(key, part):
    return layout(key)[1]


def draw_tile_place(key, part):
    return layout(key)[2]


def draw_splats(key, part):
    _, _, _, centre_x, centre_y, near = layout(key)
    keys = jax.random.split(jax.random.fold_in(key, 11), 8)
    shape = (BLOCKS, BS)
    width = 16.0 * TX
    height = 16.0 * (TILES // TX)
    harmonic_scale = jnp.where(jnp.arange(48) % 16 == 0, 0.6, 0.2)[None, :, None]
    power_draw = jax.random.uniform(keys[3], shape, jnp.float32)
    spread = 4.0
    lower, upper = (3.5, 11.0)
    logit = -8.0 + 9.0 * power_draw ** 20
    jitter = 0.9
    coeffs = jax.random.normal(keys[4], (BLOCKS, 48, BS), jnp.float32) * harmonic_scale
    across = centre_x[:, None] + jax.random.uniform(keys[0], shape, jnp.float32, -spread, spread)
    down = centre_y[:, None] + jax.random.uniform(keys[1], shape, jnp.float32, -spread, spread)
    depth = near[:, None] + jax.random.uniform(keys[2], shape, jnp.float32, 0.0, jitter)
    first_scale = jax.random.uniform(keys[5], shape, jnp.float32, math.log(lower), math.log(upper))
    second_scale = jax.random.uniform(keys[6], shape, jnp.float32, math.log(lower), math.log(upper))
    angle = jax.random.uniform(keys[7], shape, jnp.float32, -math.pi, math.pi)
    place_x = (across - 0.5 * width) * depth / width
    place_y = (down - 0.5 * height) * depth / width
    head = jnp.stack([place_x, place_y, depth, first_scale, second_scale, angle, logit], axis=1)
    return jnp.concatenate([head, coeffs], axis=1).astype(jnp.float32)


def levels(key, dims, cuts, least, high):
    factor_of = 1.0
    for dim, parts in cuts:
        heights = jax.random.uniform(jax.random.fold_in(jax.random.fold_in(key, 6), dim), (parts,), jnp.float32, least / len(cuts), high / len(cuts))
        factor_of = factor_of * jnp.repeat(jnp.exp(heights), dims[dim] // parts).reshape((-1,) + (1,) * (len(dims) - 1 - dim))
    return factor_of


def noise(own_key, shape, scale, limit, cuts=(), held_as=jnp.bfloat16):
    result = jax.random.normal(own_key, shape, jnp.float32) * scale
    if len(cuts) > 0:
        result = levels(own_key, shape, cuts, -0.22, 0.18) * result
    return jnp.clip(result, min=-limit, max=limit).astype(held_as)


def setup_inputs(seed: int = 0) -> dict:
    streams_of = jax.random.split(jax.random.key(seed), 8)
    splats = draw_splats(jax.random.fold_in(streams_of[7], 71), 0)
    moment_one = noise(streams_of[1], (BLOCKS, NP, BS), 0.05, 0.3, ((0, 32),), jnp.float32)
    moment_two = jnp.clip(jnp.exp(math.log(1.0) - 6.9077552 * jax.random.uniform(streams_of[2], (BLOCKS, NP, BS), jnp.float32) ** levels(streams_of[2], (BLOCKS, NP, BS), ((0, 32),), -0.2, 0.2)), 0.001, 1.0)
    target = jnp.clip(1.0 * jax.random.uniform(streams_of[3], (TILES, 3, 256), jnp.float32) ** levels(streams_of[3], (TILES, 3, 256), ((0, 32),), -0.2, 0.2), 0.0, 1.0)
    tile_place = draw_tile_place(jax.random.fold_in(streams_of[7], 71), 0)
    pairs = draw_pairs(jax.random.fold_in(streams_of[7], 71), 0)
    fetch = draw_fetch(jax.random.fold_in(streams_of[7], 71), 0)
    return dict(splats=splats, moment_one=moment_one, moment_two=moment_two, target=target, tile_place=tile_place, pairs=pairs, fetch=fetch)


HARMONIC_ZERO = 0.28209479177387814
HARMONIC_ONE = 0.4886025119029199
HARMONIC_TWO = (1.0925484305920792, -1.0925484305920792, 0.31539156525252005, -1.0925484305920792, 0.5462742152960396)
HARMONIC_THREE = (-0.5900435899266435, 2.890611442640554, -0.4570457994644658, 0.3731763325901154, -0.4570457994644658, 1.445305721320277, -0.5900435899266435)

def harmonics(east, north, ahead):
    east_east = east * east
    north_north = north * north
    ahead_ahead = ahead * ahead
    terms = [jnp.full_like(east, HARMONIC_ZERO), -HARMONIC_ONE * north, HARMONIC_ONE * ahead, -HARMONIC_ONE * east, HARMONIC_TWO[0] * east * north, HARMONIC_TWO[1] * north * ahead, HARMONIC_TWO[2] * (2.0 * ahead_ahead - east_east - north_north), HARMONIC_TWO[3] * east * ahead, HARMONIC_TWO[4] * (east_east - north_north), HARMONIC_THREE[0] * north * (3.0 * east_east - north_north), HARMONIC_THREE[1] * east * north * ahead, HARMONIC_THREE[2] * north * (4.0 * ahead_ahead - east_east - north_north), HARMONIC_THREE[3] * ahead * (2.0 * ahead_ahead - 3.0 * east_east - 3.0 * north_north), HARMONIC_THREE[4] * east * (4.0 * ahead_ahead - east_east - north_north), HARMONIC_THREE[5] * ahead * (east_east - north_north), HARMONIC_THREE[6] * east * (east_east - 3.0 * north_north)]
    return jnp.stack(terms, axis=1)

def derive(raw, width, height):
    place_x = raw[:, 0]
    place_y = raw[:, 1]
    place_z = raw[:, 2]
    screen_u = width * place_x / place_z + 0.5 * width
    screen_v = width * place_y / place_z + 0.5 * height
    inverse_one = jnp.exp(-2.0 * raw[:, 3])
    inverse_two = jnp.exp(-2.0 * raw[:, 4])
    cosine = jnp.cos(raw[:, 5])
    sine = jnp.sin(raw[:, 5])
    conic_a = cosine * cosine * inverse_one + sine * sine * inverse_two
    conic_b = cosine * sine * (inverse_one - inverse_two)
    conic_c = sine * sine * inverse_one + cosine * cosine * inverse_two
    opacity = jax.nn.sigmoid(raw[:, 6])
    length = jnp.sqrt(place_x * place_x + place_y * place_y + place_z * place_z)
    basis = harmonics(place_x / length, place_y / length, place_z / length)
    coeffs = raw[:, 7:].reshape(raw.shape[0], 3, 16, raw.shape[2])
    colors = 0.5 + lax.optimization_barrier(jnp.sum(coeffs * basis[:, None], axis=2))
    head = jnp.stack([screen_u, screen_v, conic_a, conic_b, conic_c, opacity], axis=1)
    return jnp.concatenate([head, colors], axis=1)

def composite(screens, pixel_x, pixel_y):

    def advance(carry, screen_splat):
        log_trans, pixel_colour = carry
        delta_x = pixel_x[:, :, None] - screen_splat[:, None, 0]
        delta_y = pixel_y[:, :, None] - screen_splat[:, None, 1]
        power = -0.5 * (screen_splat[:, None, 2] * delta_x * delta_x + 2.0 * screen_splat[:, None, 3] * delta_x * delta_y + screen_splat[:, None, 4] * delta_y * delta_y)
        alpha = screen_splat[:, None, 5] * jnp.exp(power)
        log_keep = jnp.log1p(-alpha)
        before = jnp.cumsum(log_keep, axis=2) - log_keep
        blend_weight = alpha * jnp.exp(log_trans[:, :, None] + before)
        pixel_colour = pixel_colour + jnp.einsum('ylo,yeo->yel', blend_weight, screen_splat[:, 6:9], precision=lax.Precision.HIGHEST)
        return ((log_trans + lax.optimization_barrier(jnp.sum(log_keep, axis=2)), pixel_colour), None)
    count = screens.shape[0]
    start = (jnp.zeros((count, 256), jnp.float32), jnp.zeros((count, 3, 256), jnp.float32))
    (_, pixel_colour), _ = lax.scan(jax.checkpoint(advance), start, jnp.moveaxis(screens, 1, 0))
    return pixel_colour

def reference(splats, moment_one, moment_two, target, tile_place, pairs, fetch):
    devices = N_GX * N_GY
    width = 16.0 * TX
    height = 16.0 * (TILES // TX)
    screen_all, pull_all = jax.vjp(lambda raw: derive(raw, width, height), splats)
    rows = jnp.arange(TILES, dtype=jnp.int32)
    device_of = rows // TILES_DEV
    place = jnp.maximum(pairs, 0).astype(jnp.int32)
    flat_index = (device_of[:, None] * (devices * CAP) + place).astype(jnp.int32)
    local = fetch.reshape(-1)[flat_index]
    block_id = jnp.where(pairs >= 0, place // CAP * BLK_DEV + local, 0).astype(jnp.int32)
    used = (pairs >= 0).astype(jnp.float32)
    pixel = jnp.arange(256, dtype=jnp.int32)
    corner_x = (tile_place % TX * 16).astype(jnp.float32)
    corner_y = (tile_place // TX * 16).astype(jnp.float32)
    pixel_x = corner_x[:, None] + (pixel % 16).astype(jnp.float32)[None, :] + 0.5
    pixel_y = corner_y[:, None] + (pixel // 16).astype(jnp.float32)[None, :] + 0.5
    group = 16
    groups = TILES // group

    def one_group(total, pieces):
        ids, mask, across, down, goal = pieces
        slots = screen_all[ids] * mask[:, :, None, None]

        def objective(screens):
            image = composite(screens, across, down)
            residual = image - goal
            return (image, jnp.sum(residual * residual) / 512.0)
        (image, loss), pull = jax.vjp(objective, slots)
        grads, = pull((jnp.zeros_like(image), jnp.ones_like(loss)))
        grads = grads * mask[:, :, None, None]
        total = total.at[ids.reshape(-1)].add(grads.reshape((-1,) + grads.shape[2:]))
        return (total, image)
    pieces = (block_id.reshape(groups, group, DEPTH), used.reshape(groups, group, DEPTH), pixel_x.reshape(groups, group, 256), pixel_y.reshape(groups, group, 256), target.reshape(groups, group, 3, 256))
    total, images = lax.scan(one_group, jnp.zeros_like(screen_all), pieces)
    image = images.reshape(TILES, 3, 256)
    splat_grad, = pull_all(total)
    first = 0.9 * moment_one + 0.1 * splat_grad
    second_moment = 0.999 * moment_two + 0.001 * splat_grad * splat_grad
    adam_step = first / (jnp.sqrt(second_moment) + 1e-08)
    return (image, splat_grad, adam_step)
```

```python
import functools

import jax
import jax.numpy as jnp
import numpy as np
from jax import lax
from jax.experimental import pallas as pl
from jax.experimental.pallas import tpu as pltpu
from jax.sharding import PartitionSpec as P

TX = 16
SIDE = 16
PIXELS = SIDE * SIDE
LOG2E = 1.4426950408889634
DEAD = -1.0e4
GROUP = 4
F32 = jnp.float32
BF16 = jnp.bfloat16


HARMONIC_ZERO = 0.28209479177387814
HARMONIC_ONE = 0.4886025119029199
HARMONIC_TWO = (
    1.0925484305920792,
    -1.0925484305920792,
    0.31539156525252005,
    -1.0925484305920792,
    0.5462742152960396,
)
HARMONIC_THREE = (
    -0.5900435899266435,
    2.890611442640554,
    -0.4570457994644658,
    0.3731763325901154,
    -0.4570457994644658,
    1.445305721320277,
    -0.5900435899266435,
)


def harmonics(east, north, ahead):
    east_east = east * east
    north_north = north * north
    ahead_ahead = ahead * ahead
    terms = [
        jnp.full_like(east, HARMONIC_ZERO),
        -HARMONIC_ONE * north,
        HARMONIC_ONE * ahead,
        -HARMONIC_ONE * east,
        HARMONIC_TWO[0] * east * north,
        HARMONIC_TWO[1] * north * ahead,
        HARMONIC_TWO[2] * (2.0 * ahead_ahead - east_east - north_north),
        HARMONIC_TWO[3] * east * ahead,
        HARMONIC_TWO[4] * (east_east - north_north),
        HARMONIC_THREE[0] * north * (3.0 * east_east - north_north),
        HARMONIC_THREE[1] * east * north * ahead,
        HARMONIC_THREE[2] * north * (4.0 * ahead_ahead - east_east - north_north),
        HARMONIC_THREE[3] * ahead * (2.0 * ahead_ahead - 3.0 * east_east - 3.0 * north_north),
        HARMONIC_THREE[4] * east * (4.0 * ahead_ahead - east_east - north_north),
        HARMONIC_THREE[5] * ahead * (east_east - north_north),
        HARMONIC_THREE[6] * east * (east_east - 3.0 * north_north),
    ]
    return jnp.stack(terms, axis=1)


def derive(raw, width, height):
    place_x = raw[:, 0]
    place_y = raw[:, 1]
    place_z = raw[:, 2]
    screen_u = width * place_x / place_z + 0.5 * width
    screen_v = width * place_y / place_z + 0.5 * height
    inverse_one = jnp.exp(-2.0 * raw[:, 3])
    inverse_two = jnp.exp(-2.0 * raw[:, 4])
    cosine = jnp.cos(raw[:, 5])
    sine = jnp.sin(raw[:, 5])
    conic_a = cosine * cosine * inverse_one + sine * sine * inverse_two
    conic_b = cosine * sine * (inverse_one - inverse_two)
    conic_c = sine * sine * inverse_one + cosine * cosine * inverse_two
    log_opacity = jax.nn.log_sigmoid(raw[:, 6])
    length = jnp.sqrt(place_x * place_x + place_y * place_y + place_z * place_z)
    basis = harmonics(place_x / length, place_y / length, place_z / length)
    coeffs = raw[:, 7:].reshape(raw.shape[0], 3, 16, raw.shape[2])
    colors = 0.5 + jnp.sum(coeffs * basis[:, None], axis=2)
    head = jnp.stack([screen_u, screen_v, conic_a, conic_b, conic_c, log_opacity], axis=1)
    return jnp.concatenate([head, colors], axis=1)


def pixel_basis():
    j = np.arange(PIXELS)
    x = j % SIDE + 0.5 - SIDE / 2
    y = j // SIDE + 0.5 - SIDE / 2
    rows = np.stack([x * x, x * y, y * y, x, y, np.ones_like(x), 0 * x, 0 * x])
    return np.concatenate([rows, rows, rows, 0 * rows]).astype(np.float32)


def lane_order(block):
    row = np.arange(block)
    splat = (row % 8) * (block // 8) + row // 8
    return (np.arange(block)[:, None] == splat[None, :]).astype(np.float32)


def rounded(x):
    return x.astype(BF16).astype(F32)


def shifted(x, shift):
    return pltpu.roll(x, shift % 8, 0)


def blend_kernel(
    pairs_ref, place_ref, order_ref, basis_ref, arrived_ref, target_ref, image_ref, grad_ref,
    screen, parts, hue_sum, hue_back, alphas, keeps, weights, halves, ends, slopes, steps, resid, moments,
):
    tiles, depth = pairs_ref.shape
    slots, rows, block = arrived_ref.shape
    chunks = block // 8
    sub = lax.broadcasted_iota(jnp.int32, (8, PIXELS), 0)

    grad_ref[...] = jnp.zeros_like(grad_ref)
    resid[...] = jnp.zeros_like(resid)
    parts[...] = jnp.zeros_like(parts)
    hue_sum[...] = jnp.zeros_like(hue_sum)
    hue_back[...] = jnp.zeros_like(hue_back)

    def prepare(s, _):
        screen[s, 0:rows] = arrived_ref[s]
        hue = jnp.concatenate([arrived_ref[s, 6:9], jnp.zeros((5, block), F32)], axis=0)
        hue1 = rounded(hue)
        hue2 = hue - hue1
        zero = jnp.zeros_like(hue)
        hue_sum[s] = jnp.concatenate(
            [
                jnp.concatenate([hue1, hue1], axis=1),
                jnp.concatenate([hue2, zero], axis=1),
            ],
            axis=0,
        ).astype(BF16)
        hue_back[s] = jnp.concatenate([hue1, hue2, hue1, zero], axis=0).astype(BF16)
        return 0

    lax.fori_loop(0, slots, prepare, 0)
    screen[slots] = jnp.zeros((16, block), F32)
    screen[slots, 5:6] = jnp.full((1, block), DEAD, F32)

    basis = basis_ref[...].astype(BF16)
    monomials = basis_ref[0:8].astype(BF16)
    zero_row = jnp.zeros((8, PIXELS), F32)

    def group(step, _):
        row = [order_ref[step * GROUP + t] for t in range(GROUP)]
        deepest = jnp.int32(0)
        centre = []
        for t in range(GROUP):
            tile = place_ref[row[t]]
            count = jnp.int32(0)
            for k in range(depth):
                count = count + (pairs_ref[row[t], k] >= 0).astype(jnp.int32)
            deepest = jnp.maximum(deepest, count)
            cx = (lax.rem(tile, TX) * SIDE + SIDE // 2).astype(F32)
            cy = (lax.div(tile, TX) * SIDE + SIDE // 2).astype(F32)
            centre.append((cx, cy))

        def place(t, k):
            slot = pairs_ref[row[t], k]
            return jnp.where(slot >= 0, slot, slots)

        def shape_up(k, _):
            for t in range(GROUP):
                cx, cy = centre[t]
                s = place(t, k)
                u = screen[s, 0:1] - cx
                v = screen[s, 1:2] - cy
                a, b, c = screen[s, 2:3], screen[s, 3:4], screen[s, 4:5]
                opac = jnp.maximum(screen[s, 5:6], DEAD)
                lin_x = a * u + b * v
                lin_y = b * u + c * v
                const = opac - 0.5 * (lin_x * u + lin_y * v)
                for j, value in enumerate((-0.5 * a, -b, -0.5 * c, lin_x, lin_y, const)):
                    parts[t, k, j : j + 1] = LOG2E * value
            return 0

        lax.fori_loop(0, deepest, shape_up, 0)

        def forward(k, carry):
            after = []
            for t in range(GROUP):
                trans, total = carry[2 * t], carry[2 * t + 1]
                c = parts[t, k]
                c1 = rounded(c)
                c2 = rounded(c - c1)
                c3 = c - c1 - c2
                left = jnp.concatenate([c1, c2, c3, jnp.zeros_like(c)], axis=0).astype(BF16)
                power = lax.dot_general(
                    left, basis, (((0,), (0,)), ((), ())), preferred_element_type=F32
                )
                alpha = jnp.exp2(power)
                keep = 1.0 - alpha
                alphas[t] = alpha
                keeps[t, k] = keep
                kept = keep[0:8]
                for i in range(1, chunks):
                    kept = kept * keep[8 * i : 8 * i + 8]
                scan = jnp.where(sub == 0, trans, shifted(kept, 1))
                for d in (1, 2, 4):
                    scan = scan * jnp.where(sub < d, 1.0, shifted(scan, d))
                end = scan * kept
                ends[t, k] = end
                trans = jnp.broadcast_to(end[7:8], (8, PIXELS))
                here = scan
                for i in range(0, chunks, 2):
                    lo, mid, hi = 8 * i, 8 * i + 8, 8 * i + 16
                    one = alphas[t, lo:mid] * here
                    here = here * keeps[t, k, lo:mid]
                    two = alphas[t, mid:hi] * here
                    here = here * keeps[t, k, mid:hi]
                    pair = jnp.concatenate([one, two], axis=0)
                    weights[t, k, lo:hi] = pair
                    high = pair.astype(BF16)
                    halves[t, k, lo:hi] = high
                    halves[t, k, block + lo : block + hi] = (pair - high.astype(F32)).astype(BF16)
                total = total + jnp.dot(
                    hue_sum[place(t, k)], halves[t, k], preferred_element_type=F32
                )
                after += [trans, total]
            return tuple(after)

        start = (jnp.ones((8, PIXELS), F32), jnp.zeros((16, PIXELS), F32)) * GROUP
        done = lax.fori_loop(0, deepest, forward, start)

        pulls = []
        for t in range(GROUP):
            total = done[2 * t + 1]
            image = (total[0:8] + total[8:16])[0:3]
            image_ref[row[t]] = image
            resid[t, 0:3] = (image - target_ref[row[t]]) * (2.0 / 512.0)
            g = resid[t]
            g1 = rounded(g)
            g2 = g - g1
            pulls.append(
                (
                    jnp.concatenate([g1, g1, g2, zero_row], axis=0).astype(BF16),
                    jnp.concatenate([g1, g2], axis=0).astype(BF16),
                )
            )

        def backward(index, carry):
            k = deepest - 1 - index
            after = []
            for t in range(GROUP):
                behind = carry[t]
                g3, g2 = pulls[t]
                slope = lax.dot_general(
                    hue_back[place(t, k)], g3, (((0,), (0,)), ((), ())), preferred_element_type=F32
                )
                slopes[t] = slope
                lit = weights[t, k] * slope
                run = lit[0:8]
                for i in range(1, chunks):
                    run = run + lit[8 * i : 8 * i + 8]
                scan = jnp.where(sub == 7, behind, shifted(run, -1))
                for d in (1, 2, 4):
                    scan = scan + jnp.where(sub < 8 - d, shifted(scan, -d), 0.0)
                after.append(jnp.broadcast_to((run + scan)[0:1], (8, PIXELS)))
                here = scan / jnp.maximum(ends[t, k], 1e-37)
                for i in range(chunks - 2, -1, -2):
                    lo, mid, hi = 8 * i, 8 * i + 8, 8 * i + 16
                    ahead = slopes[t, mid:hi]
                    gap = ahead - here
                    two = weights[t, k, mid:hi] * gap
                    here = ahead - keeps[t, k, mid:hi] * gap
                    ahead = slopes[t, lo:mid]
                    gap = ahead - here
                    one = weights[t, k, lo:mid] * gap
                    here = ahead - keeps[t, k, lo:mid] * gap
                    pair = jnp.concatenate([one, two], axis=0)
                    high = pair.astype(BF16)
                    steps[t, lo:hi] = high
                    steps[t, block + lo : block + hi] = (pair - high.astype(F32)).astype(BF16)
                sums = lax.dot_general(
                    monomials, steps[t], (((1,), (1,)), ((), ())), preferred_element_type=F32
                )
                moments[t, k, 0:8] = sums[:, 0:block] + sums[:, block:]
                hues = lax.dot_general(
                    g2, halves[t, k], (((1,), (1,)), ((), ())), preferred_element_type=F32
                )
                moments[t, k, 8:16] = (
                    hues[0:8, 0:block] + hues[0:8, block:] + hues[8:16, 0:block]
                )
            return tuple(after)

        lax.fori_loop(0, deepest, backward, (jnp.zeros((8, PIXELS), F32),) * GROUP)

        def settle(k, _):
            for t in range(GROUP):
                cx, cy = centre[t]
                s = place(t, k)
                u = screen[s, 0:1] - cx
                v = screen[s, 1:2] - cy
                a, b, c = screen[s, 2:3], screen[s, 3:4], screen[s, 4:5]
                mxx, mxy, myy = (moments[t, k, j : j + 1] for j in (0, 1, 2))
                mx, my, m = (moments[t, k, j : j + 1] for j in (3, 4, 5))
                off_x = mx - u * m
                off_y = my - v * m
                changes = (
                    a * off_x + b * off_y,
                    b * off_x + c * off_y,
                    -0.5 * (mxx - u * (mx + off_x)),
                    -(mxy - u * my - v * off_x),
                    -0.5 * (myy - v * (my + off_y)),
                    m,
                    moments[t, k, 8:9],
                    moments[t, k, 9:10],
                    moments[t, k, 10:11],
                )
                for j, change in enumerate(changes):
                    grad_ref[s, j : j + 1] = grad_ref[s, j : j + 1] + change
            return 0

        lax.fori_loop(0, deepest, settle, 0)
        return 0

    lax.fori_loop(0, tiles // GROUP, group, 0)


def deepest_first(pairs):
    live = jnp.sum((pairs >= 0).astype(jnp.int32), axis=1)
    row = jnp.arange(pairs.shape[0], dtype=jnp.int32)
    before = (live[None, :] > live[:, None]) | (
        (live[None, :] == live[:, None]) & (row[None, :] < row[:, None])
    )
    rank = jnp.sum(before.astype(jnp.int32), axis=1)
    return jnp.sum(jnp.where(rank[None, :] == row[:, None], row[None, :], 0), axis=1)


def blend(arrived, target, tile_place, pairs):
    tiles, channels, pixels = target.shape
    depth = pairs.shape[1]
    slots, rows, block = arrived.shape
    basis = jnp.asarray(pixel_basis())
    smem = pl.BlockSpec(memory_space=pltpu.SMEM)
    vmem = pl.BlockSpec(memory_space=pltpu.VMEM)
    image, grads = pl.pallas_call(
        blend_kernel,
        in_specs=[smem, smem, smem, vmem, vmem, vmem],
        out_specs=[vmem, vmem],
        scratch_shapes=[
            pltpu.VMEM((slots + 1, 16, block), F32),
            pltpu.VMEM((GROUP, depth, 8, block), F32),
            pltpu.VMEM((slots + 1, 16, 2 * block), BF16),
            pltpu.VMEM((slots + 1, 32, block), BF16),
            pltpu.VMEM((GROUP, block, pixels), F32),
            pltpu.VMEM((GROUP, depth, block, pixels), F32),
            pltpu.VMEM((GROUP, depth, block, pixels), F32),
            pltpu.VMEM((GROUP, depth, 2 * block, pixels), BF16),
            pltpu.VMEM((GROUP, depth, 8, pixels), F32),
            pltpu.VMEM((GROUP, block, pixels), F32),
            pltpu.VMEM((GROUP, 2 * block, pixels), BF16),
            pltpu.VMEM((GROUP, 8, pixels), F32),
            pltpu.VMEM((GROUP, depth, 16, block), F32),
        ],
        out_shape=[
            jax.ShapeDtypeStruct(target.shape, F32),
            jax.ShapeDtypeStruct((slots + 1, rows, block), F32),
        ],
        name="blend",
    )(pairs, tile_place, deepest_first(pairs), basis, arrived, target)
    return image, grads[:slots]


def trade(payload):
    return lax.all_to_all(payload, ("gx", "gy"), split_axis=0, concat_axis=0, tiled=True)


def local(splats, moment_one, moment_two, target, tile_place, pairs, fetch):
    devices = lax.axis_size("gx") * lax.axis_size("gy")
    tiles_here = target.shape[0]
    width = 16.0 * TX
    height = 16.0 * (tiles_here * devices // TX)
    order = jnp.asarray(lane_order(splats.shape[2]))

    def project(raw):
        return jnp.dot(derive(raw, width, height), order, precision=lax.Precision.HIGHEST)

    asked = lax.all_to_all(fetch[0], ("gx", "gy"), split_axis=0, concat_axis=0, tiled=True)
    wanted = jnp.maximum(asked, 0)
    own_screen, own_pull = jax.vjp(project, splats)
    payload = own_screen[wanted]
    arrived = trade(payload)
    arrived = arrived.reshape((-1,) + payload.shape[2:])
    image, received_gradients = blend(arrived, target, tile_place, pairs)
    returned = trade(received_gradients.reshape(payload.shape))
    owner_pick = (asked.reshape(-1)[None, :] == jnp.arange(splats.shape[0])[:, None]).astype(
        jnp.float32
    )
    summed = jnp.dot(
        owner_pick, returned.reshape(owner_pick.shape[1], -1), precision=lax.Precision.HIGHEST
    )
    summed = summed.reshape((splats.shape[0],) + returned.shape[2:])
    (splat_grad,) = own_pull(summed)
    first = 0.9 * moment_one + 0.1 * splat_grad
    second_moment = 0.999 * moment_two + 0.001 * splat_grad * splat_grad
    adam_step = first / (jnp.sqrt(second_moment) + 1e-08)
    return (image, splat_grad, adam_step)


def solution(mesh):
    both = ("gx", "gy")
    return jax.shard_map(
        local,
        mesh=mesh,
        in_specs=(
            P(both, None, None),
            P(both, None, None),
            P(both, None, None),
            P(both, None, None),
            P(both),
            P(both, None),
            P(both, None, None),
        ),
        out_specs=(P(both, None, None), P(both, None, None), P(both, None, None)),
        check_vma=False,
    )
```

```python
import functools

import jax
import jax.numpy as jnp
import numpy as np
from jax import lax
from jax.experimental import pallas as pl
from jax.experimental.pallas import tpu as pltpu
from jax.sharding import PartitionSpec as P

TX = 16
SIDE = 16
PIXELS = SIDE * SIDE
LOG2E = 1.4426950408889634
DEAD = -1.0e4
GROUP = 4
PAIR = 2
F32 = jnp.float32
BF16 = jnp.bfloat16


HARMONIC_ZERO = 0.28209479177387814
HARMONIC_ONE = 0.4886025119029199
HARMONIC_TWO = (
    1.0925484305920792,
    -1.0925484305920792,
    0.31539156525252005,
    -1.0925484305920792,
    0.5462742152960396,
)
HARMONIC_THREE = (
    -0.5900435899266435,
    2.890611442640554,
    -0.4570457994644658,
    0.3731763325901154,
    -0.4570457994644658,
    1.445305721320277,
    -0.5900435899266435,
)


def harmonics(east, north, ahead):
    east_east = east * east
    north_north = north * north
    ahead_ahead = ahead * ahead
    terms = [
        jnp.full_like(east, HARMONIC_ZERO),
        -HARMONIC_ONE * north,
        HARMONIC_ONE * ahead,
        -HARMONIC_ONE * east,
        HARMONIC_TWO[0] * east * north,
        HARMONIC_TWO[1] * north * ahead,
        HARMONIC_TWO[2] * (2.0 * ahead_ahead - east_east - north_north),
        HARMONIC_TWO[3] * east * ahead,
        HARMONIC_TWO[4] * (east_east - north_north),
        HARMONIC_THREE[0] * north * (3.0 * east_east - north_north),
        HARMONIC_THREE[1] * east * north * ahead,
        HARMONIC_THREE[2] * north * (4.0 * ahead_ahead - east_east - north_north),
        HARMONIC_THREE[3] * ahead * (2.0 * ahead_ahead - 3.0 * east_east - 3.0 * north_north),
        HARMONIC_THREE[4] * east * (4.0 * ahead_ahead - east_east - north_north),
        HARMONIC_THREE[5] * ahead * (east_east - north_north),
        HARMONIC_THREE[6] * east * (east_east - 3.0 * north_north),
    ]
    return jnp.stack(terms, axis=1)


def derive(raw, width, height):
    place_x = raw[:, 0]
    place_y = raw[:, 1]
    place_z = raw[:, 2]
    screen_u = width * place_x / place_z + 0.5 * width
    screen_v = width * place_y / place_z + 0.5 * height
    inverse_one = jnp.exp(-2.0 * raw[:, 3])
    inverse_two = jnp.exp(-2.0 * raw[:, 4])
    cosine = jnp.cos(raw[:, 5])
    sine = jnp.sin(raw[:, 5])
    conic_a = cosine * cosine * inverse_one + sine * sine * inverse_two
    conic_b = cosine * sine * (inverse_one - inverse_two)
    conic_c = sine * sine * inverse_one + cosine * cosine * inverse_two
    log_opacity = jax.nn.log_sigmoid(raw[:, 6])
    length = jnp.sqrt(place_x * place_x + place_y * place_y + place_z * place_z)
    basis = harmonics(place_x / length, place_y / length, place_z / length)
    coeffs = raw[:, 7:].reshape(raw.shape[0], 3, 16, raw.shape[2])
    colors = 0.5 + jnp.sum(coeffs * basis[:, None], axis=2)
    head = jnp.stack([screen_u, screen_v, conic_a, conic_b, conic_c, log_opacity], axis=1)
    return jnp.concatenate([head, colors], axis=1)


def pixel_basis():
    j = np.arange(PIXELS)
    x = j % SIDE + 0.5 - SIDE / 2
    y = j // SIDE + 0.5 - SIDE / 2
    rows = np.stack([x * x, x * y, y * y, x, y, np.ones_like(x), 0 * x, 0 * x])
    return np.concatenate([rows, rows, rows, 0 * rows]).astype(np.float32)


def lane_order(block):
    row = np.arange(block)
    splat = (row % 8) * (block // 8) + row // 8
    return (np.arange(block)[:, None] == splat[None, :]).astype(np.float32)


def rounded(x):
    return x.astype(BF16).astype(F32)


def shifted(x, shift):
    return pltpu.roll(x, shift % 8, 0)


def blend_kernel(
    pairs_ref, place_ref, order_ref, basis_ref, arrived_ref, target_ref, image_ref, grad_ref,
    screen, hue_sum, hue_back, alphas, slopes, steps, resid, *banks,
):
    tiles, depth = pairs_ref.shape
    slots, rows, block = arrived_ref.shape
    chunks = block // 8
    lanes = range(GROUP)
    spots = [(t, e) for e in range(PAIR) for t in lanes]
    parts, keeps, weights, halves, ends, moments = (
        banks[GROUP * i : GROUP * i + GROUP] for i in range(6)
    )
    sub = lax.broadcasted_iota(jnp.int32, (8, PIXELS), 0)

    resid[...] = jnp.zeros_like(resid)
    for t in lanes:
        parts[t][...] = jnp.zeros_like(parts[t])

    def prepare(s, _):
        grad_ref[s] = jnp.zeros((rows, block), F32)
        screen[s, 0:rows] = arrived_ref[s]
        hue = jnp.concatenate([arrived_ref[s, 6:9], jnp.zeros((5, block), F32)], axis=0)
        hue1 = rounded(hue)
        hue2 = hue - hue1
        zero = jnp.zeros_like(hue)
        hue_sum[s] = jnp.concatenate(
            [
                jnp.concatenate([hue1, hue1], axis=1),
                jnp.concatenate([hue2, zero], axis=1),
            ],
            axis=0,
        ).astype(BF16)
        hue_back[s] = jnp.concatenate([hue1, hue2, hue1, zero], axis=0).astype(BF16)
        return 0

    lax.fori_loop(0, slots, prepare, 0)
    grad_ref[slots] = jnp.zeros((rows, block), F32)
    screen[slots] = jnp.zeros((16, block), F32)
    screen[slots, 5:6] = jnp.full((1, block), DEAD, F32)
    hue_sum[slots] = jnp.zeros((16, 2 * block), BF16)
    hue_back[slots] = jnp.zeros((32, block), BF16)

    basis = basis_ref[...].astype(BF16)
    monomials = basis_ref[0:8].astype(BF16)
    zero_row = jnp.zeros((8, PIXELS), F32)

    def group(step, _):
        row = [order_ref[step * GROUP + t] for t in lanes]
        deepest = jnp.int32(0)
        for k in range(depth):
            deepest = deepest + (pairs_ref[row[0], k] >= 0).astype(jnp.int32)
        turns = lax.div(deepest + (PAIR - 1), PAIR)
        centre = []
        for t in lanes:
            tile = place_ref[row[t]]
            cx = (lax.rem(tile, TX) * SIDE + SIDE // 2).astype(F32)
            cy = (lax.div(tile, TX) * SIDE + SIDE // 2).astype(F32)
            centre.append((cx, cy))

        def place(t, k):
            slot = pairs_ref[row[t], k]
            return jnp.where(slot >= 0, slot, slots)

        def shape_up(k, _):
            for t, e in spots:
                cx, cy = centre[t]
                s = place(t, PAIR * k + e)
                u = screen[s, 0:1] - cx
                v = screen[s, 1:2] - cy
                a, b, c = screen[s, 2:3], screen[s, 3:4], screen[s, 4:5]
                opac = jnp.maximum(screen[s, 5:6], DEAD)
                lin_x = a * u + b * v
                lin_y = b * u + c * v
                const = opac - 0.5 * (lin_x * u + lin_y * v)
                for j, value in enumerate((-0.5 * a, -b, -0.5 * c, lin_x, lin_y, const)):
                    parts[t][k, e, j : j + 1] = LOG2E * value
            return 0

        lax.fori_loop(0, turns, shape_up, 0)

        def power_of(t, j, e):
            c = parts[t][j, e]
            c1 = rounded(c)
            c2 = rounded(c - c1)
            c3 = c - c1 - c2
            left = jnp.concatenate([c1, c2, c3, jnp.zeros_like(c)], axis=0).astype(BF16)
            return lax.dot_general(
                left, basis, (((0,), (0,)), ((), ())), preferred_element_type=F32
            )

        def draw(t, j, e, power):
            alpha = jnp.exp2(power)
            alphas[e, t] = alpha
            keep = 1.0 - alpha
            keeps[t][j, e] = keep
            kept = keep[0:8]
            for i in range(1, chunks):
                kept = kept * keep[8 * i : 8 * i + 8]
            return kept

        def scan_of(t, j, e, kept, trans):
            scan = jnp.where(sub == 0, trans, shifted(kept, 1))
            for d in (1, 2, 4):
                scan = scan * jnp.where(sub < d, 1.0, shifted(scan, d))
            end = scan * kept
            ends[t][j, e] = end
            return scan, jnp.broadcast_to(end[7:8], (8, PIXELS))

        def spread(t, j, e, here):
            for i in range(0, chunks, 2):
                lo, mid, hi = 8 * i, 8 * i + 8, 8 * i + 16
                one = alphas[e, t, lo:mid] * here
                here = here * keeps[t][j, e, lo:mid]
                two = alphas[e, t, mid:hi] * here
                here = here * keeps[t][j, e, mid:hi]
                pair = jnp.concatenate([one, two], axis=0)
                weights[t][j, e, lo:hi] = pair
                high = pair.astype(BF16)
                halves[t][j, e, lo:hi] = high
                halves[t][j, e, block + lo : block + hi] = (pair - high.astype(F32)).astype(BF16)

        def summed(t, j, e):
            return jnp.dot(
                hue_sum[place(t, PAIR * j + e)], halves[t][j, e], preferred_element_type=F32
            )

        def forward(j, carry):
            trans = [carry[2 * t] for t in lanes]
            totals = [carry[2 * t + 1] for t in lanes]
            powers = [[power_of(t, j, e) for t in lanes] for e in range(PAIR)]
            kepts = [draw(t, j, 0, powers[0][t]) for t in lanes]
            for e in range(PAIR):
                heres = []
                for t in lanes:
                    here, trans[t] = scan_of(t, j, e, kepts[t], trans[t])
                    heres.append(here)
                for t in lanes:
                    spread(t, j, e, heres[t])
                    if e + 1 < PAIR:
                        kepts[t] = draw(t, j, e + 1, powers[e + 1][t])
                totals = [totals[t] + summed(t, j, e) for t in lanes]
            return tuple(x for t in lanes for x in (trans[t], totals[t]))

        start = (jnp.ones((8, PIXELS), F32), jnp.zeros((16, PIXELS), F32)) * GROUP
        done = lax.fori_loop(0, turns, forward, start)

        pulls = []
        for t in lanes:
            total = done[2 * t + 1]
            image = (total[0:8] + total[8:16])[0:3]
            image_ref[row[t]] = image
            resid[t, 0:3] = (image - target_ref[row[t]]) * (2.0 / 512.0)
            g = resid[t]
            g1 = rounded(g)
            g2 = g - g1
            pulls.append(
                (
                    jnp.concatenate([g1, g1, g2, zero_row], axis=0).astype(BF16),
                    jnp.concatenate([g1, g2], axis=0).astype(BF16),
                )
            )

        def lean(t, j, e):
            slopes[e, t] = lax.dot_general(
                hue_back[place(t, PAIR * j + e)],
                pulls[t][0],
                (((0,), (0,)), ((), ())),
                preferred_element_type=F32,
            )

        def behind_of(t, j, e, behind):
            run = weights[t][j, e, 0:8] * slopes[e, t, 0:8]
            for i in range(1, chunks):
                lo, hi = 8 * i, 8 * i + 8
                run = run + weights[t][j, e, lo:hi] * slopes[e, t, lo:hi]
            scan = jnp.where(sub == 7, behind, shifted(run, -1))
            for d in (1, 2, 4):
                scan = scan + jnp.where(sub < 8 - d, shifted(scan, -d), 0.0)
            return (
                scan / jnp.maximum(ends[t][j, e], 1e-37),
                jnp.broadcast_to((run + scan)[0:1], (8, PIXELS)),
            )

        def step_of(t, j, e, here):
            for i in range(chunks - 2, -1, -2):
                lo, mid, hi = 8 * i, 8 * i + 8, 8 * i + 16
                ahead = slopes[e, t, mid:hi]
                gap = ahead - here
                two = weights[t][j, e, mid:hi] * gap
                here = ahead - keeps[t][j, e, mid:hi] * gap
                ahead = slopes[e, t, lo:mid]
                gap = ahead - here
                one = weights[t][j, e, lo:mid] * gap
                here = ahead - keeps[t][j, e, lo:mid] * gap
                pair = jnp.concatenate([one, two], axis=0)
                high = pair.astype(BF16)
                steps[e, t, lo:hi] = high
                steps[e, t, block + lo : block + hi] = (pair - high.astype(F32)).astype(BF16)

        def backward(index, carry):
            j = turns - 1 - index
            behind = list(carry)
            places = []
            for e in reversed(range(PAIR)):
                for t in lanes:
                    lean(t, j, e)
            for e in reversed(range(PAIR)):
                for t in lanes:
                    hues = lax.dot_general(
                        pulls[t][1], halves[t][j, e], (((1,), (1,)), ((), ())),
                        preferred_element_type=F32,
                    )
                    places.append(
                        (t, e, 8, hues[0:8, 0:block] + hues[0:8, block:] + hues[8:16, 0:block])
                    )
                heres = []
                for t in lanes:
                    here, behind[t] = behind_of(t, j, e, behind[t])
                    heres.append(here)
                for t in lanes:
                    step_of(t, j, e, heres[t])
                for t in lanes:
                    sums = lax.dot_general(
                        monomials, steps[e, t], (((1,), (1,)), ((), ())), preferred_element_type=F32
                    )
                    places.append((t, e, 0, sums[:, 0:block] + sums[:, block:]))
            for t, e, at, value in places:
                moments[t][j, e, at : at + 8] = value
            return tuple(behind)

        lax.fori_loop(0, turns, backward, (jnp.zeros((8, PIXELS), F32),) * GROUP)

        def settle(k, _):
            for t, e in spots:
                cx, cy = centre[t]
                s = place(t, PAIR * k + e)
                u = screen[s, 0:1] - cx
                v = screen[s, 1:2] - cy
                a, b, c = screen[s, 2:3], screen[s, 3:4], screen[s, 4:5]
                mxx, mxy, myy = (moments[t][k, e, j : j + 1] for j in (0, 1, 2))
                mx, my, m = (moments[t][k, e, j : j + 1] for j in (3, 4, 5))
                off_x = mx - u * m
                off_y = my - v * m
                changes = (
                    a * off_x + b * off_y,
                    b * off_x + c * off_y,
                    -0.5 * (mxx - u * (mx + off_x)),
                    -(mxy - u * my - v * off_x),
                    -0.5 * (myy - v * (my + off_y)),
                    m,
                    moments[t][k, e, 8:9],
                    moments[t][k, e, 9:10],
                    moments[t][k, e, 10:11],
                )
                for j, change in enumerate(changes):
                    grad_ref[s, j : j + 1] = grad_ref[s, j : j + 1] + change
            return 0

        lax.fori_loop(0, turns, settle, 0)
        return 0

    lax.fori_loop(0, tiles // GROUP, group, 0)


def deepest_first(pairs):
    live = jnp.sum((pairs >= 0).astype(jnp.int32), axis=1)
    row = jnp.arange(pairs.shape[0], dtype=jnp.int32)
    before = (live[None, :] > live[:, None]) | (
        (live[None, :] == live[:, None]) & (row[None, :] < row[:, None])
    )
    rank = jnp.sum(before.astype(jnp.int32), axis=1)
    return jnp.sum(jnp.where(rank[None, :] == row[:, None], row[None, :], 0), axis=1)


def blend(arrived, target, tile_place, pairs):
    tiles, channels, pixels = target.shape
    depth = pairs.shape[1]
    slots, rows, block = arrived.shape
    turns = pl.cdiv(depth, PAIR)
    pairs = jnp.pad(pairs, ((0, 0), (0, PAIR * turns - depth)), constant_values=-1)
    basis = jnp.asarray(pixel_basis())
    smem = pl.BlockSpec(memory_space=pltpu.SMEM)
    vmem = pl.BlockSpec(memory_space=pltpu.VMEM)
    image, grads = pl.pallas_call(
        blend_kernel,
        in_specs=[smem, smem, smem, vmem, vmem, vmem],
        out_specs=[vmem, vmem],
        scratch_shapes=[
            pltpu.VMEM((slots + 1, 16, block), F32),
            pltpu.VMEM((slots + 1, 16, 2 * block), BF16),
            pltpu.VMEM((slots + 1, 32, block), BF16),
            pltpu.VMEM((PAIR, GROUP, block, pixels), F32),
            pltpu.VMEM((PAIR, GROUP, block, pixels), F32),
            pltpu.VMEM((PAIR, GROUP, 2 * block, pixels), BF16),
            pltpu.VMEM((GROUP, 8, pixels), F32),
        ]
        + [pltpu.VMEM((turns, PAIR, 8, block), F32)] * GROUP
        + [pltpu.VMEM((turns, PAIR, block, pixels), F32)] * GROUP
        + [pltpu.VMEM((turns, PAIR, block, pixels), F32)] * GROUP
        + [pltpu.VMEM((turns, PAIR, 2 * block, pixels), BF16)] * GROUP
        + [pltpu.VMEM((turns, PAIR, 8, pixels), F32)] * GROUP
        + [pltpu.VMEM((turns, PAIR, 16, block), F32)] * GROUP,
        out_shape=[
            jax.ShapeDtypeStruct(target.shape, F32),
            jax.ShapeDtypeStruct((slots + 1, rows, block), F32),
        ],
        name="blend",
        compiler_params=pltpu.CompilerParams(),
    )(pairs, tile_place, deepest_first(pairs), basis, arrived, target)
    return image, grads[:slots]


def trade(payload):
    return lax.all_to_all(payload, ("gx", "gy"), split_axis=0, concat_axis=0, tiled=True)


def local(splats, moment_one, moment_two, target, tile_place, pairs, fetch):
    devices = lax.axis_size("gx") * lax.axis_size("gy")
    tiles_here = target.shape[0]
    width = 16.0 * TX
    height = 16.0 * (tiles_here * devices // TX)
    order = jnp.asarray(lane_order(splats.shape[2]))

    def project(raw):
        return jnp.dot(derive(raw, width, height), order, precision=lax.Precision.HIGHEST)

    asked = lax.all_to_all(fetch[0], ("gx", "gy"), split_axis=0, concat_axis=0, tiled=True)
    wanted = jnp.maximum(asked, 0)
    own_screen, own_pull = jax.vjp(project, splats)
    payload = own_screen[wanted]
    arrived = trade(payload)
    arrived = arrived.reshape((-1,) + payload.shape[2:])
    image, received_gradients = blend(arrived, target, tile_place, pairs)
    returned = trade(received_gradients.reshape(payload.shape))
    owner_pick = (asked.reshape(-1)[None, :] == jnp.arange(splats.shape[0])[:, None]).astype(
        jnp.float32
    )
    summed = jnp.dot(
        owner_pick, returned.reshape(owner_pick.shape[1], -1), precision=lax.Precision.HIGHEST
    )
    summed = summed.reshape((splats.shape[0],) + returned.shape[2:])
    (splat_grad,) = own_pull(summed)
    first = 0.9 * moment_one + 0.1 * splat_grad
    second_moment = 0.999 * moment_two + 0.001 * splat_grad * splat_grad
    adam_step = first / (jnp.sqrt(second_moment) + 1e-08)
    return (image, splat_grad, adam_step)


def solution(mesh):
    both = ("gx", "gy")
    return jax.shard_map(
        local,
        mesh=mesh,
        in_specs=(
            P(both, None, None),
            P(both, None, None),
            P(both, None, None),
            P(both, None, None),
            P(both),
            P(both, None),
            P(both, None, None),
        ),
        out_specs=(P(both, None, None), P(both, None, None), P(both, None, None)),
        check_vma=False,
    )
```

```python
import functools

import jax
import jax.numpy as jnp
import numpy as np
from jax import lax
from jax.experimental import pallas as pl
from jax.experimental.pallas import tpu as pltpu
from jax.sharding import PartitionSpec as P

TX = 16
SIDE = 16
PIXELS = SIDE * SIDE
LOG2E = 1.4426950408889634
DEAD = -1.0e4
GROUP = 4
PAIR = 2
F32 = jnp.float32
BF16 = jnp.bfloat16


HARMONIC_ZERO = 0.28209479177387814
HARMONIC_ONE = 0.4886025119029199
HARMONIC_TWO = (
    1.0925484305920792,
    -1.0925484305920792,
    0.31539156525252005,
    -1.0925484305920792,
    0.5462742152960396,
)
HARMONIC_THREE = (
    -0.5900435899266435,
    2.890611442640554,
    -0.4570457994644658,
    0.3731763325901154,
    -0.4570457994644658,
    1.445305721320277,
    -0.5900435899266435,
)


def harmonic_terms(east, north, ahead):
    east_east = east * east
    north_north = north * north
    ahead_ahead = ahead * ahead
    return [
        jnp.full_like(east, HARMONIC_ZERO),
        -HARMONIC_ONE * north,
        HARMONIC_ONE * ahead,
        -HARMONIC_ONE * east,
        HARMONIC_TWO[0] * east * north,
        HARMONIC_TWO[1] * north * ahead,
        HARMONIC_TWO[2] * (2.0 * ahead_ahead - east_east - north_north),
        HARMONIC_TWO[3] * east * ahead,
        HARMONIC_TWO[4] * (east_east - north_north),
        HARMONIC_THREE[0] * north * (3.0 * east_east - north_north),
        HARMONIC_THREE[1] * east * north * ahead,
        HARMONIC_THREE[2] * north * (4.0 * ahead_ahead - east_east - north_north),
        HARMONIC_THREE[3] * ahead * (2.0 * ahead_ahead - 3.0 * east_east - 3.0 * north_north),
        HARMONIC_THREE[4] * east * (4.0 * ahead_ahead - east_east - north_north),
        HARMONIC_THREE[5] * ahead * (east_east - north_north),
        HARMONIC_THREE[6] * east * (east_east - 3.0 * north_north),
    ]


def harmonics(east, north, ahead):
    return jnp.stack(harmonic_terms(east, north, ahead), axis=1)


def derive(raw, width, height):
    place_x = raw[:, 0]
    place_y = raw[:, 1]
    place_z = raw[:, 2]
    screen_u = width * place_x / place_z + 0.5 * width
    screen_v = width * place_y / place_z + 0.5 * height
    inverse_one = jnp.exp(-2.0 * raw[:, 3])
    inverse_two = jnp.exp(-2.0 * raw[:, 4])
    cosine = jnp.cos(raw[:, 5])
    sine = jnp.sin(raw[:, 5])
    conic_a = cosine * cosine * inverse_one + sine * sine * inverse_two
    conic_b = cosine * sine * (inverse_one - inverse_two)
    conic_c = sine * sine * inverse_one + cosine * cosine * inverse_two
    log_opacity = jax.nn.log_sigmoid(raw[:, 6])
    length = jnp.sqrt(place_x * place_x + place_y * place_y + place_z * place_z)
    basis = harmonics(place_x / length, place_y / length, place_z / length)
    coeffs = raw[:, 7:].reshape(raw.shape[0], 3, 16, raw.shape[2])
    colors = 0.5 + jnp.sum(coeffs * basis[:, None], axis=2)
    head = jnp.stack([screen_u, screen_v, conic_a, conic_b, conic_c, log_opacity], axis=1)
    return jnp.concatenate([head, colors], axis=1)


def pixel_basis():
    j = np.arange(PIXELS)
    x = j % SIDE + 0.5 - SIDE / 2
    y = j // SIDE + 0.5 - SIDE / 2
    rows = np.stack([x * x, x * y, y * y, x, y, np.ones_like(x), 0 * x, 0 * x])
    return np.concatenate([rows, rows, rows, 0 * rows]).astype(np.float32)


def lane_order(block):
    row = np.arange(block)
    splat = (row % 8) * (block // 8) + row // 8
    return (np.arange(block)[:, None] == splat[None, :]).astype(np.float32)


def rounded(x):
    return x.astype(BF16).astype(F32)


def shifted(x, shift):
    return pltpu.roll(x, shift % 8, 0)


def blend_kernel(
    cap, pairs_ref, place_ref, order_ref, basis_ref, arrived_ref, target_ref, image_ref, grad_ref,
    screen, hue_sum, hue_back, alphas, slopes, steps, resid, *banks,
):
    depth, tiles = pairs_ref.shape
    slots = cap * arrived_ref.shape[0]
    block = arrived_ref.shape[2]
    chunks = block // 8
    lanes = range(GROUP)
    spots = [(t, e) for e in range(PAIR) for t in lanes]
    parts, keeps, weights, halves, ends, moments = (
        banks[GROUP * i : GROUP * i + GROUP] for i in range(6)
    )
    sub = lax.broadcasted_iota(jnp.int32, (8, PIXELS), 0)

    resid[...] = jnp.zeros_like(resid)
    for t in lanes:
        parts[t][...] = jnp.zeros_like(parts[t])

    def prepare(o, _):
        grad_ref[o] = jnp.zeros(grad_ref.shape[1:], F32)
        for i in range(cap):
            s = cap * o + i
            last = arrived_ref[o, 8 * cap + i : 8 * cap + i + 1]
            screen[s, 0:8] = arrived_ref[o, 8 * i : 8 * i + 8]
            screen[s, 8:9] = last
            hue = jnp.concatenate(
                [arrived_ref[o, 8 * i + 6 : 8 * i + 8], last, jnp.zeros((5, block), F32)], axis=0
            )
            hue1 = rounded(hue)
            hue2 = hue - hue1
            zero = jnp.zeros_like(hue)
            hue_sum[s] = jnp.concatenate(
                [
                    jnp.concatenate([hue1, hue1], axis=1),
                    jnp.concatenate([hue2, zero], axis=1),
                ],
                axis=0,
            ).astype(BF16)
            hue_back[s] = jnp.concatenate([hue1, hue2, hue1, zero], axis=0).astype(BF16)
        return 0

    lax.fori_loop(0, arrived_ref.shape[0], prepare, 0)
    grad_ref[arrived_ref.shape[0]] = jnp.zeros(grad_ref.shape[1:], F32)
    screen[slots] = jnp.zeros((16, block), F32)
    screen[slots, 5:6] = jnp.full((1, block), DEAD, F32)
    hue_sum[slots] = jnp.zeros((16, 2 * block), BF16)
    hue_back[slots] = jnp.zeros((32, block), BF16)

    basis = basis_ref[...].astype(BF16)
    monomials = basis_ref[0:8].astype(BF16)
    zero_row = jnp.zeros((8, PIXELS), F32)

    def group(step, _):
        row = [order_ref[0, step * GROUP + t] for t in lanes]
        deepest = jnp.int32(0)
        for k in range(depth):
            deepest = deepest + (pairs_ref[k, row[0]] >= 0).astype(jnp.int32)
        turns = lax.div(deepest + (PAIR - 1), PAIR)
        centre = []
        for t in lanes:
            tile = place_ref[row[t]]
            cx = (lax.rem(tile, TX) * SIDE + SIDE // 2).astype(F32)
            cy = (lax.div(tile, TX) * SIDE + SIDE // 2).astype(F32)
            centre.append((cx, cy))

        def place(t, k):
            slot = pairs_ref[k, row[t]]
            return jnp.where(slot >= 0, slot, slots)

        def shape_up(k, _):
            for t, e in spots:
                cx, cy = centre[t]
                s = place(t, PAIR * k + e)
                u = screen[s, 0:1] - cx
                v = screen[s, 1:2] - cy
                a, b, c = screen[s, 2:3], screen[s, 3:4], screen[s, 4:5]
                opac = jnp.maximum(screen[s, 5:6], DEAD)
                lin_x = a * u + b * v
                lin_y = b * u + c * v
                const = opac - 0.5 * (lin_x * u + lin_y * v)
                for j, value in enumerate((-0.5 * a, -b, -0.5 * c, lin_x, lin_y, const)):
                    parts[t][k, e, j : j + 1] = LOG2E * value
            return 0

        lax.fori_loop(0, turns, shape_up, 0)

        def power_of(t, j, e):
            c = parts[t][j, e]
            c1 = rounded(c)
            c2 = rounded(c - c1)
            c3 = c - c1 - c2
            left = jnp.concatenate([c1, c2, c3, jnp.zeros_like(c)], axis=0).astype(BF16)
            return lax.dot_general(
                left, basis, (((0,), (0,)), ((), ())), preferred_element_type=F32
            )

        def draw(t, j, e, power):
            alpha = jnp.exp2(power)
            alphas[e, t] = alpha
            keep = 1.0 - alpha
            keeps[t][j, e] = keep
            kept = keep[0:8]
            for i in range(1, chunks):
                kept = kept * keep[8 * i : 8 * i + 8]
            return kept

        def scan_of(t, j, e, kept, trans):
            scan = jnp.where(sub == 0, trans, shifted(kept, 1))
            for d in (1, 2, 4):
                scan = scan * jnp.where(sub < d, 1.0, shifted(scan, d))
            end = scan * kept
            ends[t][j, e] = end
            return scan, jnp.broadcast_to(end[7:8], (8, PIXELS))

        def spread(t, j, e, here):
            for i in range(0, chunks, 2):
                lo, mid, hi = 8 * i, 8 * i + 8, 8 * i + 16
                one = alphas[e, t, lo:mid] * here
                here = here * keeps[t][j, e, lo:mid]
                two = alphas[e, t, mid:hi] * here
                here = here * keeps[t][j, e, mid:hi]
                pair = jnp.concatenate([one, two], axis=0)
                weights[t][j, e, lo:hi] = pair
                high = pair.astype(BF16)
                halves[t][j, e, lo:hi] = high
                halves[t][j, e, block + lo : block + hi] = (pair - high.astype(F32)).astype(BF16)

        def summed(t, j, e):
            return jnp.dot(
                hue_sum[place(t, PAIR * j + e)], halves[t][j, e], preferred_element_type=F32
            )

        def forward(j, carry):
            trans = [carry[2 * t] for t in lanes]
            totals = [carry[2 * t + 1] for t in lanes]
            powers = [[power_of(t, j, e) for t in lanes] for e in range(PAIR)]
            kepts = [draw(t, j, 0, powers[0][t]) for t in lanes]
            for e in range(PAIR):
                heres = []
                for t in lanes:
                    here, trans[t] = scan_of(t, j, e, kepts[t], trans[t])
                    heres.append(here)
                for t in lanes:
                    spread(t, j, e, heres[t])
                    if e + 1 < PAIR:
                        kepts[t] = draw(t, j, e + 1, powers[e + 1][t])
                totals = [totals[t] + summed(t, j, e) for t in lanes]
            return tuple(x for t in lanes for x in (trans[t], totals[t]))

        start = (jnp.ones((8, PIXELS), F32), jnp.zeros((16, PIXELS), F32)) * GROUP
        done = lax.fori_loop(0, turns, forward, start)

        pulls = []
        for t in lanes:
            total = done[2 * t + 1]
            image = (total[0:8] + total[8:16])[0:3]
            for h in range(3):
                image_ref[h, pl.ds(row[t], 1)] = image[h : h + 1]
                resid[t, h : h + 1] = (image[h : h + 1] - target_ref[h, pl.ds(row[t], 1)]) * (
                    2.0 / 512.0
                )
            g = resid[t]
            g1 = rounded(g)
            g2 = g - g1
            pulls.append(
                (
                    jnp.concatenate([g1, g1, g2, zero_row], axis=0).astype(BF16),
                    jnp.concatenate([g1, g2], axis=0).astype(BF16),
                )
            )

        def lean(t, j, e):
            slopes[e, t] = lax.dot_general(
                hue_back[place(t, PAIR * j + e)],
                pulls[t][0],
                (((0,), (0,)), ((), ())),
                preferred_element_type=F32,
            )

        def behind_of(t, j, e, behind):
            run = weights[t][j, e, 0:8] * slopes[e, t, 0:8]
            for i in range(1, chunks):
                lo, hi = 8 * i, 8 * i + 8
                run = run + weights[t][j, e, lo:hi] * slopes[e, t, lo:hi]
            scan = jnp.where(sub == 7, behind, shifted(run, -1))
            for d in (1, 2, 4):
                scan = scan + jnp.where(sub < 8 - d, shifted(scan, -d), 0.0)
            return (
                scan / jnp.maximum(ends[t][j, e], 1e-37),
                jnp.broadcast_to((run + scan)[0:1], (8, PIXELS)),
            )

        def step_of(t, j, e, here):
            for i in range(chunks - 2, -1, -2):
                lo, mid, hi = 8 * i, 8 * i + 8, 8 * i + 16
                ahead = slopes[e, t, mid:hi]
                gap = ahead - here
                two = weights[t][j, e, mid:hi] * gap
                here = ahead - keeps[t][j, e, mid:hi] * gap
                ahead = slopes[e, t, lo:mid]
                gap = ahead - here
                one = weights[t][j, e, lo:mid] * gap
                here = ahead - keeps[t][j, e, lo:mid] * gap
                pair = jnp.concatenate([one, two], axis=0)
                high = pair.astype(BF16)
                steps[e, t, lo:hi] = high
                steps[e, t, block + lo : block + hi] = (pair - high.astype(F32)).astype(BF16)

        def backward(index, carry):
            j = turns - 1 - index
            behind = list(carry)
            places = []
            for e in reversed(range(PAIR)):
                for t in lanes:
                    lean(t, j, e)
            for e in reversed(range(PAIR)):
                for t in lanes:
                    hues = lax.dot_general(
                        pulls[t][1], halves[t][j, e], (((1,), (1,)), ((), ())),
                        preferred_element_type=F32,
                    )
                    places.append(
                        (t, e, 8, hues[0:8, 0:block] + hues[0:8, block:] + hues[8:16, 0:block])
                    )
                heres = []
                for t in lanes:
                    here, behind[t] = behind_of(t, j, e, behind[t])
                    heres.append(here)
                for t in lanes:
                    step_of(t, j, e, heres[t])
                for t in lanes:
                    sums = lax.dot_general(
                        monomials, steps[e, t], (((1,), (1,)), ((), ())), preferred_element_type=F32
                    )
                    places.append((t, e, 0, sums[:, 0:block] + sums[:, block:]))
            for t, e, at, value in places:
                moments[t][j, e, at : at + 8] = value
            return tuple(behind)

        lax.fori_loop(0, turns, backward, (jnp.zeros((8, PIXELS), F32),) * GROUP)

        def settle(k, _):
            for t, e in spots:
                cx, cy = centre[t]
                s = place(t, PAIR * k + e)
                u = screen[s, 0:1] - cx
                v = screen[s, 1:2] - cy
                a, b, c = screen[s, 2:3], screen[s, 3:4], screen[s, 4:5]
                mxx, mxy, myy = (moments[t][k, e, j : j + 1] for j in (0, 1, 2))
                mx, my, m = (moments[t][k, e, j : j + 1] for j in (3, 4, 5))
                off_x = mx - u * m
                off_y = my - v * m
                changes = (
                    a * off_x + b * off_y,
                    b * off_x + c * off_y,
                    -0.5 * (mxx - u * (mx + off_x)),
                    -(mxy - u * my - v * off_x),
                    -0.5 * (myy - v * (my + off_y)),
                    m,
                    moments[t][k, e, 8:9],
                    moments[t][k, e, 9:10],
                    moments[t][k, e, 10:11],
                )
                owner, i = lax.div(s, cap), lax.rem(s, cap)
                for j, change in enumerate(changes):
                    at = pl.ds(8 * i + j if j < 8 else 8 * cap + i, 1)
                    grad_ref[owner, at] = grad_ref[owner, at] + change
            return 0

        lax.fori_loop(0, turns, settle, 0)
        return 0

    lax.fori_loop(0, tiles // GROUP, group, 0)


def blend(arrived, cap, target, tile_place, pairs, order):
    channels, tiles, pixels = target.shape
    depth = pairs.shape[0]
    devices, rows, block = arrived.shape
    slots = devices * cap
    turns = pl.cdiv(depth, PAIR)
    if depth % PAIR:
        pairs = jnp.pad(pairs, ((0, PAIR * turns - depth), (0, 0)), constant_values=-1)
    basis = jnp.asarray(pixel_basis())
    smem = pl.BlockSpec(memory_space=pltpu.SMEM)
    vmem = pl.BlockSpec(memory_space=pltpu.VMEM)
    return pl.pallas_call(
        functools.partial(blend_kernel, cap),
        in_specs=[smem, smem, smem, vmem, vmem, vmem],
        out_specs=[vmem, vmem],
        scratch_shapes=[
            pltpu.VMEM((slots + 1, 16, block), F32),
            pltpu.VMEM((slots + 1, 16, 2 * block), BF16),
            pltpu.VMEM((slots + 1, 32, block), BF16),
            pltpu.VMEM((PAIR, GROUP, block, pixels), F32),
            pltpu.VMEM((PAIR, GROUP, block, pixels), F32),
            pltpu.VMEM((PAIR, GROUP, 2 * block, pixels), BF16),
            pltpu.VMEM((GROUP, 8, pixels), F32),
        ]
        + [pltpu.VMEM((turns, PAIR, 8, block), F32)] * GROUP
        + [pltpu.VMEM((turns, PAIR, block, pixels), F32)] * GROUP
        + [pltpu.VMEM((turns, PAIR, block, pixels), F32)] * GROUP
        + [pltpu.VMEM((turns, PAIR, 2 * block, pixels), BF16)] * GROUP
        + [pltpu.VMEM((turns, PAIR, 8, pixels), F32)] * GROUP
        + [pltpu.VMEM((turns, PAIR, 16, block), F32)] * GROUP,
        out_shape=[
            jax.ShapeDtypeStruct(target.shape, F32),
            jax.ShapeDtypeStruct((devices + 1, rows, block), F32),
        ],
        name="blend",
        compiler_params=pltpu.CompilerParams(),
    )(pairs, tile_place, order, basis, arrived, target)


def whereabouts(sizes):
    nx, ny = sizes
    me = lax.axis_index("gx") * ny + lax.axis_index("gy")

    def other(n):
        o = lax.rem(me + n, nx * ny)
        return o, (lax.div(o, ny), lax.rem(o, ny))

    return me, nx * ny, other


def greet(devices, other):
    barrier = pltpu.get_barrier_semaphore()

    def call(n, _):
        pl.semaphore_signal(
            barrier, inc=1, device_id=other(n)[1], device_id_type=pl.DeviceIdType.MESH
        )
        return 0

    lax.fori_loop(1, devices, call, 0)
    return barrier


def post(source, target, sems, where):
    return pltpu.make_async_remote_copy(
        src_ref=source,
        dst_ref=target,
        send_sem=sems.at[0],
        recv_sem=sems.at[1],
        device_id=where,
        device_id_type=pl.DeviceIdType.MESH,
    )


def order_rows(pairs, order_ref):
    depth, tiles = pairs.shape
    live = jnp.sum((pairs >= 0).astype(F32), axis=0, keepdims=True)
    across = lax.broadcasted_iota(jnp.int32, (tiles, tiles), 1).astype(F32)
    down = lax.broadcasted_iota(jnp.int32, (tiles, tiles), 0).astype(F32)
    theirs = jnp.broadcast_to(live, (tiles, tiles))
    mine = jnp.sum(jnp.where(across == down, theirs, 0.0), axis=1, keepdims=True)
    before = (theirs > mine) | ((theirs == mine) & (across < down))
    rank = jnp.sum(before.astype(F32), axis=1, keepdims=True)
    order = jnp.sum(jnp.where(rank == across, down, 0.0), axis=0, keepdims=True)
    order_ref[...] = order.astype(jnp.int32)


def fetch_kernel(
    sizes, width, height, splats_ref, fetch_ref, pairs_ref, order_ref, arrived_ref, rows_ref, asked,
    own, send, ask, heard, ask_sems, sems, local_sem,
):
    me, devices, other = whereabouts(sizes)
    cap = fetch_ref.shape[0]
    blocks, _, block = own.shape
    used = 9 * cap
    barrier = greet(devices, other)

    order_rows(pairs_ref[...], rows_ref)
    table = jnp.concatenate([fetch_ref[...], jnp.zeros((8 - cap, devices), jnp.int32)], axis=0)
    if devices % 128:
        table = jnp.concatenate(
            [table, jnp.zeros((8, 128 - devices % 128), jnp.int32)], axis=1
        )
    table = jnp.transpose(table.astype(F32))[0:devices]
    ask[...] = jnp.zeros_like(ask)
    ask[:, :, 0:8] = table.astype(jnp.int32).reshape(devices, 1, 8)

    raw = splats_ref
    place_x, place_y, place_z = raw[0], raw[1], raw[2]
    inverse_one = jnp.exp(-2.0 * raw[3])
    inverse_two = jnp.exp(-2.0 * raw[4])
    cosine = jnp.cos(raw[5])
    sine = jnp.sin(raw[5])
    length = jnp.sqrt(place_x * place_x + place_y * place_y + place_z * place_z)
    terms = harmonic_terms(place_x / length, place_y / length, place_z / length)
    lines = [
        width * place_x / place_z + 0.5 * width,
        width * place_y / place_z + 0.5 * height,
        cosine * cosine * inverse_one + sine * sine * inverse_two,
        cosine * sine * (inverse_one - inverse_two),
        sine * sine * inverse_one + cosine * cosine * inverse_two,
        jnp.minimum(raw[6], 0.0) - jnp.log1p(jnp.exp(-jnp.abs(raw[6]))),
    ]
    for h in range(3):
        color = jnp.full((blocks, block), 0.5, F32)
        for k in range(16):
            color = color + raw[7 + 16 * h + k] * terms[k]
        lines.append(color)
    order = order_ref[...].astype(BF16)
    for j, line in enumerate(lines):
        one = rounded(line)
        two = rounded(line - one)
        three = line - one - two
        stack = jnp.concatenate([one, two, three], axis=0).astype(BF16)
        mixed = jnp.dot(stack, order, preferred_element_type=F32)
        mixed = mixed[0:blocks] + mixed[blocks : 2 * blocks] + mixed[2 * blocks :]
        own[:, j, :] = mixed

    pl.semaphore_wait(barrier, devices - 1)

    def inquire(n, _):
        o, where = other(n)
        post(ask.at[o], asked.at[me], ask_sems, where).start()
        return 0

    lax.fori_loop(1, devices, inquire, 0)
    keep = pltpu.make_async_copy(ask.at[me], asked.at[me], local_sem)
    keep.start()
    keep.wait()
    rest = pl.ds(0, devices - 1)
    bulk = post(ask.at[rest], asked.at[rest], ask_sems, other(1)[1])
    bulk.wait_recv()
    load = pltpu.make_async_copy(asked, heard, local_sem)
    load.start()
    load.wait()

    def pick(o, target):
        for i in range(cap):
            b = jnp.clip(heard[o, 0, i], 0, blocks - 1)
            target[o, 8 * i : 8 * i + 8] = own[b, 0:8]
            target[o, 8 * cap + i : 8 * cap + i + 1] = own[b, 8:9]

    def fill(n, _):
        pick(other(n)[0], send)
        return 0

    lax.fori_loop(1, devices, fill, 0)
    pick(me, arrived_ref)
    part = pl.ds(0, used)

    def serve(n, _):
        o, where = other(n)
        post(send.at[o, part], arrived_ref.at[me, part], sems, where).start()
        return 0

    lax.fori_loop(1, devices, serve, 0)
    bulk.wait_send()
    whole = post(send.at[rest, part], arrived_ref.at[rest, part], sems, other(1)[1])
    whole.wait_recv()
    whole.wait_send()


def fetch_blocks(splats, fetch, pairs, sizes, width, height):
    _, blocks, block = splats.shape
    cap, devices = fetch.shape
    rows = 8 * pl.cdiv(9 * cap, 8)
    order = jnp.asarray(lane_order(block))
    vmem = pl.BlockSpec(memory_space=pltpu.VMEM)
    return pl.pallas_call(
        functools.partial(fetch_kernel, sizes, width, height),
        in_specs=[vmem] * 4,
        out_specs=[vmem] * 3,
        scratch_shapes=[
            pltpu.VMEM((blocks, 16, block), F32),
            pltpu.VMEM((devices, rows, block), F32),
            pltpu.VMEM((devices, 1, 128), jnp.int32),
            pltpu.SMEM((devices, 1, 128), jnp.int32),
            pltpu.SemaphoreType.DMA((2,)),
            pltpu.SemaphoreType.DMA((2,)),
            pltpu.SemaphoreType.DMA,
        ],
        out_shape=[
            jax.ShapeDtypeStruct((devices, rows, block), F32),
            jax.ShapeDtypeStruct((1, pairs.shape[1]), jnp.int32),
            jax.ShapeDtypeStruct((devices, 1, 128), jnp.int32),
        ],
        name="fetch",
        compiler_params=pltpu.CompilerParams(collective_id=0, has_side_effects=True),
    )(splats, fetch, pairs, order)


def return_kernel(sizes, used, grad_ref, returned_ref, sems):
    me, devices, other = whereabouts(sizes)
    barrier = greet(devices, other)
    returned_ref[me] = grad_ref[me]
    pl.semaphore_wait(barrier, devices - 1)
    part = pl.ds(0, used)

    def serve(n, _):
        o, where = other(n)
        post(grad_ref.at[o, part], returned_ref.at[me, part], sems, where).start()
        return 0

    lax.fori_loop(1, devices, serve, 0)
    rest = pl.ds(0, devices - 1)
    whole = post(grad_ref.at[rest, part], returned_ref.at[rest, part], sems, other(1)[1])
    whole.wait_recv()
    whole.wait_send()


def return_grads(grads, used, sizes):
    more, rows, block = grads.shape
    vmem = pl.BlockSpec(memory_space=pltpu.VMEM)
    return pl.pallas_call(
        functools.partial(return_kernel, sizes, used),
        in_specs=[vmem],
        out_specs=vmem,
        scratch_shapes=[pltpu.SemaphoreType.DMA((2,))],
        out_shape=jax.ShapeDtypeStruct((more - 1, rows, block), F32),
        name="give_back",
        compiler_params=pltpu.CompilerParams(collective_id=1, has_side_effects=True),
    )(grads)


def local(splats, moment_one, moment_two, target, tile_place, pairs, fetch):
    sizes = (lax.axis_size("gx"), lax.axis_size("gy"))
    devices = sizes[0] * sizes[1]
    tiles_here = target.shape[0]
    cap = fetch.shape[2]
    width = 16.0 * TX
    height = 16.0 * (tiles_here * devices // TX)
    order = jnp.asarray(lane_order(splats.shape[2]))

    def project(raw):
        return jnp.dot(derive(raw, width, height), order, precision=lax.Precision.HIGHEST)

    rows_first = jnp.transpose(splats, (1, 0, 2))
    asks = jnp.transpose(fetch[0])
    lists = jnp.transpose(pairs)
    arrived, rows, asked = fetch_blocks(rows_first, asks, lists, sizes, width, height)
    image, grads = blend(
        arrived, cap, jnp.transpose(target, (1, 0, 2)), tile_place, lists, rows
    )
    returned = return_grads(grads, 9 * cap, sizes)
    _, own_pull = jax.vjp(project, splats)
    picks = [
        (asked[:, 0, i][None, :] == jnp.arange(splats.shape[0])[:, None]).astype(F32)
        for i in range(cap)
    ]
    summed = 0.0
    for i in range(cap):
        both = jnp.concatenate(
            [returned[:, 8 * i : 8 * i + 8], returned[:, 8 * cap + i : 8 * cap + i + 1]], axis=1
        )
        summed = summed + jnp.einsum(
            "bd,drs->brs", picks[i], both, precision=lax.Precision.HIGHEST
        )
    (splat_grad,) = own_pull(summed)
    first = 0.9 * moment_one + 0.1 * splat_grad
    second_moment = 0.999 * moment_two + 0.001 * splat_grad * splat_grad
    adam_step = first / (jnp.sqrt(second_moment) + 1e-08)
    return (jnp.transpose(image, (1, 0, 2)), splat_grad, adam_step)


def solution(mesh):
    both = ("gx", "gy")
    return jax.shard_map(
        local,
        mesh=mesh,
        in_specs=(
            P(both, None, None),
            P(both, None, None),
            P(both, None, None),
            P(both, None, None),
            P(both),
            P(both, None),
            P(both, None, None),
        ),
        out_specs=(P(both, None, None), P(both, None, None), P(both, None, None)),
        check_vma=False,
    )
```

```python
import functools

import jax
import jax.numpy as jnp
import numpy as np
from jax import lax
from jax.experimental import pallas as pl
from jax.experimental.pallas import tpu as pltpu
from jax.sharding import PartitionSpec as P

TX = 16
SIDE = 16
PIXELS = SIDE * SIDE
LOG2E = 1.4426950408889634
DEAD = -1.0e4
GROUP = 4
PAIR = 2
F32 = jnp.float32
BF16 = jnp.bfloat16


HARMONIC_ZERO = 0.28209479177387814
HARMONIC_ONE = 0.4886025119029199
HARMONIC_TWO = (
    1.0925484305920792,
    -1.0925484305920792,
    0.31539156525252005,
    -1.0925484305920792,
    0.5462742152960396,
)
HARMONIC_THREE = (
    -0.5900435899266435,
    2.890611442640554,
    -0.4570457994644658,
    0.3731763325901154,
    -0.4570457994644658,
    1.445305721320277,
    -0.5900435899266435,
)


def harmonic_terms(east, north, ahead):
    east_east = east * east
    north_north = north * north
    ahead_ahead = ahead * ahead
    return [
        jnp.full_like(east, HARMONIC_ZERO),
        -HARMONIC_ONE * north,
        HARMONIC_ONE * ahead,
        -HARMONIC_ONE * east,
        HARMONIC_TWO[0] * east * north,
        HARMONIC_TWO[1] * north * ahead,
        HARMONIC_TWO[2] * (2.0 * ahead_ahead - east_east - north_north),
        HARMONIC_TWO[3] * east * ahead,
        HARMONIC_TWO[4] * (east_east - north_north),
        HARMONIC_THREE[0] * north * (3.0 * east_east - north_north),
        HARMONIC_THREE[1] * east * north * ahead,
        HARMONIC_THREE[2] * north * (4.0 * ahead_ahead - east_east - north_north),
        HARMONIC_THREE[3] * ahead * (2.0 * ahead_ahead - 3.0 * east_east - 3.0 * north_north),
        HARMONIC_THREE[4] * east * (4.0 * ahead_ahead - east_east - north_north),
        HARMONIC_THREE[5] * ahead * (east_east - north_north),
        HARMONIC_THREE[6] * east * (east_east - 3.0 * north_north),
    ]


def pixel_basis():
    j = np.arange(PIXELS)
    x = j % SIDE + 0.5 - SIDE / 2
    y = j // SIDE + 0.5 - SIDE / 2
    rows = np.stack([x * x, x * y, y * y, x, y, np.ones_like(x), 0 * x, 0 * x])
    return np.concatenate([rows, rows, rows, 0 * rows]).astype(np.float32)


def lane_order(block):
    row = np.arange(block)
    splat = (row % 8) * (block // 8) + row // 8
    return (np.arange(block)[:, None] == splat[None, :]).astype(np.float32)


def rounded(x):
    return x.astype(BF16).astype(F32)


def shifted(x, shift):
    return pltpu.roll(x, shift % 8, 0)


def blend_kernel(
    cap, pairs_ref, place_ref, order_ref, basis_ref, arrived_ref, target_ref, image_ref, grad_ref,
    screen, hue_sum, hue_back, alphas, slopes, steps, resid, *banks,
):
    depth, tiles = pairs_ref.shape
    slots = cap * arrived_ref.shape[0]
    block = arrived_ref.shape[2]
    chunks = block // 8
    lanes = range(GROUP)
    spots = [(t, e) for e in range(PAIR) for t in lanes]
    parts, keeps, weights, halves, ends, moments = (
        banks[GROUP * i : GROUP * i + GROUP] for i in range(6)
    )
    sub = lax.broadcasted_iota(jnp.int32, (8, PIXELS), 0)

    resid[...] = jnp.zeros_like(resid)
    for t in lanes:
        parts[t][...] = jnp.zeros_like(parts[t])

    def prepare(o, _):
        grad_ref[o] = jnp.zeros(grad_ref.shape[1:], F32)
        for i in range(cap):
            s = cap * o + i
            last = arrived_ref[o, 8 * cap + i : 8 * cap + i + 1]
            screen[s, 0:8] = arrived_ref[o, 8 * i : 8 * i + 8]
            screen[s, 8:9] = last
            hue = jnp.concatenate(
                [arrived_ref[o, 8 * i + 6 : 8 * i + 8], last, jnp.zeros((5, block), F32)], axis=0
            )
            hue1 = rounded(hue)
            hue2 = hue - hue1
            zero = jnp.zeros_like(hue)
            hue_sum[s] = jnp.concatenate(
                [
                    jnp.concatenate([hue1, hue1], axis=1),
                    jnp.concatenate([hue2, zero], axis=1),
                ],
                axis=0,
            ).astype(BF16)
            hue_back[s] = jnp.concatenate([hue1, hue2, hue1, zero], axis=0).astype(BF16)
        return 0

    lax.fori_loop(0, arrived_ref.shape[0], prepare, 0)
    grad_ref[arrived_ref.shape[0]] = jnp.zeros(grad_ref.shape[1:], F32)
    screen[slots] = jnp.zeros((16, block), F32)
    screen[slots, 5:6] = jnp.full((1, block), DEAD, F32)
    hue_sum[slots] = jnp.zeros((16, 2 * block), BF16)
    hue_back[slots] = jnp.zeros((32, block), BF16)

    basis = basis_ref[...].astype(BF16)
    monomials = basis_ref[0:8].astype(BF16)
    zero_row = jnp.zeros((8, PIXELS), F32)

    def group(step, _):
        row = [order_ref[0, step * GROUP + t] for t in lanes]
        deepest = jnp.int32(0)
        for k in range(depth):
            deepest = deepest + (pairs_ref[k, row[0]] >= 0).astype(jnp.int32)
        turns = lax.div(deepest + (PAIR - 1), PAIR)
        centre = []
        for t in lanes:
            tile = place_ref[row[t]]
            cx = (lax.rem(tile, TX) * SIDE + SIDE // 2).astype(F32)
            cy = (lax.div(tile, TX) * SIDE + SIDE // 2).astype(F32)
            centre.append((cx, cy))

        def place(t, k):
            slot = pairs_ref[k, row[t]]
            return jnp.where(slot >= 0, slot, slots)

        def shape_up(k, _):
            for t, e in spots:
                cx, cy = centre[t]
                s = place(t, PAIR * k + e)
                u = screen[s, 0:1] - cx
                v = screen[s, 1:2] - cy
                a, b, c = screen[s, 2:3], screen[s, 3:4], screen[s, 4:5]
                opac = jnp.maximum(screen[s, 5:6], DEAD)
                lin_x = a * u + b * v
                lin_y = b * u + c * v
                const = opac - 0.5 * (lin_x * u + lin_y * v)
                for j, value in enumerate((-0.5 * a, -b, -0.5 * c, lin_x, lin_y, const)):
                    parts[t][k, e, j : j + 1] = LOG2E * value
            return 0

        lax.fori_loop(0, turns, shape_up, 0)

        def power_of(t, j, e):
            c = parts[t][j, e]
            c1 = rounded(c)
            c2 = rounded(c - c1)
            c3 = c - c1 - c2
            left = jnp.concatenate([c1, c2, c3, jnp.zeros_like(c)], axis=0).astype(BF16)
            return lax.dot_general(
                left, basis, (((0,), (0,)), ((), ())), preferred_element_type=F32
            )

        def draw(t, j, e, power):
            alpha = jnp.exp2(power)
            alphas[e, t] = alpha
            keep = 1.0 - alpha
            keeps[t][j, e] = keep
            kept = keep[0:8]
            for i in range(1, chunks):
                kept = kept * keep[8 * i : 8 * i + 8]
            return kept

        def scan_of(t, j, e, kept, trans):
            scan = jnp.where(sub == 0, trans, shifted(kept, 1))
            for d in (1, 2, 4):
                scan = scan * jnp.where(sub < d, 1.0, shifted(scan, d))
            end = scan * kept
            ends[t][j, e] = end
            return scan, jnp.broadcast_to(end[7:8], (8, PIXELS))

        def spread(t, j, e, here):
            for i in range(0, chunks, 2):
                lo, mid, hi = 8 * i, 8 * i + 8, 8 * i + 16
                one = alphas[e, t, lo:mid] * here
                here = here * keeps[t][j, e, lo:mid]
                two = alphas[e, t, mid:hi] * here
                here = here * keeps[t][j, e, mid:hi]
                pair = jnp.concatenate([one, two], axis=0)
                weights[t][j, e, lo:hi] = pair
                high = pair.astype(BF16)
                halves[t][j, e, lo:hi] = high
                halves[t][j, e, block + lo : block + hi] = (pair - high.astype(F32)).astype(BF16)

        def summed(t, j, e):
            return jnp.dot(
                hue_sum[place(t, PAIR * j + e)], halves[t][j, e], preferred_element_type=F32
            )

        def forward(j, carry):
            trans = [carry[2 * t] for t in lanes]
            totals = [carry[2 * t + 1] for t in lanes]
            powers = [[power_of(t, j, e) for t in lanes] for e in range(PAIR)]
            kepts = [draw(t, j, 0, powers[0][t]) for t in lanes]
            for e in range(PAIR):
                heres = []
                for t in lanes:
                    here, trans[t] = scan_of(t, j, e, kepts[t], trans[t])
                    heres.append(here)
                for t in lanes:
                    spread(t, j, e, heres[t])
                    if e + 1 < PAIR:
                        kepts[t] = draw(t, j, e + 1, powers[e + 1][t])
                totals = [totals[t] + summed(t, j, e) for t in lanes]
            return tuple(x for t in lanes for x in (trans[t], totals[t]))

        start = (jnp.ones((8, PIXELS), F32), jnp.zeros((16, PIXELS), F32)) * GROUP
        done = lax.fori_loop(0, turns, forward, start)

        pulls = []
        for t in lanes:
            total = done[2 * t + 1]
            image = (total[0:8] + total[8:16])[0:3]
            for h in range(3):
                image_ref[h, pl.ds(row[t], 1)] = image[h : h + 1]
                resid[t, h : h + 1] = (image[h : h + 1] - target_ref[h, pl.ds(row[t], 1)]) * (
                    2.0 / 512.0
                )
            g = resid[t]
            g1 = rounded(g)
            g2 = g - g1
            pulls.append(
                (
                    jnp.concatenate([g1, g1, g2, zero_row], axis=0).astype(BF16),
                    jnp.concatenate([g1, g2], axis=0).astype(BF16),
                )
            )

        def lean(t, j, e):
            slopes[e, t] = lax.dot_general(
                hue_back[place(t, PAIR * j + e)],
                pulls[t][0],
                (((0,), (0,)), ((), ())),
                preferred_element_type=F32,
            )

        def behind_of(t, j, e, behind):
            run = weights[t][j, e, 0:8] * slopes[e, t, 0:8]
            for i in range(1, chunks):
                lo, hi = 8 * i, 8 * i + 8
                run = run + weights[t][j, e, lo:hi] * slopes[e, t, lo:hi]
            scan = jnp.where(sub == 7, behind, shifted(run, -1))
            for d in (1, 2, 4):
                scan = scan + jnp.where(sub < 8 - d, shifted(scan, -d), 0.0)
            return (
                scan / jnp.maximum(ends[t][j, e], 1e-37),
                jnp.broadcast_to((run + scan)[0:1], (8, PIXELS)),
            )

        def step_of(t, j, e, here):
            for i in range(chunks - 2, -1, -2):
                lo, mid, hi = 8 * i, 8 * i + 8, 8 * i + 16
                ahead = slopes[e, t, mid:hi]
                gap = ahead - here
                two = weights[t][j, e, mid:hi] * gap
                here = ahead - keeps[t][j, e, mid:hi] * gap
                ahead = slopes[e, t, lo:mid]
                gap = ahead - here
                one = weights[t][j, e, lo:mid] * gap
                here = ahead - keeps[t][j, e, lo:mid] * gap
                pair = jnp.concatenate([one, two], axis=0)
                high = pair.astype(BF16)
                steps[e, t, lo:hi] = high
                steps[e, t, block + lo : block + hi] = (pair - high.astype(F32)).astype(BF16)

        def backward(index, carry):
            j = turns - 1 - index
            behind = list(carry)
            places = []
            for e in reversed(range(PAIR)):
                for t in lanes:
                    lean(t, j, e)
            for e in reversed(range(PAIR)):
                for t in lanes:
                    hues = lax.dot_general(
                        pulls[t][1], halves[t][j, e], (((1,), (1,)), ((), ())),
                        preferred_element_type=F32,
                    )
                    places.append(
                        (t, e, 8, hues[0:8, 0:block] + hues[0:8, block:] + hues[8:16, 0:block])
                    )
                heres = []
                for t in lanes:
                    here, behind[t] = behind_of(t, j, e, behind[t])
                    heres.append(here)
                for t in lanes:
                    step_of(t, j, e, heres[t])
                for t in lanes:
                    sums = lax.dot_general(
                        monomials, steps[e, t], (((1,), (1,)), ((), ())), preferred_element_type=F32
                    )
                    places.append((t, e, 0, sums[:, 0:block] + sums[:, block:]))
            for t, e, at, value in places:
                moments[t][j, e, at : at + 8] = value
            return tuple(behind)

        lax.fori_loop(0, turns, backward, (jnp.zeros((8, PIXELS), F32),) * GROUP)

        def settle(k, _):
            for t, e in spots:
                cx, cy = centre[t]
                s = place(t, PAIR * k + e)
                u = screen[s, 0:1] - cx
                v = screen[s, 1:2] - cy
                a, b, c = screen[s, 2:3], screen[s, 3:4], screen[s, 4:5]
                mxx, mxy, myy = (moments[t][k, e, j : j + 1] for j in (0, 1, 2))
                mx, my, m = (moments[t][k, e, j : j + 1] for j in (3, 4, 5))
                off_x = mx - u * m
                off_y = my - v * m
                changes = (
                    a * off_x + b * off_y,
                    b * off_x + c * off_y,
                    -0.5 * (mxx - u * (mx + off_x)),
                    -(mxy - u * my - v * off_x),
                    -0.5 * (myy - v * (my + off_y)),
                    m,
                    moments[t][k, e, 8:9],
                    moments[t][k, e, 9:10],
                    moments[t][k, e, 10:11],
                )
                owner, i = lax.div(s, cap), lax.rem(s, cap)
                for j, change in enumerate(changes):
                    at = pl.ds(8 * i + j if j < 8 else 8 * cap + i, 1)
                    grad_ref[owner, at] = grad_ref[owner, at] + change
            return 0

        lax.fori_loop(0, turns, settle, 0)
        return 0

    lax.fori_loop(0, tiles // GROUP, group, 0)


def blend(arrived, cap, target, tile_place, pairs, order):
    channels, tiles, pixels = target.shape
    depth = pairs.shape[0]
    devices, rows, block = arrived.shape
    slots = devices * cap
    turns = pl.cdiv(depth, PAIR)
    if depth % PAIR:
        pairs = jnp.pad(pairs, ((0, PAIR * turns - depth), (0, 0)), constant_values=-1)
    basis = jnp.asarray(pixel_basis())
    smem = pl.BlockSpec(memory_space=pltpu.SMEM)
    vmem = pl.BlockSpec(memory_space=pltpu.VMEM)
    return pl.pallas_call(
        functools.partial(blend_kernel, cap),
        in_specs=[smem, smem, smem, vmem, vmem, vmem],
        out_specs=[vmem, vmem],
        scratch_shapes=[
            pltpu.VMEM((slots + 1, 16, block), F32),
            pltpu.VMEM((slots + 1, 16, 2 * block), BF16),
            pltpu.VMEM((slots + 1, 32, block), BF16),
            pltpu.VMEM((PAIR, GROUP, block, pixels), F32),
            pltpu.VMEM((PAIR, GROUP, block, pixels), F32),
            pltpu.VMEM((PAIR, GROUP, 2 * block, pixels), BF16),
            pltpu.VMEM((GROUP, 8, pixels), F32),
        ]
        + [pltpu.VMEM((turns, PAIR, 8, block), F32)] * GROUP
        + [pltpu.VMEM((turns, PAIR, block, pixels), F32)] * GROUP
        + [pltpu.VMEM((turns, PAIR, block, pixels), F32)] * GROUP
        + [pltpu.VMEM((turns, PAIR, 2 * block, pixels), BF16)] * GROUP
        + [pltpu.VMEM((turns, PAIR, 8, pixels), F32)] * GROUP
        + [pltpu.VMEM((turns, PAIR, 16, block), F32)] * GROUP,
        out_shape=[
            jax.ShapeDtypeStruct(target.shape, F32),
            jax.ShapeDtypeStruct((devices + 1, rows, block), F32),
        ],
        name="blend",
        compiler_params=pltpu.CompilerParams(),
    )(pairs, tile_place, order, basis, arrived, target)


def whereabouts(sizes):
    nx, ny = sizes
    me = lax.axis_index("gx") * ny + lax.axis_index("gy")

    def other(n):
        o = lax.rem(me + n, nx * ny)
        return o, (lax.div(o, ny), lax.rem(o, ny))

    return me, nx * ny, other


def greet(devices, other):
    barrier = pltpu.get_barrier_semaphore()

    def call(n, _):
        pl.semaphore_signal(
            barrier, inc=1, device_id=other(n)[1], device_id_type=pl.DeviceIdType.MESH
        )
        return 0

    lax.fori_loop(1, devices, call, 0)
    return barrier


def post(source, target, sems, where):
    return pltpu.make_async_remote_copy(
        src_ref=source,
        dst_ref=target,
        send_sem=sems.at[0],
        recv_sem=sems.at[1],
        device_id=where,
        device_id_type=pl.DeviceIdType.MESH,
    )


def order_rows(pairs, order_ref):
    depth, tiles = pairs.shape
    live = jnp.sum((pairs >= 0).astype(F32), axis=0, keepdims=True)
    across = lax.broadcasted_iota(jnp.int32, (tiles, tiles), 1).astype(F32)
    down = lax.broadcasted_iota(jnp.int32, (tiles, tiles), 0).astype(F32)
    theirs = jnp.broadcast_to(live, (tiles, tiles))
    mine = jnp.sum(jnp.where(across == down, theirs, 0.0), axis=1, keepdims=True)
    before = (theirs > mine) | ((theirs == mine) & (across < down))
    rank = jnp.sum(before.astype(F32), axis=1, keepdims=True)
    order = jnp.sum(jnp.where(rank == across, down, 0.0), axis=0, keepdims=True)
    order_ref[...] = order.astype(jnp.int32)


def fetch_kernel(
    sizes, width, height, splats_ref, fetch_ref, pairs_ref, order_ref, arrived_ref, rows_ref, asked,
    own, send, ask, heard, ask_sems, sems, local_sem,
):
    me, devices, other = whereabouts(sizes)
    cap = fetch_ref.shape[0]
    blocks, _, block = own.shape
    used = 9 * cap
    barrier = greet(devices, other)

    order_rows(pairs_ref[...], rows_ref)
    table = jnp.concatenate([fetch_ref[...], jnp.zeros((8 - cap, devices), jnp.int32)], axis=0)
    if devices % 128:
        table = jnp.concatenate(
            [table, jnp.zeros((8, 128 - devices % 128), jnp.int32)], axis=1
        )
    table = jnp.transpose(table.astype(F32))[0:devices]
    ask[...] = jnp.zeros_like(ask)
    ask[:, :, 0:8] = table.astype(jnp.int32).reshape(devices, 1, 8)

    raw = splats_ref
    place_x, place_y, place_z = raw[0], raw[1], raw[2]
    inverse_one = jnp.exp(-2.0 * raw[3])
    inverse_two = jnp.exp(-2.0 * raw[4])
    cosine = jnp.cos(raw[5])
    sine = jnp.sin(raw[5])
    length = jnp.sqrt(place_x * place_x + place_y * place_y + place_z * place_z)
    terms = harmonic_terms(place_x / length, place_y / length, place_z / length)
    lines = [
        width * place_x / place_z + 0.5 * width,
        width * place_y / place_z + 0.5 * height,
        cosine * cosine * inverse_one + sine * sine * inverse_two,
        cosine * sine * (inverse_one - inverse_two),
        sine * sine * inverse_one + cosine * cosine * inverse_two,
        jnp.minimum(raw[6], 0.0) - jnp.log1p(jnp.exp(-jnp.abs(raw[6]))),
    ]
    for h in range(3):
        color = jnp.full((blocks, block), 0.5, F32)
        for k in range(16):
            color = color + raw[7 + 16 * h + k] * terms[k]
        lines.append(color)
    order = order_ref[...].astype(BF16)
    for j, line in enumerate(lines):
        one = rounded(line)
        two = rounded(line - one)
        three = line - one - two
        stack = jnp.concatenate([one, two, three], axis=0).astype(BF16)
        mixed = jnp.dot(stack, order, preferred_element_type=F32)
        mixed = mixed[0:blocks] + mixed[blocks : 2 * blocks] + mixed[2 * blocks :]
        own[:, j, :] = mixed

    pl.semaphore_wait(barrier, devices - 1)

    def inquire(n, _):
        o, where = other(n)
        post(ask.at[o], asked.at[me], ask_sems, where).start()
        return 0

    lax.fori_loop(1, devices, inquire, 0)
    keep = pltpu.make_async_copy(ask.at[me], asked.at[me], local_sem)
    keep.start()
    keep.wait()
    rest = pl.ds(0, devices - 1)
    bulk = post(ask.at[rest], asked.at[rest], ask_sems, other(1)[1])
    bulk.wait_recv()
    load = pltpu.make_async_copy(asked, heard, local_sem)
    load.start()
    load.wait()

    def pick(o, target):
        for i in range(cap):
            b = jnp.clip(heard[o, 0, i], 0, blocks - 1)
            target[o, 8 * i : 8 * i + 8] = own[b, 0:8]
            target[o, 8 * cap + i : 8 * cap + i + 1] = own[b, 8:9]

    def fill(n, _):
        pick(other(n)[0], send)
        return 0

    lax.fori_loop(1, devices, fill, 0)
    pick(me, arrived_ref)
    part = pl.ds(0, used)

    def serve(n, _):
        o, where = other(n)
        post(send.at[o, part], arrived_ref.at[me, part], sems, where).start()
        return 0

    lax.fori_loop(1, devices, serve, 0)
    bulk.wait_send()
    whole = post(send.at[rest, part], arrived_ref.at[rest, part], sems, other(1)[1])
    whole.wait_recv()
    whole.wait_send()


def fetch_blocks(splats, fetch, pairs, sizes, width, height):
    _, blocks, block = splats.shape
    cap, devices = fetch.shape
    rows = 8 * pl.cdiv(9 * cap, 8)
    order = jnp.asarray(lane_order(block))
    vmem = pl.BlockSpec(memory_space=pltpu.VMEM)
    return pl.pallas_call(
        functools.partial(fetch_kernel, sizes, width, height),
        in_specs=[vmem] * 4,
        out_specs=[vmem] * 3,
        scratch_shapes=[
            pltpu.VMEM((blocks, 16, block), F32),
            pltpu.VMEM((devices, rows, block), F32),
            pltpu.VMEM((devices, 1, 128), jnp.int32),
            pltpu.SMEM((devices, 1, 128), jnp.int32),
            pltpu.SemaphoreType.DMA((2,)),
            pltpu.SemaphoreType.DMA((2,)),
            pltpu.SemaphoreType.DMA,
        ],
        out_shape=[
            jax.ShapeDtypeStruct((devices, rows, block), F32),
            jax.ShapeDtypeStruct((1, pairs.shape[1]), jnp.int32),
            jax.ShapeDtypeStruct((devices, 1, 128), jnp.int32),
        ],
        name="fetch",
        compiler_params=pltpu.CompilerParams(collective_id=0, has_side_effects=True),
    )(splats, fetch, pairs, order)


def thirds(x):
    one = rounded(x)
    two = rounded(x - one)
    return [one, two, x - one - two]


def return_kernel(
    sizes, cap, blocks, grad_ref, asked_ref, order_ref, total_ref, returned, sems
):
    me, devices, other = whereabouts(sizes)
    barrier = greet(devices, other)
    returned[me] = grad_ref[me]
    lane = lax.broadcasted_iota(jnp.int32, (devices, blocks), 1)
    owners = []
    for i in range(cap):
        column = jnp.broadcast_to(asked_ref[:, 0, i : i + 1], (devices, blocks))
        owners += [(column == lane).astype(F32)] * 3
    owners = jnp.concatenate(owners, axis=0).astype(BF16)
    order = order_ref[...].astype(BF16)
    pl.semaphore_wait(barrier, devices - 1)
    part = pl.ds(0, 9 * cap)

    def serve(n, _):
        o, where = other(n)
        post(grad_ref.at[o, part], returned.at[me, part], sems, where).start()
        return 0

    lax.fori_loop(1, devices, serve, 0)
    rest = pl.ds(0, devices - 1)
    whole = post(grad_ref.at[rest, part], returned.at[rest, part], sems, other(1)[1])
    whole.wait_recv()
    for r in range(9):
        terms = []
        for i in range(cap):
            terms += thirds(returned[:, 8 * i + r if r < 8 else 8 * cap + i, :])
        summed = lax.dot_general(
            owners,
            jnp.concatenate(terms, axis=0).astype(BF16),
            (((0,), (0,)), ((), ())),
            preferred_element_type=F32,
        )
        mixed = lax.dot_general(
            jnp.concatenate(thirds(summed), axis=0).astype(BF16),
            order,
            (((1,), (1,)), ((), ())),
            preferred_element_type=F32,
        )
        total_ref[r] = mixed[0:blocks] + mixed[blocks : 2 * blocks] + mixed[2 * blocks :]
    whole.wait_send()


def return_grads(grads, asked, blocks, sizes):
    more, rows, block = grads.shape
    cap = rows // 9
    order = jnp.asarray(lane_order(block))
    vmem = pl.BlockSpec(memory_space=pltpu.VMEM)
    return pl.pallas_call(
        functools.partial(return_kernel, sizes, cap, blocks),
        in_specs=[vmem] * 3,
        out_specs=vmem,
        scratch_shapes=[
            pltpu.VMEM((more - 1, rows, block), F32),
            pltpu.SemaphoreType.DMA((2,)),
        ],
        out_shape=jax.ShapeDtypeStruct((9, blocks, block), F32),
        name="give_back",
        compiler_params=pltpu.CompilerParams(collective_id=1, has_side_effects=True),
    )(grads, asked, order)


def outline(width, height, x, y, z, first, second, angle):
    inverse_one = jnp.exp(-2.0 * first)
    inverse_two = jnp.exp(-2.0 * second)
    cosine = jnp.cos(angle)
    sine = jnp.sin(angle)
    return (
        width * x / z + 0.5 * width,
        width * y / z + 0.5 * height,
        cosine * cosine * inverse_one + sine * sine * inverse_two,
        cosine * sine * (inverse_one - inverse_two),
        sine * sine * inverse_one + cosine * cosine * inverse_two,
    )


def directions(x, y, z):
    length = jnp.sqrt(x * x + y * y + z * z)
    return tuple(harmonic_terms(x / length, y / length, z / length))


def adam_kernel(
    width, height, total_ref, splats_ref, one_ref, two_ref, grad_ref, step_ref,
    raw, one, two, grad, step, load_sems, store_sems,
):
    count = raw.shape[0]
    cuts = [0, 7] + [7 + 16 * h for h in range(1, 4)]
    spans = [pl.ds(lo, hi - lo) for lo, hi in zip(cuts, cuts[1:])]
    load = pltpu.make_async_copy(splats_ref, raw, load_sems.at[0])
    load.start()
    loads = []
    for n, span in enumerate(spans[1:] + spans[:1]):
        pair = [
            pltpu.make_async_copy(one_ref.at[span], one.at[span], load_sems.at[1 + 2 * n]),
            pltpu.make_async_copy(two_ref.at[span], two.at[span], load_sems.at[2 + 2 * n]),
        ]
        for copy in pair:
            copy.start()
        loads.append(pair)
    load.wait()
    place = (raw[0], raw[1], raw[2])
    terms, turn = jax.vjp(directions, *place)
    slants = [jnp.zeros_like(place[0]) for _ in terms]
    stores = []

    def finish(n, span, lo, hi):
        for copy in loads[n]:
            copy.wait()
        for r in range(lo, hi):
            change = grad[r]
            first = 0.9 * one[r] + 0.1 * change
            second = 0.999 * two[r] + 0.001 * change * change
            step[r] = first / (jnp.sqrt(second) + 1e-08)
        for m, (source, target) in enumerate(((grad, grad_ref), (step, step_ref))):
            copy = pltpu.make_async_copy(
                source.at[span], target.at[span], store_sems.at[2 * n + m]
            )
            copy.start()
            stores.append(copy)

    for h in range(3):
        hue = total_ref[6 + h]
        for k in range(16):
            r = 7 + 16 * h + k
            grad[r] = hue * terms[k]
            slants[k] = slants[k] + hue * raw[r]
        finish(h, spans[1 + h], cuts[1 + h], cuts[2 + h])
    _, pull = jax.vjp(
        functools.partial(outline, width, height), *place, raw[3], raw[4], raw[5]
    )
    flat = pull(tuple(total_ref[j] for j in range(5)))
    tilt = turn(tuple(slants))
    for j in range(3):
        grad[j] = flat[j] + tilt[j]
    for j in range(3, 6):
        grad[j] = flat[j]
    grad[6] = total_ref[5] / (1.0 + jnp.exp(raw[6]))
    finish(3, spans[0], 0, 7)
    for copy in stores:
        copy.wait()


def adam(total, splats, moment_one, moment_two, width, height):
    anywhere = pl.BlockSpec(memory_space=pl.ANY)
    vmem = pl.BlockSpec(memory_space=pltpu.VMEM)
    like = jax.ShapeDtypeStruct(splats.shape, F32)
    return pl.pallas_call(
        functools.partial(adam_kernel, width, height),
        in_specs=[vmem, anywhere, anywhere, anywhere],
        out_specs=[anywhere, anywhere],
        scratch_shapes=[pltpu.VMEM(splats.shape, F32)] * 5
        + [pltpu.SemaphoreType.DMA((9,)), pltpu.SemaphoreType.DMA((8,))],
        out_shape=[like, like],
        name="adam",
    )(total, splats, moment_one, moment_two)


def local(splats, moment_one, moment_two, target, tile_place, pairs, fetch):
    sizes = (lax.axis_size("gx"), lax.axis_size("gy"))
    devices = sizes[0] * sizes[1]
    tiles_here = target.shape[0]
    cap = fetch.shape[2]
    width = 16.0 * TX
    height = 16.0 * (tiles_here * devices // TX)

    rows_first = jnp.transpose(splats, (1, 0, 2))
    asks = jnp.transpose(fetch[0])
    lists = jnp.transpose(pairs)
    arrived, rows, asked = fetch_blocks(rows_first, asks, lists, sizes, width, height)
    image, grads = blend(
        arrived, cap, jnp.transpose(target, (1, 0, 2)), tile_place, lists, rows
    )
    total = return_grads(grads, asked, splats.shape[0], sizes)
    splat_grad, adam_step = adam(
        total,
        rows_first,
        jnp.transpose(moment_one, (1, 0, 2)),
        jnp.transpose(moment_two, (1, 0, 2)),
        width,
        height,
    )
    back = lambda x: jnp.transpose(x, (1, 0, 2))
    return (back(image), back(splat_grad), back(adam_step))


def solution(mesh):
    both = ("gx", "gy")
    return jax.shard_map(
        local,
        mesh=mesh,
        in_specs=(
            P(both, None, None),
            P(both, None, None),
            P(both, None, None),
            P(both, None, None),
            P(both),
            P(both, None),
            P(both, None, None),
        ),
        out_specs=(P(both, None, None), P(both, None, None), P(both, None, None)),
        check_vma=False,
    )
```

```python
import functools

import jax
import jax.numpy as jnp
import numpy as np
from jax import lax
from jax.experimental import pallas as pl
from jax.experimental.pallas import tpu as pltpu
from jax.sharding import PartitionSpec as P

TX = 16
SIDE = 16
PIXELS = SIDE * SIDE
LOG2E = 1.4426950408889634
DEAD = -1.0e4
GROUP = 4
PAIR = 2
F32 = jnp.float32
BF16 = jnp.bfloat16


HARMONIC_ZERO = 0.28209479177387814
HARMONIC_ONE = 0.4886025119029199
HARMONIC_TWO = (
    1.0925484305920792,
    -1.0925484305920792,
    0.31539156525252005,
    -1.0925484305920792,
    0.5462742152960396,
)
HARMONIC_THREE = (
    -0.5900435899266435,
    2.890611442640554,
    -0.4570457994644658,
    0.3731763325901154,
    -0.4570457994644658,
    1.445305721320277,
    -0.5900435899266435,
)


def harmonic_terms(east, north, ahead):
    east_east = east * east
    north_north = north * north
    ahead_ahead = ahead * ahead
    return [
        jnp.full_like(east, HARMONIC_ZERO),
        -HARMONIC_ONE * north,
        HARMONIC_ONE * ahead,
        -HARMONIC_ONE * east,
        HARMONIC_TWO[0] * east * north,
        HARMONIC_TWO[1] * north * ahead,
        HARMONIC_TWO[2] * (2.0 * ahead_ahead - east_east - north_north),
        HARMONIC_TWO[3] * east * ahead,
        HARMONIC_TWO[4] * (east_east - north_north),
        HARMONIC_THREE[0] * north * (3.0 * east_east - north_north),
        HARMONIC_THREE[1] * east * north * ahead,
        HARMONIC_THREE[2] * north * (4.0 * ahead_ahead - east_east - north_north),
        HARMONIC_THREE[3] * ahead * (2.0 * ahead_ahead - 3.0 * east_east - 3.0 * north_north),
        HARMONIC_THREE[4] * east * (4.0 * ahead_ahead - east_east - north_north),
        HARMONIC_THREE[5] * ahead * (east_east - north_north),
        HARMONIC_THREE[6] * east * (east_east - 3.0 * north_north),
    ]


def pixel_basis():
    j = np.arange(PIXELS)
    x = j % SIDE + 0.5 - SIDE / 2
    y = j // SIDE + 0.5 - SIDE / 2
    rows = np.stack([x * x, x * y, y * y, x, y, np.ones_like(x), 0 * x, 0 * x])
    return np.concatenate([rows, rows, rows, 0 * rows]).astype(np.float32)


def lane_order(block):
    row = np.arange(block)
    splat = (row % 8) * (block // 8) + row // 8
    return (np.arange(block)[:, None] == splat[None, :]).astype(np.float32)


def rounded(x):
    return x.astype(BF16).astype(F32)


def shifted(x, shift):
    return pltpu.roll(x, shift % 8, 0)


def blend_kernel(
    cap, pairs_ref, place_ref, order_ref, basis_ref, arrived_ref, target_ref, image_ref, grad_ref,
    screen, owed, hue_sum, hue_back, alphas, slopes, steps, resid, parts, moments, *banks,
):
    tiles = target_ref.shape[1]
    depth = pairs_ref.shape[0] - PAIR
    slots = cap * arrived_ref.shape[0]
    block = arrived_ref.shape[2]
    chunks = block // 8
    lanes = range(GROUP)
    spots = [(t, e) for e in range(PAIR) for t in lanes]
    keeps, weights, halves, ends = (banks[GROUP * i : GROUP * i + GROUP] for i in range(4))
    sub = lax.broadcasted_iota(jnp.int32, (8, PIXELS), 0)

    resid[...] = jnp.zeros_like(resid)
    parts[...] = jnp.zeros_like(parts)

    def prepare(o, _):
        for i in range(cap):
            s = cap * o + i
            owed[s] = jnp.zeros((16, block), F32)
            last = arrived_ref[o, 8 * cap + i : 8 * cap + i + 1]
            screen[s, 0:8] = arrived_ref[o, 8 * i : 8 * i + 8]
            screen[s, 8:9] = last
            hue = jnp.concatenate(
                [arrived_ref[o, 8 * i + 6 : 8 * i + 8], last, jnp.zeros((5, block), F32)], axis=0
            )
            hue1 = rounded(hue)
            hue2 = hue - hue1
            zero = jnp.zeros_like(hue)
            hue_sum[s] = jnp.concatenate(
                [
                    jnp.concatenate([hue1, hue1], axis=1),
                    jnp.concatenate([hue2, zero], axis=1),
                ],
                axis=0,
            ).astype(BF16)
            hue_back[s] = jnp.concatenate([hue1, hue2, hue1, zero], axis=0).astype(BF16)
        return 0

    lax.fori_loop(0, arrived_ref.shape[0], prepare, 0)
    owed[slots] = jnp.zeros((16, block), F32)
    screen[slots] = jnp.zeros((16, block), F32)
    screen[slots, 5:6] = jnp.full((1, block), DEAD, F32)
    hue_sum[slots] = jnp.zeros((16, 2 * block), BF16)
    hue_back[slots] = jnp.zeros((32, block), BF16)

    basis = basis_ref[...].astype(BF16)
    monomials = basis_ref[0:8].astype(BF16)
    zero_row = jnp.zeros((8, PIXELS), F32)

    def group(step, _):
        row = [order_ref[0, step * GROUP + t] for t in lanes]
        deepest = jnp.int32(0)
        for k in range(depth):
            deepest = deepest + (pairs_ref[k, row[0]] >= 0).astype(jnp.int32)
        turns = lax.div(deepest + (PAIR - 1), PAIR)
        centre = []
        for t in lanes:
            tile = place_ref[row[t]]
            cx = (lax.rem(tile, TX) * SIDE + SIDE // 2).astype(F32)
            cy = (lax.div(tile, TX) * SIDE + SIDE // 2).astype(F32)
            centre.append((cx, cy))

        def place(t, k):
            slot = pairs_ref[k, row[t]]
            return jnp.where(slot >= 0, slot, slots)

        def shape_up(j):
            for t, e in spots:
                cx, cy = centre[t]
                s = place(t, PAIR * j + e)
                u = screen[s, 0:1] - cx
                v = screen[s, 1:2] - cy
                a, b, c = screen[s, 2:3], screen[s, 3:4], screen[s, 4:5]
                opac = jnp.maximum(screen[s, 5:6], DEAD)
                lin_x = a * u + b * v
                lin_y = b * u + c * v
                const = opac - 0.5 * (lin_x * u + lin_y * v)
                for r, value in enumerate((-0.5 * a, -b, -0.5 * c, lin_x, lin_y, const)):
                    parts[e, t, r : r + 1] = LOG2E * value

        shape_up(0)

        def power_of(t, e):
            c = parts[e, t]
            c1 = rounded(c)
            c2 = rounded(c - c1)
            c3 = c - c1 - c2
            left = jnp.concatenate([c1, c2, c3, jnp.zeros_like(c)], axis=0).astype(BF16)
            return lax.dot_general(
                left, basis, (((0,), (0,)), ((), ())), preferred_element_type=F32
            )

        def draw(t, j, e, power):
            alpha = jnp.exp2(power)
            alphas[e, t] = alpha
            keep = 1.0 - alpha
            keeps[t][j, e] = keep
            kept = keep[0:8]
            for i in range(1, chunks):
                kept = kept * keep[8 * i : 8 * i + 8]
            return kept

        def scan_of(t, j, e, kept, trans):
            scan = jnp.where(sub == 0, trans, shifted(kept, 1))
            for d in (1, 2, 4):
                scan = scan * jnp.where(sub < d, 1.0, shifted(scan, d))
            end = scan * kept
            ends[t][j, e] = end
            return scan, jnp.broadcast_to(end[7:8], (8, PIXELS))

        def spread(t, j, e, here):
            for i in range(0, chunks, 2):
                lo, mid, hi = 8 * i, 8 * i + 8, 8 * i + 16
                one = alphas[e, t, lo:mid] * here
                here = here * keeps[t][j, e, lo:mid]
                two = alphas[e, t, mid:hi] * here
                here = here * keeps[t][j, e, mid:hi]
                pair = jnp.concatenate([one, two], axis=0)
                weights[t][j, e, lo:hi] = pair
                high = pair.astype(BF16)
                halves[t][j, e, lo:hi] = high
                halves[t][j, e, block + lo : block + hi] = (pair - high.astype(F32)).astype(BF16)

        def summed(t, j, e):
            return jnp.dot(
                hue_sum[place(t, PAIR * j + e)], halves[t][j, e], preferred_element_type=F32
            )

        def forward(j, carry):
            trans = [carry[2 * t] for t in lanes]
            totals = [carry[2 * t + 1] for t in lanes]
            powers = [[power_of(t, e) for t in lanes] for e in range(PAIR)]
            kepts = [draw(t, j, 0, powers[0][t]) for t in lanes]
            for e in range(PAIR):
                heres = []
                for t in lanes:
                    here, trans[t] = scan_of(t, j, e, kepts[t], trans[t])
                    heres.append(here)
                for t in lanes:
                    spread(t, j, e, heres[t])
                    if e + 1 < PAIR:
                        kepts[t] = draw(t, j, e + 1, powers[e + 1][t])
                totals = [totals[t] + summed(t, j, e) for t in lanes]
            shape_up(j + 1)
            return tuple(x for t in lanes for x in (trans[t], totals[t]))

        start = (jnp.ones((8, PIXELS), F32), jnp.zeros((16, PIXELS), F32)) * GROUP
        done = lax.fori_loop(0, turns, forward, start)

        pulls = []
        for t in lanes:
            total = done[2 * t + 1]
            image = (total[0:8] + total[8:16])[0:3]
            for h in range(3):
                image_ref[h, pl.ds(row[t], 1)] = image[h : h + 1]
                resid[t, h : h + 1] = (image[h : h + 1] - target_ref[h, pl.ds(row[t], 1)]) * (
                    2.0 / 512.0
                )
            g = resid[t]
            g1 = rounded(g)
            g2 = g - g1
            pulls.append(
                (
                    jnp.concatenate([g1, g1, g2, zero_row], axis=0).astype(BF16),
                    jnp.concatenate([g1, g2], axis=0).astype(BF16),
                )
            )

        def lean(t, j, e):
            slopes[e, t] = lax.dot_general(
                hue_back[place(t, PAIR * j + e)],
                pulls[t][0],
                (((0,), (0,)), ((), ())),
                preferred_element_type=F32,
            )

        def behind_of(t, j, e, behind):
            run = weights[t][j, e, 0:8] * slopes[e, t, 0:8]
            for i in range(1, chunks):
                lo, hi = 8 * i, 8 * i + 8
                run = run + weights[t][j, e, lo:hi] * slopes[e, t, lo:hi]
            scan = jnp.where(sub == 7, behind, shifted(run, -1))
            for d in (1, 2, 4):
                scan = scan + jnp.where(sub < 8 - d, shifted(scan, -d), 0.0)
            return (
                scan / jnp.maximum(ends[t][j, e], 1e-37),
                jnp.broadcast_to((run + scan)[0:1], (8, PIXELS)),
            )

        def step_of(t, j, e, here):
            for i in range(chunks - 2, -1, -2):
                lo, mid, hi = 8 * i, 8 * i + 8, 8 * i + 16
                ahead = slopes[e, t, mid:hi]
                gap = ahead - here
                two = weights[t][j, e, mid:hi] * gap
                here = ahead - keeps[t][j, e, mid:hi] * gap
                ahead = slopes[e, t, lo:mid]
                gap = ahead - here
                one = weights[t][j, e, lo:mid] * gap
                here = ahead - keeps[t][j, e, lo:mid] * gap
                pair = jnp.concatenate([one, two], axis=0)
                high = pair.astype(BF16)
                steps[e, t, lo:hi] = high
                steps[e, t, block + lo : block + hi] = (pair - high.astype(F32)).astype(BF16)

        def settle(j):
            for t, e in spots:
                cx, cy = centre[t]
                s = place(t, PAIR * j + e)
                u = screen[s, 0:1] - cx
                v = screen[s, 1:2] - cy
                a, b, c = screen[s, 2:3], screen[s, 3:4], screen[s, 4:5]
                mxx, mxy, myy, mx, my, m = (moments[e, t, r : r + 1] for r in range(6))
                off_x = mx - u * m
                off_y = my - v * m
                changes = (
                    a * off_x + b * off_y,
                    b * off_x + c * off_y,
                    -0.5 * (mxx - u * (mx + off_x)),
                    -(mxy - u * my - v * off_x),
                    -0.5 * (myy - v * (my + off_y)),
                    m,
                    moments[e, t, 8:9],
                    moments[e, t, 9:10],
                    moments[e, t, 10:11],
                )
                for r, change in enumerate(changes):
                    owed[s, r : r + 1] = owed[s, r : r + 1] + change

        def backward(index, carry):
            j = turns - 1 - index
            behind = list(carry)
            settle(j + 1)
            places = []
            for e in reversed(range(PAIR)):
                for t in lanes:
                    lean(t, j, e)
            for e in reversed(range(PAIR)):
                for t in lanes:
                    hues = lax.dot_general(
                        pulls[t][1], halves[t][j, e], (((1,), (1,)), ((), ())),
                        preferred_element_type=F32,
                    )
                    places.append(
                        (t, e, 8, hues[0:8, 0:block] + hues[0:8, block:] + hues[8:16, 0:block])
                    )
                heres = []
                for t in lanes:
                    here, behind[t] = behind_of(t, j, e, behind[t])
                    heres.append(here)
                for t in lanes:
                    step_of(t, j, e, heres[t])
                for t in lanes:
                    sums = lax.dot_general(
                        monomials, steps[e, t], (((1,), (1,)), ((), ())), preferred_element_type=F32
                    )
                    places.append((t, e, 0, sums[:, 0:block] + sums[:, block:]))
            for t, e, at, value in places:
                moments[e, t, at : at + 8] = value
            return tuple(behind)

        lax.fori_loop(0, turns, backward, (jnp.zeros((8, PIXELS), F32),) * GROUP)

        settle(0)
        return 0

    lax.fori_loop(0, tiles // GROUP, group, 0)

    def pack(o, _):
        for i in range(cap):
            grad_ref[o, 8 * i : 8 * i + 8] = owed[cap * o + i, 0:8]
            grad_ref[o, 8 * cap + i : 8 * cap + i + 1] = owed[cap * o + i, 8:9]
        return 0

    lax.fori_loop(0, arrived_ref.shape[0], pack, 0)


def blend(arrived, cap, target, tile_place, pairs, order):
    channels, tiles, pixels = target.shape
    devices, rows, block = arrived.shape
    slots = devices * cap
    turns = pairs.shape[0] // PAIR
    basis = jnp.asarray(pixel_basis())
    smem = pl.BlockSpec(memory_space=pltpu.SMEM)
    vmem = pl.BlockSpec(memory_space=pltpu.VMEM)
    return pl.pallas_call(
        functools.partial(blend_kernel, cap),
        in_specs=[smem, smem, smem, vmem, vmem, vmem],
        out_specs=[vmem, vmem],
        scratch_shapes=[
            pltpu.VMEM((slots + 1, 16, block), F32),
            pltpu.VMEM((slots + 1, 16, block), F32),
            pltpu.VMEM((slots + 1, 16, 2 * block), BF16),
            pltpu.VMEM((slots + 1, 32, block), BF16),
            pltpu.VMEM((PAIR, GROUP, block, pixels), F32),
            pltpu.VMEM((PAIR, GROUP, block, pixels), F32),
            pltpu.VMEM((PAIR, GROUP, 2 * block, pixels), BF16),
            pltpu.VMEM((GROUP, 8, pixels), F32),
            pltpu.VMEM((PAIR, GROUP, 8, block), F32),
            pltpu.VMEM((PAIR, GROUP, 16, block), F32),
        ]
        + [pltpu.VMEM((turns, PAIR, block, pixels), F32)] * GROUP
        + [pltpu.VMEM((turns, PAIR, block, pixels), F32)] * GROUP
        + [pltpu.VMEM((turns, PAIR, 2 * block, pixels), BF16)] * GROUP
        + [pltpu.VMEM((turns, PAIR, 8, pixels), F32)] * GROUP,
        out_shape=[
            jax.ShapeDtypeStruct(target.shape, F32),
            jax.ShapeDtypeStruct((devices, rows, block), F32),
        ],
        name="blend",
        compiler_params=pltpu.CompilerParams(),
    )(pairs, tile_place, order, basis, arrived, target)


def whereabouts(sizes):
    nx, ny = sizes
    me = lax.axis_index("gx") * ny + lax.axis_index("gy")

    def other(n):
        o = lax.rem(me + n, nx * ny)
        return o, (lax.div(o, ny), lax.rem(o, ny))

    return me, nx * ny, other


def greet(devices, other):
    barrier = pltpu.get_barrier_semaphore()

    def call(n, _):
        pl.semaphore_signal(
            barrier, inc=1, device_id=other(n)[1], device_id_type=pl.DeviceIdType.MESH
        )
        return 0

    lax.fori_loop(1, devices, call, 0)
    return barrier


def post(source, target, sems, where):
    return pltpu.make_async_remote_copy(
        src_ref=source,
        dst_ref=target,
        send_sem=sems.at[0],
        recv_sem=sems.at[1],
        device_id=where,
        device_id_type=pl.DeviceIdType.MESH,
    )


def order_rows(pairs, order_ref):
    depth, tiles = pairs.shape
    live = jnp.sum((pairs >= 0).astype(F32), axis=0, keepdims=True)
    across = lax.broadcasted_iota(jnp.int32, (tiles, tiles), 1).astype(F32)
    down = lax.broadcasted_iota(jnp.int32, (tiles, tiles), 0).astype(F32)
    theirs = jnp.broadcast_to(live, (tiles, tiles))
    mine = jnp.sum(jnp.where(across == down, theirs, 0.0), axis=1, keepdims=True)
    before = (theirs > mine) | ((theirs == mine) & (across < down))
    rank = jnp.sum(before.astype(F32), axis=1, keepdims=True)
    order = jnp.sum(jnp.where(rank == across, down, 0.0), axis=0, keepdims=True)
    order_ref[...] = order.astype(jnp.int32)


def fetch_kernel(
    sizes, width, height, splats_ref, fetch_ref, pairs_ref, order_ref,
    arrived_ref, rows_ref, lists_ref, asked,
    raw, wants, lists, mix, own, send, ask, heard, ask_sems, sems, local_sems,
):
    me, devices, other = whereabouts(sizes)
    cap = fetch_ref.shape[0]
    blocks, _, block = own.shape
    used = 9 * cap
    barrier = greet(devices, other)
    loads = [
        pltpu.make_async_copy(source, target, local_sems.at[n])
        for n, (source, target) in enumerate(
            ((fetch_ref, wants), (pairs_ref, lists), (splats_ref, raw), (order_ref, mix))
        )
    ]
    for load in loads:
        load.start()

    loads[0].wait()
    table = jnp.concatenate([wants[...], jnp.zeros((8 - cap, devices), jnp.int32)], axis=0)
    if devices % 128:
        table = jnp.concatenate(
            [table, jnp.zeros((8, 128 - devices % 128), jnp.int32)], axis=1
        )
    table = jnp.transpose(table.astype(F32))[0:devices]
    ask[...] = jnp.zeros_like(ask)
    ask[:, :, 0:8] = table.astype(jnp.int32).reshape(devices, 1, 8)

    loads[1].wait()
    order_rows(lists[...], rows_ref)
    depth = lists.shape[0]
    lists_ref[...] = jnp.full(lists_ref.shape, -1, jnp.int32)
    lists_ref[0:depth] = lists[...]
    loads[2].wait()
    loads[3].wait()
    place_x, place_y, place_z = raw[0], raw[1], raw[2]
    inverse_one = jnp.exp(-2.0 * raw[3])
    inverse_two = jnp.exp(-2.0 * raw[4])
    cosine = jnp.cos(raw[5])
    sine = jnp.sin(raw[5])
    length = jnp.sqrt(place_x * place_x + place_y * place_y + place_z * place_z)
    terms = harmonic_terms(place_x / length, place_y / length, place_z / length)
    lines = [
        width * place_x / place_z + 0.5 * width,
        width * place_y / place_z + 0.5 * height,
        cosine * cosine * inverse_one + sine * sine * inverse_two,
        cosine * sine * (inverse_one - inverse_two),
        sine * sine * inverse_one + cosine * cosine * inverse_two,
        jnp.minimum(raw[6], 0.0) - jnp.log1p(jnp.exp(-jnp.abs(raw[6]))),
    ]
    for h in range(3):
        color = jnp.full((blocks, block), 0.5, F32)
        for k in range(16):
            color = color + raw[7 + 16 * h + k] * terms[k]
        lines.append(color)
    order = mix[...].astype(BF16)
    for j, line in enumerate(lines):
        one = rounded(line)
        two = rounded(line - one)
        three = line - one - two
        stack = jnp.concatenate([one, two, three], axis=0).astype(BF16)
        mixed = jnp.dot(stack, order, preferred_element_type=F32)
        mixed = mixed[0:blocks] + mixed[blocks : 2 * blocks] + mixed[2 * blocks :]
        own[:, j, :] = mixed

    pl.semaphore_wait(barrier, devices - 1)

    def inquire(n, _):
        o, where = other(n)
        post(ask.at[o], asked.at[me], ask_sems, where).start()
        return 0

    lax.fori_loop(1, devices, inquire, 0)
    keep = pltpu.make_async_copy(ask.at[me], asked.at[me], local_sems.at[0])
    keep.start()
    keep.wait()
    rest = pl.ds(0, devices - 1)
    bulk = post(ask.at[rest], asked.at[rest], ask_sems, other(1)[1])
    bulk.wait_recv()
    load = pltpu.make_async_copy(asked, heard, local_sems.at[1])
    load.start()
    load.wait()

    def pick(o):
        for i in range(cap):
            b = jnp.clip(heard[o, 0, i], 0, blocks - 1)
            send[o, 8 * i : 8 * i + 8] = own[b, 0:8]
            send[o, 8 * cap + i : 8 * cap + i + 1] = own[b, 8:9]

    part = pl.ds(0, used)

    def serve(n):
        o, where = other(n)
        post(send.at[o, part], arrived_ref.at[me, part], sems, where).start()

    lag = 2
    for n in range(1, lag + 1):
        pick(other(n)[0])

    def run(n, _):
        pick(other(n + lag)[0])
        serve(n)
        return 0

    lax.fori_loop(1, devices - lag, run, 0)
    pick(me)
    for n in range(devices - lag, devices):
        serve(n)
    keep = pltpu.make_async_copy(send.at[me], arrived_ref.at[me], local_sems.at[0])
    keep.start()
    bulk.wait_send()
    whole = post(send.at[rest, part], arrived_ref.at[rest, part], sems, other(1)[1])
    whole.wait_recv()
    whole.wait_send()
    keep.wait()


def fetch_blocks(splats, fetch, pairs, sizes, width, height):
    _, blocks, block = splats.shape
    cap, devices = fetch.shape
    rows = 8 * pl.cdiv(9 * cap, 8)
    order = jnp.asarray(lane_order(block))
    depth = PAIR * pl.cdiv(pairs.shape[0], PAIR)
    vmem = pl.BlockSpec(memory_space=pltpu.VMEM)
    anywhere = pl.BlockSpec(memory_space=pl.ANY)
    return pl.pallas_call(
        functools.partial(fetch_kernel, sizes, width, height),
        in_specs=[anywhere] * 4,
        out_specs=[anywhere] + [vmem] * 3,
        scratch_shapes=[
            pltpu.VMEM(splats.shape, F32),
            pltpu.VMEM(fetch.shape, jnp.int32),
            pltpu.VMEM(pairs.shape, jnp.int32),
            pltpu.VMEM(order.shape, F32),
            pltpu.VMEM((blocks, 16, block), F32),
            pltpu.VMEM((devices, rows, block), F32),
            pltpu.VMEM((devices, 1, 128), jnp.int32),
            pltpu.SMEM((devices, 1, 128), jnp.int32),
            pltpu.SemaphoreType.DMA((2,)),
            pltpu.SemaphoreType.DMA((2,)),
            pltpu.SemaphoreType.DMA((4,)),
        ],
        out_shape=[
            jax.ShapeDtypeStruct((devices, rows, block), F32),
            jax.ShapeDtypeStruct((1, pairs.shape[1]), jnp.int32),
            jax.ShapeDtypeStruct((depth + PAIR, pairs.shape[1]), jnp.int32),
            jax.ShapeDtypeStruct((devices, 1, 128), jnp.int32),
        ],
        name="fetch",
        compiler_params=pltpu.CompilerParams(collective_id=0, has_side_effects=True),
    )(splats, fetch, pairs, order)


def thirds(x):
    one = rounded(x)
    two = rounded(x - one)
    return [one, two, x - one - two]


def return_kernel(
    sizes, cap, blocks, grad_ref, asked_ref, order_ref, total_ref,
    returned, asked, mix, sems, local_sems,
):
    me, devices, other = whereabouts(sizes)
    barrier = greet(devices, other)
    loads = [
        pltpu.make_async_copy(source, target, local_sems.at[n])
        for n, (source, target) in enumerate(
            ((grad_ref.at[me], returned.at[me]), (asked_ref, asked), (order_ref, mix))
        )
    ]
    for load in loads:
        load.start()
    for load in loads:
        load.wait()
    lane = lax.broadcasted_iota(jnp.int32, (devices, blocks), 1)
    owners = []
    for i in range(cap):
        column = jnp.broadcast_to(asked[:, 0, i : i + 1], (devices, blocks))
        owners += [(column == lane).astype(F32)] * 3
    owners = jnp.concatenate(owners, axis=0).astype(BF16)
    order = mix[...].astype(BF16)
    pl.semaphore_wait(barrier, devices - 1)
    part = pl.ds(0, 9 * cap)

    def serve(n, _):
        o, where = other(n)
        post(grad_ref.at[o, part], returned.at[me, part], sems, where).start()
        return 0

    lax.fori_loop(1, devices, serve, 0)
    rest = pl.ds(0, devices - 1)
    whole = post(grad_ref.at[rest, part], returned.at[rest, part], sems, other(1)[1])
    whole.wait_recv()
    for r in range(9):
        terms = []
        for i in range(cap):
            terms += thirds(returned[:, 8 * i + r if r < 8 else 8 * cap + i, :])
        summed = lax.dot_general(
            owners,
            jnp.concatenate(terms, axis=0).astype(BF16),
            (((0,), (0,)), ((), ())),
            preferred_element_type=F32,
        )
        mixed = lax.dot_general(
            jnp.concatenate(thirds(summed), axis=0).astype(BF16),
            order,
            (((1,), (1,)), ((), ())),
            preferred_element_type=F32,
        )
        total_ref[r] = mixed[0:blocks] + mixed[blocks : 2 * blocks] + mixed[2 * blocks :]
    whole.wait_send()


def return_grads(grads, asked, cap, blocks, sizes):
    devices, rows, block = grads.shape
    order = jnp.asarray(lane_order(block))
    vmem = pl.BlockSpec(memory_space=pltpu.VMEM)
    return pl.pallas_call(
        functools.partial(return_kernel, sizes, cap, blocks),
        in_specs=[pl.BlockSpec(memory_space=pl.ANY)] * 3,
        out_specs=vmem,
        scratch_shapes=[
            pltpu.VMEM((devices, rows, block), F32),
            pltpu.VMEM(asked.shape, jnp.int32),
            pltpu.VMEM(order.shape, F32),
            pltpu.SemaphoreType.DMA((2,)),
            pltpu.SemaphoreType.DMA((3,)),
        ],
        out_shape=jax.ShapeDtypeStruct((9, blocks, block), F32),
        name="give_back",
        compiler_params=pltpu.CompilerParams(collective_id=1, has_side_effects=True),
    )(grads, asked, order)


def outline(width, height, x, y, z, first, second, angle):
    inverse_one = jnp.exp(-2.0 * first)
    inverse_two = jnp.exp(-2.0 * second)
    cosine = jnp.cos(angle)
    sine = jnp.sin(angle)
    return (
        width * x / z + 0.5 * width,
        width * y / z + 0.5 * height,
        cosine * cosine * inverse_one + sine * sine * inverse_two,
        cosine * sine * (inverse_one - inverse_two),
        sine * sine * inverse_one + cosine * cosine * inverse_two,
    )


def directions(x, y, z):
    length = jnp.sqrt(x * x + y * y + z * z)
    return tuple(harmonic_terms(x / length, y / length, z / length))


def adam_kernel(
    width, height, total_ref, splats_ref, one_ref, two_ref, grad_ref, step_ref,
    raw, one, two, grad, step, load_sems, store_sems,
):
    count = raw.shape[0]
    cuts = [0, 7] + [7 + 16 * h for h in range(1, 4)]
    spans = [pl.ds(lo, hi - lo) for lo, hi in zip(cuts, cuts[1:])]
    load = pltpu.make_async_copy(splats_ref, raw, load_sems.at[0])
    load.start()
    loads = []
    for n, span in enumerate(spans[1:] + spans[:1]):
        pair = [
            pltpu.make_async_copy(one_ref.at[span], one.at[span], load_sems.at[1 + 2 * n]),
            pltpu.make_async_copy(two_ref.at[span], two.at[span], load_sems.at[2 + 2 * n]),
        ]
        for copy in pair:
            copy.start()
        loads.append(pair)
    load.wait()
    place = (raw[0], raw[1], raw[2])
    terms, turn = jax.vjp(directions, *place)
    slants = [jnp.zeros_like(place[0]) for _ in terms]
    stores = []

    def finish(n, span, lo, hi):
        for copy in loads[n]:
            copy.wait()
        for r in range(lo, hi):
            change = grad[r]
            first = 0.9 * one[r] + 0.1 * change
            second = 0.999 * two[r] + 0.001 * change * change
            step[r] = first / (second * lax.rsqrt(second) + 1e-08)
        for m, (source, target) in enumerate(((grad, grad_ref), (step, step_ref))):
            copy = pltpu.make_async_copy(
                source.at[span], target.at[span], store_sems.at[2 * n + m]
            )
            copy.start()
            stores.append(copy)

    for h in range(3):
        hue = total_ref[6 + h]
        for k in range(16):
            r = 7 + 16 * h + k
            grad[r] = hue * terms[k]
            slants[k] = slants[k] + hue * raw[r]
        finish(h, spans[1 + h], cuts[1 + h], cuts[2 + h])
    _, pull = jax.vjp(
        functools.partial(outline, width, height), *place, raw[3], raw[4], raw[5]
    )
    flat = pull(tuple(total_ref[j] for j in range(5)))
    tilt = turn(tuple(slants))
    for j in range(3):
        grad[j] = flat[j] + tilt[j]
    for j in range(3, 6):
        grad[j] = flat[j]
    grad[6] = total_ref[5] / (1.0 + jnp.exp(raw[6]))
    finish(3, spans[0], 0, 7)
    for copy in stores:
        copy.wait()


def adam(total, splats, moment_one, moment_two, width, height):
    anywhere = pl.BlockSpec(memory_space=pl.ANY)
    vmem = pl.BlockSpec(memory_space=pltpu.VMEM)
    like = jax.ShapeDtypeStruct(splats.shape, F32)
    return pl.pallas_call(
        functools.partial(adam_kernel, width, height),
        in_specs=[vmem, anywhere, anywhere, anywhere],
        out_specs=[anywhere, anywhere],
        scratch_shapes=[pltpu.VMEM(splats.shape, F32)] * 5
        + [pltpu.SemaphoreType.DMA((9,)), pltpu.SemaphoreType.DMA((8,))],
        out_shape=[like, like],
        name="adam",
    )(total, splats, moment_one, moment_two)


def local(splats, moment_one, moment_two, target, tile_place, pairs, fetch):
    sizes = (lax.axis_size("gx"), lax.axis_size("gy"))
    devices = sizes[0] * sizes[1]
    tiles_here = target.shape[0]
    cap = fetch.shape[2]
    width = 16.0 * TX
    height = 16.0 * (tiles_here * devices // TX)

    rows_first = jnp.transpose(splats, (1, 0, 2))
    asks = jnp.transpose(fetch[0])
    arrived, rows, lists, asked = fetch_blocks(
        rows_first, asks, jnp.transpose(pairs), sizes, width, height
    )
    image, grads = blend(
        arrived, cap, jnp.transpose(target, (1, 0, 2)), tile_place, lists, rows
    )
    total = return_grads(grads, asked, cap, splats.shape[0], sizes)
    splat_grad, adam_step = adam(
        total,
        rows_first,
        jnp.transpose(moment_one, (1, 0, 2)),
        jnp.transpose(moment_two, (1, 0, 2)),
        width,
        height,
    )
    back = lambda x: jnp.transpose(x, (1, 0, 2))
    return (back(image), back(splat_grad), back(adam_step))


def solution(mesh):
    both = ("gx", "gy")
    return jax.shard_map(
        local,
        mesh=mesh,
        in_specs=(
            P(both, None, None),
            P(both, None, None),
            P(both, None, None),
            P(both, None, None),
            P(both),
            P(both, None),
            P(both, None, None),
        ),
        out_specs=(P(both, None, None), P(both, None, None), P(both, None, None)),
        check_vma=False,
    )
```

```python
import functools

import jax
import jax.numpy as jnp
import numpy as np
from jax import lax
from jax.experimental import pallas as pl
from jax.experimental.pallas import tpu as pltpu
from jax.sharding import PartitionSpec as P

TX = 16
SIDE = 16
PIXELS = SIDE * SIDE
LOG2E = 1.4426950408889634
DEAD = -1.0e4
GROUP = 2
PAIR = 4
F32 = jnp.float32
BF16 = jnp.bfloat16


HARMONIC_ZERO = 0.28209479177387814
HARMONIC_ONE = 0.4886025119029199
HARMONIC_TWO = (
    1.0925484305920792,
    -1.0925484305920792,
    0.31539156525252005,
    -1.0925484305920792,
    0.5462742152960396,
)
HARMONIC_THREE = (
    -0.5900435899266435,
    2.890611442640554,
    -0.4570457994644658,
    0.3731763325901154,
    -0.4570457994644658,
    1.445305721320277,
    -0.5900435899266435,
)


def harmonic_terms(east, north, ahead):
    east_east = east * east
    north_north = north * north
    ahead_ahead = ahead * ahead
    return [
        jnp.full_like(east, HARMONIC_ZERO),
        -HARMONIC_ONE * north,
        HARMONIC_ONE * ahead,
        -HARMONIC_ONE * east,
        HARMONIC_TWO[0] * east * north,
        HARMONIC_TWO[1] * north * ahead,
        HARMONIC_TWO[2] * (2.0 * ahead_ahead - east_east - north_north),
        HARMONIC_TWO[3] * east * ahead,
        HARMONIC_TWO[4] * (east_east - north_north),
        HARMONIC_THREE[0] * north * (3.0 * east_east - north_north),
        HARMONIC_THREE[1] * east * north * ahead,
        HARMONIC_THREE[2] * north * (4.0 * ahead_ahead - east_east - north_north),
        HARMONIC_THREE[3] * ahead * (2.0 * ahead_ahead - 3.0 * east_east - 3.0 * north_north),
        HARMONIC_THREE[4] * east * (4.0 * ahead_ahead - east_east - north_north),
        HARMONIC_THREE[5] * ahead * (east_east - north_north),
        HARMONIC_THREE[6] * east * (east_east - 3.0 * north_north),
    ]


def pixel_basis():
    j = np.arange(PIXELS)
    x = j % SIDE + 0.5 - SIDE / 2
    y = j // SIDE + 0.5 - SIDE / 2
    rows = np.stack([x * x, x * y, y * y, x, y, np.ones_like(x), 0 * x, 0 * x])
    return np.concatenate([rows, rows, rows, 0 * rows]).astype(np.float32)


def lane_order(block):
    row = np.arange(block)
    splat = (row % 8) * (block // 8) + row // 8
    return (np.arange(block)[:, None] == splat[None, :]).astype(np.float32)


def rounded(x):
    return x.astype(BF16).astype(F32)


def shifted(x, shift):
    return pltpu.roll(x, shift % 8, 0)


def blend_kernel(
    cap, pairs_ref, place_ref, order_ref, basis_ref, arrived_ref, target_ref, image_ref, grad_ref,
    screen, owed, hue_sum, hue_back, alphas, slopes, steps, resid, parts, moments, *banks,
):
    tiles = target_ref.shape[1]
    depth = pairs_ref.shape[0] - PAIR
    slots = cap * arrived_ref.shape[0]
    block = arrived_ref.shape[2]
    chunks = block // 8
    lanes = range(GROUP)
    spots = [(t, e) for e in range(PAIR) for t in lanes]
    keeps, weights, halves, ends = (banks[GROUP * i : GROUP * i + GROUP] for i in range(4))
    sub = lax.broadcasted_iota(jnp.int32, (8, PIXELS), 0)

    resid[...] = jnp.zeros_like(resid)
    parts[...] = jnp.zeros_like(parts)

    def prepare(o, _):
        for i in range(cap):
            s = cap * o + i
            owed[s] = jnp.zeros((16, block), F32)
            last = arrived_ref[o, 8 * cap + i : 8 * cap + i + 1]
            screen[s, 0:8] = arrived_ref[o, 8 * i : 8 * i + 8]
            screen[s, 8:9] = last
            hue = jnp.concatenate(
                [arrived_ref[o, 8 * i + 6 : 8 * i + 8], last, jnp.zeros((5, block), F32)], axis=0
            )
            hue1 = rounded(hue)
            hue2 = hue - hue1
            zero = jnp.zeros_like(hue)
            hue_sum[s] = jnp.concatenate(
                [
                    jnp.concatenate([hue1, hue1], axis=1),
                    jnp.concatenate([hue2, zero], axis=1),
                ],
                axis=0,
            ).astype(BF16)
            hue_back[s] = jnp.concatenate([hue1, hue2, hue1, zero], axis=0).astype(BF16)
        return 0

    lax.fori_loop(0, arrived_ref.shape[0], prepare, 0)
    owed[slots] = jnp.zeros((16, block), F32)
    screen[slots] = jnp.zeros((16, block), F32)
    screen[slots, 5:6] = jnp.full((1, block), DEAD, F32)
    hue_sum[slots] = jnp.zeros((16, 2 * block), BF16)
    hue_back[slots] = jnp.zeros((32, block), BF16)

    basis = basis_ref[...].astype(BF16)
    monomials = basis_ref[0:8].astype(BF16)
    zero_row = jnp.zeros((8, PIXELS), F32)

    def group(step, _):
        row = [order_ref[0, step * GROUP + t] for t in lanes]
        deepest = jnp.int32(0)
        for k in range(depth):
            deepest = deepest + (pairs_ref[k, row[0]] >= 0).astype(jnp.int32)
        turns = lax.div(deepest + (PAIR - 1), PAIR)
        centre = []
        for t in lanes:
            tile = place_ref[row[t]]
            cx = (lax.rem(tile, TX) * SIDE + SIDE // 2).astype(F32)
            cy = (lax.div(tile, TX) * SIDE + SIDE // 2).astype(F32)
            centre.append((cx, cy))

        def place(t, k):
            slot = pairs_ref[k, row[t]]
            return jnp.where(slot >= 0, slot, slots)

        def shape_up(j):
            for t, e in spots:
                cx, cy = centre[t]
                s = place(t, PAIR * j + e)
                u = screen[s, 0:1] - cx
                v = screen[s, 1:2] - cy
                a, b, c = screen[s, 2:3], screen[s, 3:4], screen[s, 4:5]
                opac = jnp.maximum(screen[s, 5:6], DEAD)
                lin_x = a * u + b * v
                lin_y = b * u + c * v
                const = opac - 0.5 * (lin_x * u + lin_y * v)
                for r, value in enumerate((-0.5 * a, -b, -0.5 * c, lin_x, lin_y, const)):
                    parts[e, t, r : r + 1] = LOG2E * value

        shape_up(0)

        def power_of(t, e):
            c = parts[e, t]
            c1 = rounded(c)
            c2 = rounded(c - c1)
            c3 = c - c1 - c2
            left = jnp.concatenate([c1, c2, c3, jnp.zeros_like(c)], axis=0).astype(BF16)
            return lax.dot_general(
                left, basis, (((0,), (0,)), ((), ())), preferred_element_type=F32
            )

        def draw(t, j, e, power):
            alpha = jnp.exp2(power)
            alphas[e, t] = alpha
            keep = 1.0 - alpha
            keeps[t][j, e] = keep
            kept = keep[0:8]
            for i in range(1, chunks):
                kept = kept * keep[8 * i : 8 * i + 8]
            return kept

        def scan_of(t, j, e, kept, trans):
            scan = jnp.where(sub == 0, trans, shifted(kept, 1))
            for d in (1, 2, 4):
                scan = scan * jnp.where(sub < d, 1.0, shifted(scan, d))
            end = scan * kept
            ends[t][j, e] = end
            return scan, jnp.broadcast_to(end[7:8], (8, PIXELS))

        def spread(t, j, e, here):
            for i in range(0, chunks, 2):
                lo, mid, hi = 8 * i, 8 * i + 8, 8 * i + 16
                one = alphas[e, t, lo:mid] * here
                here = here * keeps[t][j, e, lo:mid]
                two = alphas[e, t, mid:hi] * here
                here = here * keeps[t][j, e, mid:hi]
                pair = jnp.concatenate([one, two], axis=0)
                weights[t][j, e, lo:hi] = pair
                high = pair.astype(BF16)
                halves[t][j, e, lo:hi] = high
                halves[t][j, e, block + lo : block + hi] = (pair - high.astype(F32)).astype(BF16)

        def summed(t, j, e):
            return jnp.dot(
                hue_sum[place(t, PAIR * j + e)], halves[t][j, e], preferred_element_type=F32
            )

        def forward(j, carry):
            trans = [carry[2 * t] for t in lanes]
            totals = [carry[2 * t + 1] for t in lanes]
            powers = [[power_of(t, e) for t in lanes] for e in range(PAIR)]
            kepts = [draw(t, j, 0, powers[0][t]) for t in lanes]
            for e in range(PAIR):
                heres = []
                for t in lanes:
                    here, trans[t] = scan_of(t, j, e, kepts[t], trans[t])
                    heres.append(here)
                for t in lanes:
                    spread(t, j, e, heres[t])
                    if e + 1 < PAIR:
                        kepts[t] = draw(t, j, e + 1, powers[e + 1][t])
                totals = [totals[t] + summed(t, j, e) for t in lanes]
            shape_up(j + 1)
            return tuple(x for t in lanes for x in (trans[t], totals[t]))

        start = (jnp.ones((8, PIXELS), F32), jnp.zeros((16, PIXELS), F32)) * GROUP
        done = lax.fori_loop(0, turns, forward, start)

        pulls = []
        for t in lanes:
            total = done[2 * t + 1]
            image = (total[0:8] + total[8:16])[0:3]
            for h in range(3):
                image_ref[h, pl.ds(row[t], 1)] = image[h : h + 1]
                resid[t, h : h + 1] = (image[h : h + 1] - target_ref[h, pl.ds(row[t], 1)]) * (
                    2.0 / 512.0
                )
            g = resid[t]
            g1 = rounded(g)
            g2 = g - g1
            pulls.append(
                (
                    jnp.concatenate([g1, g1, g2, zero_row], axis=0).astype(BF16),
                    jnp.concatenate([g1, g2], axis=0).astype(BF16),
                )
            )

        def lean(t, j, e):
            slopes[e, t] = lax.dot_general(
                hue_back[place(t, PAIR * j + e)],
                pulls[t][0],
                (((0,), (0,)), ((), ())),
                preferred_element_type=F32,
            )

        def behind_of(t, j, e, behind):
            run = weights[t][j, e, 0:8] * slopes[e, t, 0:8]
            for i in range(1, chunks):
                lo, hi = 8 * i, 8 * i + 8
                run = run + weights[t][j, e, lo:hi] * slopes[e, t, lo:hi]
            scan = jnp.where(sub == 7, behind, shifted(run, -1))
            for d in (1, 2, 4):
                scan = scan + jnp.where(sub < 8 - d, shifted(scan, -d), 0.0)
            return (
                scan / jnp.maximum(ends[t][j, e], 1e-37),
                jnp.broadcast_to((run + scan)[0:1], (8, PIXELS)),
            )

        def step_of(t, j, e, here):
            for i in range(chunks - 2, -1, -2):
                lo, mid, hi = 8 * i, 8 * i + 8, 8 * i + 16
                ahead = slopes[e, t, mid:hi]
                gap = ahead - here
                two = weights[t][j, e, mid:hi] * gap
                here = ahead - keeps[t][j, e, mid:hi] * gap
                ahead = slopes[e, t, lo:mid]
                gap = ahead - here
                one = weights[t][j, e, lo:mid] * gap
                here = ahead - keeps[t][j, e, lo:mid] * gap
                pair = jnp.concatenate([one, two], axis=0)
                high = pair.astype(BF16)
                steps[e, t, lo:hi] = high
                steps[e, t, block + lo : block + hi] = (pair - high.astype(F32)).astype(BF16)

        def settle(j):
            for t, e in spots:
                cx, cy = centre[t]
                s = place(t, PAIR * j + e)
                u = screen[s, 0:1] - cx
                v = screen[s, 1:2] - cy
                a, b, c = screen[s, 2:3], screen[s, 3:4], screen[s, 4:5]
                mxx, mxy, myy, mx, my, m = (moments[e, t, r : r + 1] for r in range(6))
                off_x = mx - u * m
                off_y = my - v * m
                changes = (
                    a * off_x + b * off_y,
                    b * off_x + c * off_y,
                    -0.5 * (mxx - u * (mx + off_x)),
                    -(mxy - u * my - v * off_x),
                    -0.5 * (myy - v * (my + off_y)),
                    m,
                    moments[e, t, 8:9],
                    moments[e, t, 9:10],
                    moments[e, t, 10:11],
                )
                for r, change in enumerate(changes):
                    owed[s, r : r + 1] = owed[s, r : r + 1] + change

        def backward(index, carry):
            j = turns - 1 - index
            behind = list(carry)
            settle(j + 1)
            places = []
            for e in reversed(range(PAIR)):
                for t in lanes:
                    lean(t, j, e)
            for e in reversed(range(PAIR)):
                for t in lanes:
                    hues = lax.dot_general(
                        pulls[t][1], halves[t][j, e], (((1,), (1,)), ((), ())),
                        preferred_element_type=F32,
                    )
                    places.append(
                        (t, e, 8, hues[0:8, 0:block] + hues[0:8, block:] + hues[8:16, 0:block])
                    )
                heres = []
                for t in lanes:
                    here, behind[t] = behind_of(t, j, e, behind[t])
                    heres.append(here)
                for t in lanes:
                    step_of(t, j, e, heres[t])
                for t in lanes:
                    sums = lax.dot_general(
                        monomials, steps[e, t], (((1,), (1,)), ((), ())), preferred_element_type=F32
                    )
                    places.append((t, e, 0, sums[:, 0:block] + sums[:, block:]))
            for t, e, at, value in places:
                moments[e, t, at : at + 8] = value
            return tuple(behind)

        lax.fori_loop(0, turns, backward, (jnp.zeros((8, PIXELS), F32),) * GROUP)

        settle(0)
        return 0

    lax.fori_loop(0, tiles // GROUP, group, 0)

    def pack(o):
        for i in range(cap):
            grad_ref[o, 8 * i : 8 * i + 8] = owed[cap * o + i, 0:8]
            grad_ref[o, 8 * cap + i : 8 * cap + i + 1] = owed[cap * o + i, 8:9]

    each(0, arrived_ref.shape[0], pack)


def blend(arrived, cap, target, tile_place, pairs, order):
    channels, tiles, pixels = target.shape
    devices, rows, block = arrived.shape
    slots = devices * cap
    turns = pairs.shape[0] // PAIR
    basis = jnp.asarray(pixel_basis())
    smem = pl.BlockSpec(memory_space=pltpu.SMEM)
    vmem = pl.BlockSpec(memory_space=pltpu.VMEM)
    return pl.pallas_call(
        functools.partial(blend_kernel, cap),
        in_specs=[smem, smem, smem, vmem, vmem, vmem],
        out_specs=[vmem, vmem],
        scratch_shapes=[
            pltpu.VMEM((slots + 1, 16, block), F32),
            pltpu.VMEM((slots + 1, 16, block), F32),
            pltpu.VMEM((slots + 1, 16, 2 * block), BF16),
            pltpu.VMEM((slots + 1, 32, block), BF16),
            pltpu.VMEM((PAIR, GROUP, block, pixels), F32),
            pltpu.VMEM((PAIR, GROUP, block, pixels), F32),
            pltpu.VMEM((PAIR, GROUP, 2 * block, pixels), BF16),
            pltpu.VMEM((GROUP, 8, pixels), F32),
            pltpu.VMEM((PAIR, GROUP, 8, block), F32),
            pltpu.VMEM((PAIR, GROUP, 16, block), F32),
        ]
        + [pltpu.VMEM((turns, PAIR, block, pixels), F32)] * GROUP
        + [pltpu.VMEM((turns, PAIR, block, pixels), F32)] * GROUP
        + [pltpu.VMEM((turns, PAIR, 2 * block, pixels), BF16)] * GROUP
        + [pltpu.VMEM((turns, PAIR, 8, pixels), F32)] * GROUP,
        out_shape=[
            jax.ShapeDtypeStruct(target.shape, F32),
            jax.ShapeDtypeStruct((devices, rows, block), F32),
        ],
        name="blend",
        compiler_params=pltpu.CompilerParams(),
    )(pairs, tile_place, order, basis, arrived, target)


def whereabouts(sizes):
    nx, ny = sizes
    me = lax.axis_index("gx") * ny + lax.axis_index("gy")

    def other(n):
        o = lax.rem(me + n, nx * ny)
        return o, (lax.div(o, ny), lax.rem(o, ny))

    return me, nx * ny, other


def each(start, stop, body, width=4):
    whole = (stop - start) // width

    def some(c, _):
        for w in range(width):
            body(start + width * c + w)
        return 0

    lax.fori_loop(0, whole, some, 0)
    for n in range(start + width * whole, stop):
        body(n)


def greet(devices, other):
    barrier = pltpu.get_barrier_semaphore()

    def call(n):
        pl.semaphore_signal(
            barrier, inc=1, device_id=other(n)[1], device_id_type=pl.DeviceIdType.MESH
        )

    each(1, devices, call)
    return barrier


def post(source, target, sems, where):
    return pltpu.make_async_remote_copy(
        src_ref=source,
        dst_ref=target,
        send_sem=sems.at[0],
        recv_sem=sems.at[1],
        device_id=where,
        device_id_type=pl.DeviceIdType.MESH,
    )


def order_rows(pairs, order_ref):
    depth, tiles = pairs.shape
    live = jnp.sum((pairs >= 0).astype(F32), axis=0, keepdims=True)
    across = lax.broadcasted_iota(jnp.int32, (tiles, tiles), 1).astype(F32)
    down = lax.broadcasted_iota(jnp.int32, (tiles, tiles), 0).astype(F32)
    theirs = jnp.broadcast_to(live, (tiles, tiles))
    mine = jnp.sum(jnp.where(across == down, theirs, 0.0), axis=1, keepdims=True)
    before = (theirs > mine) | ((theirs == mine) & (across < down))
    rank = jnp.sum(before.astype(F32), axis=1, keepdims=True)
    order = jnp.sum(jnp.where(rank == across, down, 0.0), axis=0, keepdims=True)
    order_ref[...] = order.astype(jnp.int32)


def fetch_kernel(
    sizes, width, height, splats_ref, fetch_ref, pairs_ref, order_ref,
    arrived_ref, rows_ref, lists_ref, asked,
    raw, wants, lists, mix, own, send, ask, heard, ask_sems, sems, local_sems,
):
    me, devices, other = whereabouts(sizes)
    cap = fetch_ref.shape[0]
    _, blocks, block = raw.shape
    used = 9 * cap
    barrier = greet(devices, other)
    loads = [
        pltpu.make_async_copy(source, target, local_sems.at[n])
        for n, (source, target) in enumerate(
            ((fetch_ref, wants), (pairs_ref, lists), (splats_ref, raw), (order_ref, mix))
        )
    ]
    for load in loads:
        load.start()

    loads[0].wait()
    table = jnp.concatenate([wants[...], jnp.zeros((8 - cap, devices), jnp.int32)], axis=0)
    if devices % 128:
        table = jnp.concatenate(
            [table, jnp.zeros((8, 128 - devices % 128), jnp.int32)], axis=1
        )
    table = jnp.transpose(table.astype(F32))[0:devices]
    ask[...] = jnp.zeros_like(ask)
    ask[:, :, 0:8] = table.astype(jnp.int32).reshape(devices, 1, 8)

    pl.semaphore_wait(barrier, devices - 1)

    def inquire(n):
        o, where = other(n)
        post(ask.at[o], asked.at[me], ask_sems, where).start()

    each(1, devices, inquire)
    keep = pltpu.make_async_copy(ask.at[me], asked.at[me], local_sems.at[0])
    keep.start()
    keep.wait()
    rest = pl.ds(0, devices - 1)
    bulk = post(ask.at[rest], asked.at[rest], ask_sems, other(1)[1])
    loads[1].wait()
    order_rows(lists[...], rows_ref)
    depth = lists.shape[0]
    lists_ref[...] = jnp.full(lists_ref.shape, -1, jnp.int32)
    lists_ref[0:depth] = lists[...]
    loads[2].wait()
    loads[3].wait()
    place_x, place_y, place_z = raw[0], raw[1], raw[2]
    inverse_one = jnp.exp(-2.0 * raw[3])
    inverse_two = jnp.exp(-2.0 * raw[4])
    cosine = jnp.cos(raw[5])
    sine = jnp.sin(raw[5])
    length = jnp.sqrt(place_x * place_x + place_y * place_y + place_z * place_z)
    terms = harmonic_terms(place_x / length, place_y / length, place_z / length)
    lines = [
        width * place_x / place_z + 0.5 * width,
        width * place_y / place_z + 0.5 * height,
        cosine * cosine * inverse_one + sine * sine * inverse_two,
        cosine * sine * (inverse_one - inverse_two),
        sine * sine * inverse_one + cosine * cosine * inverse_two,
        jnp.minimum(raw[6], 0.0) - jnp.log1p(jnp.exp(-jnp.abs(raw[6]))),
    ]
    for h in range(3):
        color = jnp.full((blocks, block), 0.5, F32)
        for k in range(16):
            color = color + raw[7 + 16 * h + k] * terms[k]
        lines.append(color)
    order = mix[...].astype(BF16)
    for j, line in enumerate(lines):
        one = rounded(line)
        two = rounded(line - one)
        three = line - one - two
        stack = jnp.concatenate([one, two, three], axis=0).astype(BF16)
        mixed = jnp.dot(stack, order, preferred_element_type=F32)
        mixed = mixed[0:blocks] + mixed[blocks : 2 * blocks] + mixed[2 * blocks :]
        own[:, j, :] = mixed

    bulk.wait_recv()
    load = pltpu.make_async_copy(asked, heard, local_sems.at[1])
    load.start()
    load.wait()

    def pick(o):
        for i in range(cap):
            b = jnp.clip(heard[o, 0, i], 0, blocks - 1)
            send[o, 8 * i : 8 * i + 8] = own[b, 0:8]
            send[o, 8 * cap + i : 8 * cap + i + 1] = own[b, 8:9]

    part = pl.ds(0, used)

    def serve(n):
        o, where = other(n)
        post(send.at[o, part], arrived_ref.at[me, part], sems, where).start()

    lag = 4
    width = 4
    turns = (devices - 1 - lag) // width
    for n in range(1, 1 + lag):
        pick(other(n)[0])

    def run(c, _):
        for w in range(width):
            pick(other(1 + lag + width * c + w)[0])
        for w in range(width):
            serve(1 + width * c + w)
        return 0

    lax.fori_loop(0, turns, run, 0)
    for n in range(1 + lag + width * turns, devices):
        pick(other(n)[0])
    pick(me)
    for n in range(1 + width * turns, devices):
        serve(n)
    keep = pltpu.make_async_copy(send.at[me], arrived_ref.at[me], local_sems.at[0])
    keep.start()
    bulk.wait_send()
    whole = post(send.at[rest, part], arrived_ref.at[rest, part], sems, other(1)[1])
    whole.wait_recv()
    whole.wait_send()
    keep.wait()


def fetch_blocks(splats, fetch, pairs, sizes, width, height):
    _, blocks, block = splats.shape
    cap, devices = fetch.shape
    rows = 8 * pl.cdiv(9 * cap, 8)
    order = jnp.asarray(lane_order(block))
    depth = PAIR * pl.cdiv(pairs.shape[0], PAIR)
    vmem = pl.BlockSpec(memory_space=pltpu.VMEM)
    anywhere = pl.BlockSpec(memory_space=pl.ANY)
    return pl.pallas_call(
        functools.partial(fetch_kernel, sizes, width, height),
        in_specs=[anywhere] * 4,
        out_specs=[anywhere] + [vmem] * 3,
        scratch_shapes=[
            pltpu.VMEM(splats.shape, F32),
            pltpu.VMEM(fetch.shape, jnp.int32),
            pltpu.VMEM(pairs.shape, jnp.int32),
            pltpu.VMEM(order.shape, F32),
            pltpu.VMEM((blocks, 16, block), F32),
            pltpu.VMEM((devices, rows, block), F32),
            pltpu.VMEM((devices, 1, 128), jnp.int32),
            pltpu.SMEM((devices, 1, 128), jnp.int32),
            pltpu.SemaphoreType.DMA((2,)),
            pltpu.SemaphoreType.DMA((2,)),
            pltpu.SemaphoreType.DMA((4,)),
        ],
        out_shape=[
            jax.ShapeDtypeStruct((devices, rows, block), F32),
            jax.ShapeDtypeStruct((1, pairs.shape[1]), jnp.int32),
            jax.ShapeDtypeStruct((depth + PAIR, pairs.shape[1]), jnp.int32),
            jax.ShapeDtypeStruct((devices, 1, 128), jnp.int32),
        ],
        name="fetch",
        compiler_params=pltpu.CompilerParams(collective_id=0, has_side_effects=True),
    )(splats, fetch, pairs, order)


def thirds(x):
    one = rounded(x)
    two = rounded(x - one)
    return [one, two, x - one - two]


def return_kernel(
    sizes, cap, blocks, grad_ref, asked_ref, order_ref, total_ref,
    returned, asked, mix, sems, local_sems,
):
    me, devices, other = whereabouts(sizes)
    barrier = greet(devices, other)
    rows = grad_ref.shape[1]
    used = 9 * cap
    spot = pl.ds(pl.multiple_of(me * rows, 8), rows)
    loads = [
        pltpu.make_async_copy(source, target, local_sems.at[n])
        for n, (source, target) in enumerate(
            ((grad_ref.at[me], returned.at[spot]), (asked_ref, asked), (order_ref, mix))
        )
    ]
    for load in loads:
        load.start()
    for load in loads:
        load.wait()
    lane = lax.broadcasted_iota(jnp.int32, (devices, blocks), 1)
    owners = []
    for i in range(cap):
        column = jnp.broadcast_to(asked[:, 0, i : i + 1], (devices, blocks))
        owners += [(column == lane).astype(F32)] * 3
    owners = jnp.concatenate(owners, axis=0).astype(BF16)
    order = mix[...].astype(BF16)
    pl.semaphore_wait(barrier, devices - 1)
    part = pl.ds(0, used)
    land = pl.ds(pl.multiple_of(me * rows, 8), used)

    def serve(n):
        o, where = other(n)
        post(grad_ref.at[o, part], returned.at[land], sems, where).start()

    each(1, devices, serve)
    rest = pl.ds(0, devices - 1)
    bulk = returned.at[pl.ds(0, (devices - 1) * used)]
    post(bulk, bulk, sems, other(1)[1]).wait_recv()
    for r in range(9):
        terms = []
        for i in range(cap):
            at = 8 * i + r if r < 8 else 8 * cap + i
            terms += thirds(returned[pl.ds(at, devices, stride=rows), :])
        summed = lax.dot_general(
            owners,
            jnp.concatenate(terms, axis=0).astype(BF16),
            (((0,), (0,)), ((), ())),
            preferred_element_type=F32,
        )
        mixed = lax.dot_general(
            jnp.concatenate(thirds(summed), axis=0).astype(BF16),
            order,
            (((1,), (1,)), ((), ())),
            preferred_element_type=F32,
        )
        total_ref[r] = mixed[0:blocks] + mixed[blocks : 2 * blocks] + mixed[2 * blocks :]
    sent = grad_ref.at[rest, part]
    post(sent, sent, sems, other(1)[1]).wait_send()


def return_grads(grads, asked, cap, blocks, sizes):
    devices, rows, block = grads.shape
    order = jnp.asarray(lane_order(block))
    vmem = pl.BlockSpec(memory_space=pltpu.VMEM)
    return pl.pallas_call(
        functools.partial(return_kernel, sizes, cap, blocks),
        in_specs=[pl.BlockSpec(memory_space=pl.ANY)] * 3,
        out_specs=vmem,
        scratch_shapes=[
            pltpu.VMEM((devices * rows, block), F32),
            pltpu.VMEM(asked.shape, jnp.int32),
            pltpu.VMEM(order.shape, F32),
            pltpu.SemaphoreType.DMA((2,)),
            pltpu.SemaphoreType.DMA((3,)),
        ],
        out_shape=jax.ShapeDtypeStruct((9, blocks, block), F32),
        name="give_back",
        compiler_params=pltpu.CompilerParams(collective_id=1, has_side_effects=True),
    )(grads, asked, order)


def outline(width, height, x, y, z, first, second, angle):
    inverse_one = jnp.exp(-2.0 * first)
    inverse_two = jnp.exp(-2.0 * second)
    cosine = jnp.cos(angle)
    sine = jnp.sin(angle)
    return (
        width * x / z + 0.5 * width,
        width * y / z + 0.5 * height,
        cosine * cosine * inverse_one + sine * sine * inverse_two,
        cosine * sine * (inverse_one - inverse_two),
        sine * sine * inverse_one + cosine * cosine * inverse_two,
    )


def directions(x, y, z):
    length = jnp.sqrt(x * x + y * y + z * z)
    return tuple(harmonic_terms(x / length, y / length, z / length))


def adam_kernel(
    width, height, total_ref, splats_ref, one_ref, two_ref, grad_ref, step_ref,
    raw, one, two, grad, step, load_sems, store_sems,
):
    count = raw.shape[0]
    cuts = [0, 7] + [7 + 16 * h for h in range(1, 4)]
    spans = [pl.ds(lo, hi - lo) for lo, hi in zip(cuts, cuts[1:])]
    load = pltpu.make_async_copy(splats_ref, raw, load_sems.at[0])
    load.start()
    loads = []
    for n, span in enumerate(spans[1:] + spans[:1]):
        pair = [
            pltpu.make_async_copy(one_ref.at[span], one.at[span], load_sems.at[1 + 2 * n]),
            pltpu.make_async_copy(two_ref.at[span], two.at[span], load_sems.at[2 + 2 * n]),
        ]
        for copy in pair:
            copy.start()
        loads.append(pair)
    load.wait()
    place = (raw[0], raw[1], raw[2])
    terms, turn = jax.vjp(directions, *place)
    slants = [jnp.zeros_like(place[0]) for _ in terms]
    stores = []

    def finish(n, span, lo, hi):
        for copy in loads[n]:
            copy.wait()
        for r in range(lo, hi):
            change = grad[r]
            first = 0.9 * one[r] + 0.1 * change
            second = 0.999 * two[r] + 0.001 * change * change
            step[r] = first / (second * lax.rsqrt(second) + 1e-08)
        for m, (source, target) in enumerate(((grad, grad_ref), (step, step_ref))):
            copy = pltpu.make_async_copy(
                source.at[span], target.at[span], store_sems.at[2 * n + m]
            )
            copy.start()
            stores.append(copy)

    for h in range(3):
        hue = total_ref[6 + h]
        for k in range(16):
            r = 7 + 16 * h + k
            grad[r] = hue * terms[k]
            slants[k] = slants[k] + hue * raw[r]
        finish(h, spans[1 + h], cuts[1 + h], cuts[2 + h])
    _, pull = jax.vjp(
        functools.partial(outline, width, height), *place, raw[3], raw[4], raw[5]
    )
    flat = pull(tuple(total_ref[j] for j in range(5)))
    tilt = turn(tuple(slants))
    for j in range(3):
        grad[j] = flat[j] + tilt[j]
    for j in range(3, 6):
        grad[j] = flat[j]
    grad[6] = total_ref[5] / (1.0 + jnp.exp(raw[6]))
    finish(3, spans[0], 0, 7)
    for copy in stores:
        copy.wait()


def adam(total, splats, moment_one, moment_two, width, height):
    anywhere = pl.BlockSpec(memory_space=pl.ANY)
    vmem = pl.BlockSpec(memory_space=pltpu.VMEM)
    like = jax.ShapeDtypeStruct(splats.shape, F32)
    return pl.pallas_call(
        functools.partial(adam_kernel, width, height),
        in_specs=[vmem, anywhere, anywhere, anywhere],
        out_specs=[anywhere, anywhere],
        scratch_shapes=[pltpu.VMEM(splats.shape, F32)] * 5
        + [pltpu.SemaphoreType.DMA((9,)), pltpu.SemaphoreType.DMA((8,))],
        out_shape=[like, like],
        name="adam",
    )(total, splats, moment_one, moment_two)


def local(splats, moment_one, moment_two, target, tile_place, pairs, fetch):
    sizes = (lax.axis_size("gx"), lax.axis_size("gy"))
    devices = sizes[0] * sizes[1]
    tiles_here = target.shape[0]
    cap = fetch.shape[2]
    width = 16.0 * TX
    height = 16.0 * (tiles_here * devices // TX)

    rows_first = jnp.transpose(splats, (1, 0, 2))
    asks = jnp.transpose(fetch[0])
    arrived, rows, lists, asked = fetch_blocks(
        rows_first, asks, jnp.transpose(pairs), sizes, width, height
    )
    image, grads = blend(
        arrived, cap, jnp.transpose(target, (1, 0, 2)), tile_place, lists, rows
    )
    total = return_grads(grads, asked, cap, splats.shape[0], sizes)
    splat_grad, adam_step = adam(
        total,
        rows_first,
        jnp.transpose(moment_one, (1, 0, 2)),
        jnp.transpose(moment_two, (1, 0, 2)),
        width,
        height,
    )
    back = lambda x: jnp.transpose(x, (1, 0, 2))
    return (back(image), back(splat_grad), back(adam_step))


def solution(mesh):
    both = ("gx", "gy")
    return jax.shard_map(
        local,
        mesh=mesh,
        in_specs=(
            P(both, None, None),
            P(both, None, None),
            P(both, None, None),
            P(both, None, None),
            P(both),
            P(both, None),
            P(both, None, None),
        ),
        out_specs=(P(both, None, None), P(both, None, None), P(both, None, None)),
        check_vma=False,
    )
```

```python
import functools

import jax
import jax.numpy as jnp
import numpy as np
from jax import lax
from jax.experimental import pallas as pl
from jax.experimental.pallas import tpu as pltpu
from jax.sharding import PartitionSpec as P

TX = 16
SIDE = 16
PIXELS = SIDE * SIDE
LOG2E = 1.4426950408889634
DEAD = -1.0e4
GROUP = 2
PAIR = 4
F32 = jnp.float32
BF16 = jnp.bfloat16


HARMONIC_ZERO = 0.28209479177387814
HARMONIC_ONE = 0.4886025119029199
HARMONIC_TWO = (
    1.0925484305920792,
    -1.0925484305920792,
    0.31539156525252005,
    -1.0925484305920792,
    0.5462742152960396,
)
HARMONIC_THREE = (
    -0.5900435899266435,
    2.890611442640554,
    -0.4570457994644658,
    0.3731763325901154,
    -0.4570457994644658,
    1.445305721320277,
    -0.5900435899266435,
)


def harmonic_terms(east, north, ahead):
    east_east = east * east
    north_north = north * north
    ahead_ahead = ahead * ahead
    return [
        jnp.full_like(east, HARMONIC_ZERO),
        -HARMONIC_ONE * north,
        HARMONIC_ONE * ahead,
        -HARMONIC_ONE * east,
        HARMONIC_TWO[0] * east * north,
        HARMONIC_TWO[1] * north * ahead,
        HARMONIC_TWO[2] * (2.0 * ahead_ahead - east_east - north_north),
        HARMONIC_TWO[3] * east * ahead,
        HARMONIC_TWO[4] * (east_east - north_north),
        HARMONIC_THREE[0] * north * (3.0 * east_east - north_north),
        HARMONIC_THREE[1] * east * north * ahead,
        HARMONIC_THREE[2] * north * (4.0 * ahead_ahead - east_east - north_north),
        HARMONIC_THREE[3] * ahead * (2.0 * ahead_ahead - 3.0 * east_east - 3.0 * north_north),
        HARMONIC_THREE[4] * east * (4.0 * ahead_ahead - east_east - north_north),
        HARMONIC_THREE[5] * ahead * (east_east - north_north),
        HARMONIC_THREE[6] * east * (east_east - 3.0 * north_north),
    ]


def pixel_basis():
    j = np.arange(PIXELS)
    x = j % SIDE + 0.5 - SIDE / 2
    y = j // SIDE + 0.5 - SIDE / 2
    rows = np.stack([x * x, x * y, y * y, x, y, np.ones_like(x), 0 * x, 0 * x])
    return np.concatenate([rows, rows, rows, 0 * rows]).astype(np.float32)


def lane_order(block):
    row = np.arange(block)
    splat = (row % 8) * (block // 8) + row // 8
    return (np.arange(block)[:, None] == splat[None, :]).astype(np.float32)


def rounded(x):
    return x.astype(BF16).astype(F32)


def shifted(x, shift):
    return pltpu.roll(x, shift % 8, 0)


def blend_kernel(
    cap, pairs_ref, place_ref, order_ref, basis_ref, arrived_hbm, target_hbm, image_hbm, grad_hbm,
    arrived_ref, target_ref, image_ref, grad_ref, sems, screen, owed, hue_sum, hue_back, resid, parts, moments, *banks,
):
    tiles = target_ref.shape[1]
    depth = pairs_ref.shape[0] - PAIR
    slots = cap * arrived_ref.shape[0]
    block = arrived_ref.shape[2]
    chunks = block // 8
    lanes = range(GROUP)
    spots = [(t, e) for e in range(PAIR) for t in lanes]
    many = GROUP * PAIR
    keeps, weights, halves, ends, alphas, slopes, steps = (
        [banks[many * i + PAIR * t : many * i + PAIR * t + PAIR] for t in lanes] for i in range(7)
    )
    sub = lax.broadcasted_iota(jnp.int32, (8, PIXELS), 0)
    devices = arrived_ref.shape[0]
    cuts = 4 if devices % 4 == 0 else 1
    share = devices // cuts
    spans = [pl.ds(share * c, share) for c in range(cuts)]
    loads = [
        pltpu.make_async_copy(arrived_hbm.at[span], arrived_ref.at[span], sems.at[c])
        for c, span in enumerate(spans)
    ]
    loads.append(pltpu.make_async_copy(target_hbm, target_ref, sems.at[cuts]))
    for load in loads:
        load.start()

    resid[...] = jnp.zeros_like(resid)
    parts[...] = jnp.zeros_like(parts)

    def prepare(o, _):
        for i in range(cap):
            s = cap * o + i
            owed[s] = jnp.zeros((16, block), F32)
            last = arrived_ref[o, 8 * cap + i : 8 * cap + i + 1]
            screen[s, 0:8] = arrived_ref[o, 8 * i : 8 * i + 8]
            screen[s, 8:9] = last
            hue = jnp.concatenate(
                [arrived_ref[o, 8 * i + 6 : 8 * i + 8], last, jnp.zeros((5, block), F32)], axis=0
            )
            hue1 = rounded(hue)
            hue2 = hue - hue1
            zero = jnp.zeros_like(hue)
            hue_sum[s] = jnp.concatenate(
                [
                    jnp.concatenate([hue1, hue1], axis=1),
                    jnp.concatenate([hue2, zero], axis=1),
                ],
                axis=0,
            ).astype(BF16)
            hue_back[s] = jnp.concatenate([hue1, hue2, hue1, zero], axis=0).astype(BF16)
        return 0

    for c in range(cuts):
        loads[c].wait()
        lax.fori_loop(share * c, share * (c + 1), prepare, 0)
    loads[cuts].wait()
    owed[slots] = jnp.zeros((16, block), F32)
    screen[slots] = jnp.zeros((16, block), F32)
    screen[slots, 5:6] = jnp.full((1, block), DEAD, F32)
    hue_sum[slots] = jnp.zeros((16, 2 * block), BF16)
    hue_back[slots] = jnp.zeros((32, block), BF16)

    basis = basis_ref[...].astype(BF16)
    monomials = basis_ref[0:8].astype(BF16)
    zero_row = jnp.zeros((8, PIXELS), F32)

    def group(step, _):
        row = [order_ref[0, step * GROUP + t] for t in lanes]
        deepest = jnp.int32(0)
        for k in range(depth):
            deepest = deepest + (pairs_ref[k, row[0]] >= 0).astype(jnp.int32)
        turns = lax.div(deepest + (PAIR - 1), PAIR)
        centre = []
        for t in lanes:
            tile = place_ref[row[t]]
            cx = (lax.rem(tile, TX) * SIDE + SIDE // 2).astype(F32)
            cy = (lax.div(tile, TX) * SIDE + SIDE // 2).astype(F32)
            centre.append((cx, cy))

        def place(t, k):
            slot = pairs_ref[k, row[t]]
            return jnp.where(slot >= 0, slot, slots)

        def shape_up(j):
            for t, e in spots:
                cx, cy = centre[t]
                s = place(t, PAIR * j + e)
                u = screen[s, 0:1] - cx
                v = screen[s, 1:2] - cy
                a, b, c = screen[s, 2:3], screen[s, 3:4], screen[s, 4:5]
                opac = jnp.maximum(screen[s, 5:6], DEAD)
                lin_x = a * u + b * v
                lin_y = b * u + c * v
                const = opac - 0.5 * (lin_x * u + lin_y * v)
                for r, value in enumerate((-0.5 * a, -b, -0.5 * c, lin_x, lin_y, const)):
                    parts[e, t, r : r + 1] = LOG2E * value

        shape_up(0)

        def power_of(t, e):
            c = parts[e, t]
            c1 = rounded(c)
            c2 = rounded(c - c1)
            c3 = c - c1 - c2
            left = jnp.concatenate([c1, c2, c3, jnp.zeros_like(c)], axis=0).astype(BF16)
            return lax.dot_general(
                left, basis, (((0,), (0,)), ((), ())), preferred_element_type=F32
            )

        def draw(t, j, e, power):
            alpha = jnp.exp2(power)
            alphas[t][e][0] = alpha
            keep = 1.0 - alpha
            keeps[t][e][j] = keep
            kept = keep[0:8]
            for i in range(1, chunks):
                kept = kept * keep[8 * i : 8 * i + 8]
            return kept

        def scan_of(t, j, e, kept, trans):
            scan = jnp.where(sub == 0, trans, shifted(kept, 1))
            for d in (1, 2, 4):
                scan = scan * jnp.where(sub < d, 1.0, shifted(scan, d))
            end = scan * kept
            ends[t][e][j] = end
            return scan, jnp.broadcast_to(end[7:8], (8, PIXELS))

        def spread(t, j, e, here):
            for i in range(0, chunks, 2):
                lo, mid, hi = 8 * i, 8 * i + 8, 8 * i + 16
                one = alphas[t][e][0, lo:mid] * here
                here = here * keeps[t][e][j, lo:mid]
                two = alphas[t][e][0, mid:hi] * here
                here = here * keeps[t][e][j, mid:hi]
                pair = jnp.concatenate([one, two], axis=0)
                weights[t][e][j, lo:hi] = pair
                high = pair.astype(BF16)
                halves[t][e][j, lo:hi] = high
                halves[t][e][j, block + lo : block + hi] = (pair - high.astype(F32)).astype(BF16)

        def summed(t, j, e):
            return jnp.dot(
                hue_sum[place(t, PAIR * j + e)], halves[t][e][j], preferred_element_type=F32
            )

        def forward(j, carry):
            trans = [carry[2 * t] for t in lanes]
            totals = [carry[2 * t + 1] for t in lanes]
            powers = [[power_of(t, e) for t in lanes] for e in range(PAIR)]
            kepts = [draw(t, j, 0, powers[0][t]) for t in lanes]
            for e in range(PAIR):
                heres = []
                for t in lanes:
                    here, trans[t] = scan_of(t, j, e, kepts[t], trans[t])
                    heres.append(here)
                for t in lanes:
                    spread(t, j, e, heres[t])
                    if e + 1 < PAIR:
                        kepts[t] = draw(t, j, e + 1, powers[e + 1][t])
                totals = [totals[t] + summed(t, j, e) for t in lanes]
            shape_up(j + 1)
            return tuple(x for t in lanes for x in (trans[t], totals[t]))

        start = (jnp.ones((8, PIXELS), F32), jnp.zeros((16, PIXELS), F32)) * GROUP
        done = lax.fori_loop(0, turns, forward, start)

        pulls = []
        for t in lanes:
            total = done[2 * t + 1]
            image = (total[0:8] + total[8:16])[0:3]
            for h in range(3):
                image_ref[h, pl.ds(row[t], 1)] = image[h : h + 1]
                resid[t, h : h + 1] = (image[h : h + 1] - target_ref[h, pl.ds(row[t], 1)]) * (
                    2.0 / 512.0
                )
            g = resid[t]
            g1 = rounded(g)
            g2 = g - g1
            pulls.append(
                (
                    jnp.concatenate([g1, g1, g2, zero_row], axis=0).astype(BF16),
                    jnp.concatenate([g1, g2], axis=0).astype(BF16),
                )
            )

        def lean(t, j, e):
            slopes[t][e][0] = lax.dot_general(
                hue_back[place(t, PAIR * j + e)],
                pulls[t][0],
                (((0,), (0,)), ((), ())),
                preferred_element_type=F32,
            )

        def behind_of(t, j, e, behind):
            run = weights[t][e][j, 0:8] * slopes[t][e][0, 0:8]
            for i in range(1, chunks):
                lo, hi = 8 * i, 8 * i + 8
                run = run + weights[t][e][j, lo:hi] * slopes[t][e][0, lo:hi]
            scan = jnp.where(sub == 7, behind, shifted(run, -1))
            for d in (1, 2, 4):
                scan = scan + jnp.where(sub < 8 - d, shifted(scan, -d), 0.0)
            return (
                scan / jnp.maximum(ends[t][e][j], 1e-37),
                jnp.broadcast_to((run + scan)[0:1], (8, PIXELS)),
            )

        def step_of(t, j, e, here):
            for i in range(chunks - 2, -1, -2):
                lo, mid, hi = 8 * i, 8 * i + 8, 8 * i + 16
                ahead = slopes[t][e][0, mid:hi]
                gap = ahead - here
                two = weights[t][e][j, mid:hi] * gap
                here = ahead - keeps[t][e][j, mid:hi] * gap
                ahead = slopes[t][e][0, lo:mid]
                gap = ahead - here
                one = weights[t][e][j, lo:mid] * gap
                here = ahead - keeps[t][e][j, lo:mid] * gap
                pair = jnp.concatenate([one, two], axis=0)
                high = pair.astype(BF16)
                steps[t][e][0, lo:hi] = high
                steps[t][e][0, block + lo : block + hi] = (pair - high.astype(F32)).astype(BF16)

        def settle(j):
            for t, e in spots:
                cx, cy = centre[t]
                s = place(t, PAIR * j + e)
                u = screen[s, 0:1] - cx
                v = screen[s, 1:2] - cy
                a, b, c = screen[s, 2:3], screen[s, 3:4], screen[s, 4:5]
                mxx, mxy, myy, mx, my, m = (moments[e, t, r : r + 1] for r in range(6))
                off_x = mx - u * m
                off_y = my - v * m
                changes = (
                    a * off_x + b * off_y,
                    b * off_x + c * off_y,
                    -0.5 * (mxx - u * (mx + off_x)),
                    -(mxy - u * my - v * off_x),
                    -0.5 * (myy - v * (my + off_y)),
                    m,
                    moments[e, t, 8:9],
                    moments[e, t, 9:10],
                    moments[e, t, 10:11],
                )
                for r, change in enumerate(changes):
                    owed[s, r : r + 1] = owed[s, r : r + 1] + change

        def backward(index, carry):
            j = turns - 1 - index
            behind = list(carry)
            settle(j + 1)
            places = []
            for e in reversed(range(PAIR)):
                for t in lanes:
                    lean(t, j, e)
            for e in reversed(range(PAIR)):
                for t in lanes:
                    hues = lax.dot_general(
                        pulls[t][1], halves[t][e][j], (((1,), (1,)), ((), ())),
                        preferred_element_type=F32,
                    )
                    places.append(
                        (t, e, 8, hues[0:8, 0:block] + hues[0:8, block:] + hues[8:16, 0:block])
                    )
                heres = []
                for t in lanes:
                    here, behind[t] = behind_of(t, j, e, behind[t])
                    heres.append(here)
                for t in lanes:
                    step_of(t, j, e, heres[t])
                for t in lanes:
                    sums = lax.dot_general(
                        monomials, steps[t][e][0], (((1,), (1,)), ((), ())), preferred_element_type=F32
                    )
                    places.append((t, e, 0, sums[:, 0:block] + sums[:, block:]))
            for t, e, at, value in places:
                moments[e, t, at : at + 8] = value
            return tuple(behind)

        lax.fori_loop(0, turns, backward, (jnp.zeros((8, PIXELS), F32),) * GROUP)

        settle(0)
        return 0

    lax.fori_loop(0, tiles // GROUP, group, 0)

    def pack(o):
        for i in range(cap):
            grad_ref[o, 8 * i : 8 * i + 8] = owed[cap * o + i, 0:8]
            grad_ref[o, 8 * cap + i : 8 * cap + i + 1] = owed[cap * o + i, 8:9]

    stores = [pltpu.make_async_copy(image_ref, image_hbm, sems.at[cuts])]
    stores[0].start()
    for c, span in enumerate(spans):
        each(share * c, share * (c + 1), pack)
        stores.append(pltpu.make_async_copy(grad_ref.at[span], grad_hbm.at[span], sems.at[c]))
        stores[-1].start()
    for store in stores:
        store.wait()


def blend(arrived, cap, target, tile_place, pairs, order):
    channels, tiles, pixels = target.shape
    devices, rows, block = arrived.shape
    slots = devices * cap
    turns = pairs.shape[0] // PAIR
    many = GROUP * PAIR
    basis = jnp.asarray(pixel_basis())
    smem = pl.BlockSpec(memory_space=pltpu.SMEM)
    anywhere = pl.BlockSpec(memory_space=pl.ANY)
    vmem = pl.BlockSpec(memory_space=pltpu.VMEM)
    return pl.pallas_call(
        functools.partial(blend_kernel, cap),
        in_specs=[smem, smem, smem, vmem, anywhere, anywhere],
        out_specs=[anywhere, anywhere],
        scratch_shapes=[
            pltpu.VMEM(arrived.shape, F32),
            pltpu.VMEM(target.shape, F32),
            pltpu.VMEM(target.shape, F32),
            pltpu.VMEM(arrived.shape, F32),
            pltpu.SemaphoreType.DMA((5,)),
            pltpu.VMEM((slots + 1, 16, block), F32),
            pltpu.VMEM((slots + 1, 16, block), F32),
            pltpu.VMEM((slots + 1, 16, 2 * block), BF16),
            pltpu.VMEM((slots + 1, 32, block), BF16),
            pltpu.VMEM((GROUP, 8, pixels), F32),
            pltpu.VMEM((PAIR, GROUP, 8, block), F32),
            pltpu.VMEM((PAIR, GROUP, 16, block), F32),
        ]
        + [pltpu.VMEM((turns, block, pixels), F32)] * many
        + [pltpu.VMEM((turns, block, pixels), F32)] * many
        + [pltpu.VMEM((turns, 2 * block, pixels), BF16)] * many
        + [pltpu.VMEM((turns, 8, pixels), F32)] * many
        + [pltpu.VMEM((2, block, pixels), F32)] * many
        + [pltpu.VMEM((2, block, pixels), F32)] * many
        + [pltpu.VMEM((2, 2 * block, pixels), BF16)] * many,
        out_shape=[
            jax.ShapeDtypeStruct(target.shape, F32),
            jax.ShapeDtypeStruct((devices, rows, block), F32),
        ],
        name="blend",
        compiler_params=pltpu.CompilerParams(),
    )(pairs, tile_place, order, basis, arrived, target)


def whereabouts(sizes):
    nx, ny = sizes
    me = lax.axis_index("gx") * ny + lax.axis_index("gy")

    def other(n):
        o = lax.rem(me + n, nx * ny)
        return o, (lax.div(o, ny), lax.rem(o, ny))

    return me, nx * ny, other


def each(start, stop, body, width=4):
    whole = (stop - start) // width

    def some(c, _):
        for w in range(width):
            body(start + width * c + w)
        return 0

    lax.fori_loop(0, whole, some, 0)
    for n in range(start + width * whole, stop):
        body(n)


def greet(devices, other):
    barrier = pltpu.get_barrier_semaphore()

    def call(n):
        pl.semaphore_signal(
            barrier, inc=1, device_id=other(n)[1], device_id_type=pl.DeviceIdType.MESH
        )

    each(1, devices, call)
    return barrier


def post(source, target, sems, where):
    return pltpu.make_async_remote_copy(
        src_ref=source,
        dst_ref=target,
        send_sem=sems.at[0],
        recv_sem=sems.at[1],
        device_id=where,
        device_id_type=pl.DeviceIdType.MESH,
    )


def order_rows(pairs, order_ref):
    depth, tiles = pairs.shape
    live = jnp.sum((pairs >= 0).astype(F32), axis=0, keepdims=True)
    across = lax.broadcasted_iota(jnp.int32, (tiles, tiles), 1).astype(F32)
    down = lax.broadcasted_iota(jnp.int32, (tiles, tiles), 0).astype(F32)
    theirs = jnp.broadcast_to(live, (tiles, tiles))
    mine = jnp.sum(jnp.where(across == down, theirs, 0.0), axis=1, keepdims=True)
    before = (theirs > mine) | ((theirs == mine) & (across < down))
    rank = jnp.sum(before.astype(F32), axis=1, keepdims=True)
    order = jnp.sum(jnp.where(rank == across, down, 0.0), axis=0, keepdims=True)
    order_ref[...] = order.astype(jnp.int32)


def fetch_kernel(
    sizes, width, height, splats_ref, fetch_ref, pairs_ref, order_ref,
    arrived_ref, rows_hbm, lists_hbm, asked_hbm,
    rows_ref, lists_ref, asked, raw, wants, lists, mix, own, send, ask, heard,
    ask_sems, sems, local_sems,
):
    me, devices, other = whereabouts(sizes)
    cap = fetch_ref.shape[0]
    _, blocks, block = raw.shape
    used = 9 * cap
    barrier = greet(devices, other)
    loads = [
        pltpu.make_async_copy(source, target, local_sems.at[n])
        for n, (source, target) in enumerate(
            ((fetch_ref, wants), (pairs_ref, lists), (splats_ref, raw), (order_ref, mix))
        )
    ]
    for load in loads:
        load.start()

    loads[0].wait()
    table = jnp.concatenate([wants[...], jnp.zeros((8 - cap, devices), jnp.int32)], axis=0)
    if devices % 128:
        table = jnp.concatenate(
            [table, jnp.zeros((8, 128 - devices % 128), jnp.int32)], axis=1
        )
    table = jnp.transpose(table.astype(F32))[0:devices]
    ask[...] = jnp.zeros_like(ask)
    ask[:, :, 0:8] = table.astype(jnp.int32).reshape(devices, 1, 8)

    pl.semaphore_wait(barrier, devices - 1)

    def inquire(n):
        o, where = other(n)
        post(ask.at[o], asked.at[me], ask_sems, where).start()

    each(1, devices, inquire)
    keep = pltpu.make_async_copy(ask.at[me], asked.at[me], local_sems.at[0])
    keep.start()
    keep.wait()
    rest = pl.ds(0, devices - 1)
    bulk = post(ask.at[rest], asked.at[rest], ask_sems, other(1)[1])
    loads[1].wait()
    order_rows(lists[...], rows_ref)
    depth = lists.shape[0]
    lists_ref[...] = jnp.full(lists_ref.shape, -1, jnp.int32)
    lists_ref[0:depth] = lists[...]
    stores = [
        pltpu.make_async_copy(rows_ref, rows_hbm, local_sems.at[0]),
        pltpu.make_async_copy(lists_ref, lists_hbm, local_sems.at[1]),
        pltpu.make_async_copy(asked, asked_hbm, local_sems.at[4]),
    ]
    loads[2].wait()
    loads[3].wait()
    place_x, place_y, place_z = raw[0], raw[1], raw[2]
    inverse_one = jnp.exp(-2.0 * raw[3])
    inverse_two = jnp.exp(-2.0 * raw[4])
    cosine = jnp.cos(raw[5])
    sine = jnp.sin(raw[5])
    length = jnp.sqrt(place_x * place_x + place_y * place_y + place_z * place_z)
    terms = harmonic_terms(place_x / length, place_y / length, place_z / length)
    lines = [
        width * place_x / place_z + 0.5 * width,
        width * place_y / place_z + 0.5 * height,
        cosine * cosine * inverse_one + sine * sine * inverse_two,
        cosine * sine * (inverse_one - inverse_two),
        sine * sine * inverse_one + cosine * cosine * inverse_two,
        jnp.minimum(raw[6], 0.0) - jnp.log1p(jnp.exp(-jnp.abs(raw[6]))),
    ]
    for h in range(3):
        color = jnp.full((blocks, block), 0.5, F32)
        for k in range(16):
            color = color + raw[7 + 16 * h + k] * terms[k]
        lines.append(color)
    order = mix[...].astype(BF16)
    for j, line in enumerate(lines):
        one = rounded(line)
        two = rounded(line - one)
        three = line - one - two
        stack = jnp.concatenate([one, two, three], axis=0).astype(BF16)
        mixed = jnp.dot(stack, order, preferred_element_type=F32)
        mixed = mixed[0:blocks] + mixed[blocks : 2 * blocks] + mixed[2 * blocks :]
        own[:, j, :] = mixed

    bulk.wait_recv()
    load = pltpu.make_async_copy(asked, heard, local_sems.at[2])
    load.start()
    for store in stores:
        store.start()
    load.wait()

    def pick(o):
        for i in range(cap):
            b = jnp.clip(heard[o, 0, i], 0, blocks - 1)
            send[o, 8 * i : 8 * i + 8] = own[b, 0:8]
            send[o, 8 * cap + i : 8 * cap + i + 1] = own[b, 8:9]

    part = pl.ds(0, used)

    def serve(n):
        o, where = other(n)
        post(send.at[o, part], arrived_ref.at[me, part], sems, where).start()

    lag = 4
    width = 4
    turns = (devices - 1 - lag) // width
    for n in range(1, 1 + lag):
        pick(other(n)[0])

    def run(c, _):
        for w in range(width):
            pick(other(1 + lag + width * c + w)[0])
        for w in range(width):
            serve(1 + width * c + w)
        return 0

    lax.fori_loop(0, turns, run, 0)
    for n in range(1 + lag + width * turns, devices):
        pick(other(n)[0])
    pick(me)
    for n in range(1 + width * turns, devices):
        serve(n)
    keep = pltpu.make_async_copy(send.at[me], arrived_ref.at[me], local_sems.at[3])
    keep.start()
    bulk.wait_send()
    whole = post(send.at[rest, part], arrived_ref.at[rest, part], sems, other(1)[1])
    whole.wait_recv()
    whole.wait_send()
    keep.wait()
    for store in stores:
        store.wait()


def fetch_blocks(splats, fetch, pairs, sizes, width, height):
    _, blocks, block = splats.shape
    cap, devices = fetch.shape
    rows = 8 * pl.cdiv(9 * cap, 8)
    order = jnp.asarray(lane_order(block))
    depth = PAIR * pl.cdiv(pairs.shape[0], PAIR)
    anywhere = pl.BlockSpec(memory_space=pl.ANY)
    return pl.pallas_call(
        functools.partial(fetch_kernel, sizes, width, height),
        in_specs=[anywhere] * 4,
        out_specs=[anywhere] * 4,
        scratch_shapes=[
            pltpu.VMEM((1, pairs.shape[1]), jnp.int32),
            pltpu.VMEM((depth + PAIR, pairs.shape[1]), jnp.int32),
            pltpu.VMEM((devices, 1, 128), jnp.int32),
            pltpu.VMEM(splats.shape, F32),
            pltpu.VMEM(fetch.shape, jnp.int32),
            pltpu.VMEM(pairs.shape, jnp.int32),
            pltpu.VMEM(order.shape, F32),
            pltpu.VMEM((blocks, 16, block), F32),
            pltpu.VMEM((devices, rows, block), F32),
            pltpu.VMEM((devices, 1, 128), jnp.int32),
            pltpu.SMEM((devices, 1, 128), jnp.int32),
            pltpu.SemaphoreType.DMA((2,)),
            pltpu.SemaphoreType.DMA((2,)),
            pltpu.SemaphoreType.DMA((5,)),
        ],
        out_shape=[
            jax.ShapeDtypeStruct((devices, rows, block), F32),
            jax.ShapeDtypeStruct((1, pairs.shape[1]), jnp.int32),
            jax.ShapeDtypeStruct((depth + PAIR, pairs.shape[1]), jnp.int32),
            jax.ShapeDtypeStruct((devices, 1, 128), jnp.int32),
        ],
        name="fetch",
        compiler_params=pltpu.CompilerParams(collective_id=0, has_side_effects=True),
    )(splats, fetch, pairs, order)


def thirds(x):
    one = rounded(x)
    two = rounded(x - one)
    return [one, two, x - one - two]


def return_kernel(
    sizes, cap, blocks, grad_ref, asked_ref, order_ref, total_hbm,
    total_ref, returned, asked, mix, sems, local_sems, store_sem,
):
    me, devices, other = whereabouts(sizes)
    barrier = greet(devices, other)
    rows = grad_ref.shape[1]
    used = 9 * cap
    spot = pl.ds(pl.multiple_of(me * rows, 8), rows)
    loads = [
        pltpu.make_async_copy(source, target, local_sems.at[n])
        for n, (source, target) in enumerate(
            ((grad_ref.at[me], returned.at[spot]), (asked_ref, asked), (order_ref, mix))
        )
    ]
    for load in loads:
        load.start()
    for load in loads:
        load.wait()
    lane = lax.broadcasted_iota(jnp.int32, (devices, blocks), 1)
    owners = []
    for i in range(cap):
        column = jnp.broadcast_to(asked[:, 0, i : i + 1], (devices, blocks))
        owners += [(column == lane).astype(F32)] * 3
    owners = jnp.concatenate(owners, axis=0).astype(BF16)
    order = mix[...].astype(BF16)
    pl.semaphore_wait(barrier, devices - 1)
    part = pl.ds(0, used)
    land = pl.ds(pl.multiple_of(me * rows, 8), used)

    def serve(n):
        o, where = other(n)
        post(grad_ref.at[o, part], returned.at[land], sems, where).start()

    each(1, devices, serve)
    rest = pl.ds(0, devices - 1)
    bulk = returned.at[pl.ds(0, (devices - 1) * used)]
    post(bulk, bulk, sems, other(1)[1]).wait_recv()
    for r in range(9):
        terms = []
        for i in range(cap):
            at = 8 * i + r if r < 8 else 8 * cap + i
            terms += thirds(returned[pl.ds(at, devices, stride=rows), :])
        summed = lax.dot_general(
            owners,
            jnp.concatenate(terms, axis=0).astype(BF16),
            (((0,), (0,)), ((), ())),
            preferred_element_type=F32,
        )
        mixed = lax.dot_general(
            jnp.concatenate(thirds(summed), axis=0).astype(BF16),
            order,
            (((1,), (1,)), ((), ())),
            preferred_element_type=F32,
        )
        total_ref[r] = mixed[0:blocks] + mixed[blocks : 2 * blocks] + mixed[2 * blocks :]
        if r % 3 == 2:
            span = pl.ds(r - 2, 3)
            pltpu.make_async_copy(total_ref.at[span], total_hbm.at[span], store_sem).start()
    sent = grad_ref.at[rest, part]
    post(sent, sent, sems, other(1)[1]).wait_send()
    pltpu.make_async_copy(total_ref, total_hbm, store_sem).wait()


def return_grads(grads, asked, cap, blocks, sizes):
    devices, rows, block = grads.shape
    order = jnp.asarray(lane_order(block))
    return pl.pallas_call(
        functools.partial(return_kernel, sizes, cap, blocks),
        in_specs=[pl.BlockSpec(memory_space=pl.ANY)] * 3,
        out_specs=pl.BlockSpec(memory_space=pl.ANY),
        scratch_shapes=[
            pltpu.VMEM((9, blocks, block), F32),
            pltpu.VMEM((devices * rows, block), F32),
            pltpu.VMEM(asked.shape, jnp.int32),
            pltpu.VMEM(order.shape, F32),
            pltpu.SemaphoreType.DMA((2,)),
            pltpu.SemaphoreType.DMA((3,)),
            pltpu.SemaphoreType.DMA,
        ],
        out_shape=jax.ShapeDtypeStruct((9, blocks, block), F32),
        name="give_back",
        compiler_params=pltpu.CompilerParams(collective_id=1, has_side_effects=True),
    )(grads, asked, order)


def outline(width, height, x, y, z, first, second, angle):
    inverse_one = jnp.exp(-2.0 * first)
    inverse_two = jnp.exp(-2.0 * second)
    cosine = jnp.cos(angle)
    sine = jnp.sin(angle)
    return (
        width * x / z + 0.5 * width,
        width * y / z + 0.5 * height,
        cosine * cosine * inverse_one + sine * sine * inverse_two,
        cosine * sine * (inverse_one - inverse_two),
        sine * sine * inverse_one + cosine * cosine * inverse_two,
    )


def directions(x, y, z):
    length = jnp.sqrt(x * x + y * y + z * z)
    return tuple(harmonic_terms(x / length, y / length, z / length))


def adam_kernel(
    width, height, total_hbm, splats_ref, one_ref, two_ref, grad_ref, step_ref,
    total_ref, raw, one, two, grad, step, load_sems, store_sems,
):
    count = raw.shape[0]
    cuts = [0, 7] + [7 + 16 * h for h in range(1, 4)]
    spans = [pl.ds(lo, hi - lo) for lo, hi in zip(cuts, cuts[1:])]
    load = pltpu.make_async_copy(splats_ref, raw, load_sems.at[0])
    load.start()
    sums = pltpu.make_async_copy(total_hbm, total_ref, load_sems.at[9])
    sums.start()
    loads = []
    for n, span in enumerate(spans[1:] + spans[:1]):
        pair = [
            pltpu.make_async_copy(one_ref.at[span], one.at[span], load_sems.at[1 + 2 * n]),
            pltpu.make_async_copy(two_ref.at[span], two.at[span], load_sems.at[2 + 2 * n]),
        ]
        for copy in pair:
            copy.start()
        loads.append(pair)
    load.wait()
    place = (raw[0], raw[1], raw[2])
    terms, turn = jax.vjp(directions, *place)
    sums.wait()
    slants = [jnp.zeros_like(place[0]) for _ in terms]
    stores = []

    def finish(n, span, lo, hi):
        for copy in loads[n]:
            copy.wait()
        for r in range(lo, hi):
            change = grad[r]
            first = 0.9 * one[r] + 0.1 * change
            second = 0.999 * two[r] + 0.001 * change * change
            step[r] = first / (second * lax.rsqrt(second) + 1e-08)
        for m, (source, target) in enumerate(((grad, grad_ref), (step, step_ref))):
            copy = pltpu.make_async_copy(
                source.at[span], target.at[span], store_sems.at[2 * n + m]
            )
            copy.start()
            stores.append(copy)

    for h in range(3):
        hue = total_ref[6 + h]
        for k in range(16):
            r = 7 + 16 * h + k
            grad[r] = hue * terms[k]
            slants[k] = slants[k] + hue * raw[r]
        finish(h, spans[1 + h], cuts[1 + h], cuts[2 + h])
    _, pull = jax.vjp(
        functools.partial(outline, width, height), *place, raw[3], raw[4], raw[5]
    )
    flat = pull(tuple(total_ref[j] for j in range(5)))
    tilt = turn(tuple(slants))
    for j in range(3):
        grad[j] = flat[j] + tilt[j]
    for j in range(3, 6):
        grad[j] = flat[j]
    grad[6] = total_ref[5] / (1.0 + jnp.exp(raw[6]))
    finish(3, spans[0], 0, 7)
    for copy in stores:
        copy.wait()


def adam(total, splats, moment_one, moment_two, width, height):
    anywhere = pl.BlockSpec(memory_space=pl.ANY)
    like = jax.ShapeDtypeStruct(splats.shape, F32)
    return pl.pallas_call(
        functools.partial(adam_kernel, width, height),
        in_specs=[anywhere] * 4,
        out_specs=[anywhere, anywhere],
        scratch_shapes=[pltpu.VMEM(total.shape, F32)]
        + [pltpu.VMEM(splats.shape, F32)] * 5
        + [pltpu.SemaphoreType.DMA((10,)), pltpu.SemaphoreType.DMA((8,))],
        out_shape=[like, like],
        name="adam",
    )(total, splats, moment_one, moment_two)


def local(splats, moment_one, moment_two, target, tile_place, pairs, fetch):
    sizes = (lax.axis_size("gx"), lax.axis_size("gy"))
    devices = sizes[0] * sizes[1]
    tiles_here = target.shape[0]
    cap = fetch.shape[2]
    width = 16.0 * TX
    height = 16.0 * (tiles_here * devices // TX)

    rows_first = jnp.transpose(splats, (1, 0, 2))
    asks = jnp.transpose(fetch[0])
    arrived, rows, lists, asked = fetch_blocks(
        rows_first, asks, jnp.transpose(pairs), sizes, width, height
    )
    image, grads = blend(
        arrived, cap, jnp.transpose(target, (1, 0, 2)), tile_place, lists, rows
    )
    total = return_grads(grads, asked, cap, splats.shape[0], sizes)
    splat_grad, adam_step = adam(
        total,
        rows_first,
        jnp.transpose(moment_one, (1, 0, 2)),
        jnp.transpose(moment_two, (1, 0, 2)),
        width,
        height,
    )
    back = lambda x: jnp.transpose(x, (1, 0, 2))
    return (back(image), back(splat_grad), back(adam_step))


def solution(mesh):
    both = ("gx", "gy")
    return jax.shard_map(
        local,
        mesh=mesh,
        in_specs=(
            P(both, None, None),
            P(both, None, None),
            P(both, None, None),
            P(both, None, None),
            P(both),
            P(both, None),
            P(both, None, None),
        ),
        out_specs=(P(both, None, None), P(both, None, None), P(both, None, None)),
        check_vma=False,
    )
```

```python
import functools

import jax
import jax.numpy as jnp
import numpy as np
from jax import lax
from jax.experimental import pallas as pl
from jax.experimental.pallas import tpu as pltpu
from jax.sharding import PartitionSpec as P

TX = 16
SIDE = 16
PIXELS = SIDE * SIDE
LOG2E = 1.4426950408889634
DEAD = -1.0e4
GROUP = 2
PAIR = 4
F32 = jnp.float32
BF16 = jnp.bfloat16


HARMONIC_ZERO = 0.28209479177387814
HARMONIC_ONE = 0.4886025119029199
HARMONIC_TWO = (
    1.0925484305920792,
    -1.0925484305920792,
    0.31539156525252005,
    -1.0925484305920792,
    0.5462742152960396,
)
HARMONIC_THREE = (
    -0.5900435899266435,
    2.890611442640554,
    -0.4570457994644658,
    0.3731763325901154,
    -0.4570457994644658,
    1.445305721320277,
    -0.5900435899266435,
)


def harmonic_terms(east, north, ahead):
    east_east = east * east
    north_north = north * north
    ahead_ahead = ahead * ahead
    return [
        jnp.full_like(east, HARMONIC_ZERO),
        -HARMONIC_ONE * north,
        HARMONIC_ONE * ahead,
        -HARMONIC_ONE * east,
        HARMONIC_TWO[0] * east * north,
        HARMONIC_TWO[1] * north * ahead,
        HARMONIC_TWO[2] * (2.0 * ahead_ahead - east_east - north_north),
        HARMONIC_TWO[3] * east * ahead,
        HARMONIC_TWO[4] * (east_east - north_north),
        HARMONIC_THREE[0] * north * (3.0 * east_east - north_north),
        HARMONIC_THREE[1] * east * north * ahead,
        HARMONIC_THREE[2] * north * (4.0 * ahead_ahead - east_east - north_north),
        HARMONIC_THREE[3] * ahead * (2.0 * ahead_ahead - 3.0 * east_east - 3.0 * north_north),
        HARMONIC_THREE[4] * east * (4.0 * ahead_ahead - east_east - north_north),
        HARMONIC_THREE[5] * ahead * (east_east - north_north),
        HARMONIC_THREE[6] * east * (east_east - 3.0 * north_north),
    ]


def pixel_basis():
    j = np.arange(PIXELS)
    x = j % SIDE + 0.5 - SIDE / 2
    y = j // SIDE + 0.5 - SIDE / 2
    rows = np.stack([x * x, x * y, y * y, x, y, np.ones_like(x), 0 * x, 0 * x])
    return np.concatenate([rows, rows, rows, 0 * rows]).astype(np.float32)


def lane_order(block):
    row = np.arange(block)
    splat = (row % 8) * (block // 8) + row // 8
    return (np.arange(block)[:, None] == splat[None, :]).astype(np.float32)


def rounded(x):
    return x.astype(BF16).astype(F32)


def shifted(x, shift):
    return pltpu.roll(x, shift % 8, 0)


def blend_kernel(
    cap, pairs_ref, place_ref, order_ref, basis_ref, arrived_ref, target_ref, image_hbm, grad_hbm,
    image_ref, grad_ref, sems, screen, owed, hue_sum, hue_back, resid, parts, moments, *banks,
):
    tiles = target_ref.shape[1]
    depth = pairs_ref.shape[0] - PAIR
    slots = cap * arrived_ref.shape[0]
    block = arrived_ref.shape[2]
    chunks = block // 8
    lanes = range(GROUP)
    spots = [(t, e) for e in range(PAIR) for t in lanes]
    many = GROUP * PAIR
    keeps, weights, halves, ends, alphas, slopes, steps = (
        [banks[many * i + PAIR * t : many * i + PAIR * t + PAIR] for t in lanes] for i in range(7)
    )
    sub = lax.broadcasted_iota(jnp.int32, (8, PIXELS), 0)
    devices = arrived_ref.shape[0]
    cuts = 4 if devices % 4 == 0 else 1
    share = devices // cuts
    spans = [pl.ds(share * c, share) for c in range(cuts)]

    resid[...] = jnp.zeros_like(resid)
    parts[...] = jnp.zeros_like(parts)

    def prepare(o, _):
        for i in range(cap):
            s = cap * o + i
            owed[s] = jnp.zeros((16, block), F32)
            last = arrived_ref[o, 8 * cap + i : 8 * cap + i + 1]
            screen[s, 0:8] = arrived_ref[o, 8 * i : 8 * i + 8]
            screen[s, 8:9] = last
            hue = jnp.concatenate(
                [arrived_ref[o, 8 * i + 6 : 8 * i + 8], last, jnp.zeros((5, block), F32)], axis=0
            )
            hue1 = rounded(hue)
            hue2 = hue - hue1
            zero = jnp.zeros_like(hue)
            hue_sum[s] = jnp.concatenate(
                [
                    jnp.concatenate([hue1, hue1], axis=1),
                    jnp.concatenate([hue2, zero], axis=1),
                ],
                axis=0,
            ).astype(BF16)
            hue_back[s] = jnp.concatenate([hue1, hue2, hue1, zero], axis=0).astype(BF16)
        return 0

    for c in range(cuts):
        lax.fori_loop(share * c, share * (c + 1), prepare, 0)
    owed[slots] = jnp.zeros((16, block), F32)
    screen[slots] = jnp.zeros((16, block), F32)
    screen[slots, 5:6] = jnp.full((1, block), DEAD, F32)
    hue_sum[slots] = jnp.zeros((16, 2 * block), BF16)
    hue_back[slots] = jnp.zeros((32, block), BF16)

    basis = basis_ref[...].astype(BF16)
    monomials = basis_ref[0:8].astype(BF16)
    zero_row = jnp.zeros((8, PIXELS), F32)

    def group(step, _):
        row = [order_ref[0, step * GROUP + t] for t in lanes]
        deepest = jnp.int32(0)
        for k in range(depth):
            deepest = deepest + (pairs_ref[k, row[0]] >= 0).astype(jnp.int32)
        turns = lax.div(deepest + (PAIR - 1), PAIR)
        centre = []
        for t in lanes:
            tile = place_ref[row[t]]
            cx = (lax.rem(tile, TX) * SIDE + SIDE // 2).astype(F32)
            cy = (lax.div(tile, TX) * SIDE + SIDE // 2).astype(F32)
            centre.append((cx, cy))

        def place(t, k):
            slot = pairs_ref[k, row[t]]
            return jnp.where(slot >= 0, slot, slots)

        def shape_up(j):
            for t, e in spots:
                cx, cy = centre[t]
                s = place(t, PAIR * j + e)
                u = screen[s, 0:1] - cx
                v = screen[s, 1:2] - cy
                a, b, c = screen[s, 2:3], screen[s, 3:4], screen[s, 4:5]
                opac = jnp.maximum(screen[s, 5:6], DEAD)
                lin_x = a * u + b * v
                lin_y = b * u + c * v
                const = opac - 0.5 * (lin_x * u + lin_y * v)
                for r, value in enumerate((-0.5 * a, -b, -0.5 * c, lin_x, lin_y, const)):
                    parts[e, t, r : r + 1] = LOG2E * value

        shape_up(0)

        def power_of(t, e):
            c = parts[e, t]
            c1 = rounded(c)
            c2 = rounded(c - c1)
            c3 = c - c1 - c2
            left = jnp.concatenate([c1, c2, c3, jnp.zeros_like(c)], axis=0).astype(BF16)
            return lax.dot_general(
                left, basis, (((0,), (0,)), ((), ())), preferred_element_type=F32
            )

        def draw(t, j, e, power):
            alpha = jnp.exp2(power)
            alphas[t][e][0] = alpha
            keep = 1.0 - alpha
            keeps[t][e][j] = keep
            kept = keep[0:8]
            for i in range(1, chunks):
                kept = kept * keep[8 * i : 8 * i + 8]
            return kept

        def scan_of(t, j, e, kept, trans):
            scan = jnp.where(sub == 0, trans, shifted(kept, 1))
            for d in (1, 2, 4):
                scan = scan * jnp.where(sub < d, 1.0, shifted(scan, d))
            end = scan * kept
            ends[t][e][j] = end
            return scan, jnp.broadcast_to(end[7:8], (8, PIXELS))

        def spread(t, j, e, here):
            for i in range(0, chunks, 2):
                lo, mid, hi = 8 * i, 8 * i + 8, 8 * i + 16
                one = alphas[t][e][0, lo:mid] * here
                here = here * keeps[t][e][j, lo:mid]
                two = alphas[t][e][0, mid:hi] * here
                here = here * keeps[t][e][j, mid:hi]
                pair = jnp.concatenate([one, two], axis=0)
                weights[t][e][j, lo:hi] = pair
                high = pair.astype(BF16)
                halves[t][e][j, lo:hi] = high
                halves[t][e][j, block + lo : block + hi] = (pair - high.astype(F32)).astype(BF16)

        def summed(t, j, e):
            return jnp.dot(
                hue_sum[place(t, PAIR * j + e)], halves[t][e][j], preferred_element_type=F32
            )

        def forward(j, carry):
            trans = [carry[2 * t] for t in lanes]
            totals = [carry[2 * t + 1] for t in lanes]
            powers = [[power_of(t, e) for t in lanes] for e in range(PAIR)]
            kepts = [draw(t, j, 0, powers[0][t]) for t in lanes]
            for e in range(PAIR):
                heres = []
                for t in lanes:
                    here, trans[t] = scan_of(t, j, e, kepts[t], trans[t])
                    heres.append(here)
                for t in lanes:
                    spread(t, j, e, heres[t])
                    if e + 1 < PAIR:
                        kepts[t] = draw(t, j, e + 1, powers[e + 1][t])
                totals = [totals[t] + summed(t, j, e) for t in lanes]
            shape_up(j + 1)
            return tuple(x for t in lanes for x in (trans[t], totals[t]))

        start = (jnp.ones((8, PIXELS), F32), jnp.zeros((16, PIXELS), F32)) * GROUP
        done = lax.fori_loop(0, turns, forward, start)

        pulls = []
        for t in lanes:
            total = done[2 * t + 1]
            image = (total[0:8] + total[8:16])[0:3]
            for h in range(3):
                image_ref[h, pl.ds(row[t], 1)] = image[h : h + 1]
                resid[t, h : h + 1] = (image[h : h + 1] - target_ref[h, pl.ds(row[t], 1)]) * (
                    2.0 / 512.0
                )
            g = resid[t]
            g1 = rounded(g)
            g2 = g - g1
            pulls.append(
                (
                    jnp.concatenate([g1, g1, g2, zero_row], axis=0).astype(BF16),
                    jnp.concatenate([g1, g2], axis=0).astype(BF16),
                )
            )

        def lean(t, j, e):
            slopes[t][e][0] = lax.dot_general(
                hue_back[place(t, PAIR * j + e)],
                pulls[t][0],
                (((0,), (0,)), ((), ())),
                preferred_element_type=F32,
            )

        def behind_of(t, j, e, behind):
            run = weights[t][e][j, 0:8] * slopes[t][e][0, 0:8]
            for i in range(1, chunks):
                lo, hi = 8 * i, 8 * i + 8
                run = run + weights[t][e][j, lo:hi] * slopes[t][e][0, lo:hi]
            scan = jnp.where(sub == 7, behind, shifted(run, -1))
            for d in (1, 2, 4):
                scan = scan + jnp.where(sub < 8 - d, shifted(scan, -d), 0.0)
            return (
                scan / jnp.maximum(ends[t][e][j], 1e-37),
                jnp.broadcast_to((run + scan)[0:1], (8, PIXELS)),
            )

        def step_of(t, j, e, here):
            for i in range(chunks - 2, -1, -2):
                lo, mid, hi = 8 * i, 8 * i + 8, 8 * i + 16
                ahead = slopes[t][e][0, mid:hi]
                gap = ahead - here
                two = weights[t][e][j, mid:hi] * gap
                here = ahead - keeps[t][e][j, mid:hi] * gap
                ahead = slopes[t][e][0, lo:mid]
                gap = ahead - here
                one = weights[t][e][j, lo:mid] * gap
                here = ahead - keeps[t][e][j, lo:mid] * gap
                pair = jnp.concatenate([one, two], axis=0)
                high = pair.astype(BF16)
                steps[t][e][0, lo:hi] = high
                steps[t][e][0, block + lo : block + hi] = (pair - high.astype(F32)).astype(BF16)

        def settle(j):
            for t, e in spots:
                cx, cy = centre[t]
                s = place(t, PAIR * j + e)
                u = screen[s, 0:1] - cx
                v = screen[s, 1:2] - cy
                a, b, c = screen[s, 2:3], screen[s, 3:4], screen[s, 4:5]
                mxx, mxy, myy, mx, my, m = (moments[e, t, r : r + 1] for r in range(6))
                off_x = mx - u * m
                off_y = my - v * m
                changes = (
                    a * off_x + b * off_y,
                    b * off_x + c * off_y,
                    -0.5 * (mxx - u * (mx + off_x)),
                    -(mxy - u * my - v * off_x),
                    -0.5 * (myy - v * (my + off_y)),
                    m,
                    moments[e, t, 8:9],
                    moments[e, t, 9:10],
                    moments[e, t, 10:11],
                )
                for r, change in enumerate(changes):
                    owed[s, r : r + 1] = owed[s, r : r + 1] + change

        def backward(index, carry):
            j = turns - 1 - index
            behind = list(carry)
            settle(j + 1)
            places = []
            for e in reversed(range(PAIR)):
                for t in lanes:
                    lean(t, j, e)
            for e in reversed(range(PAIR)):
                for t in lanes:
                    hues = lax.dot_general(
                        pulls[t][1], halves[t][e][j], (((1,), (1,)), ((), ())),
                        preferred_element_type=F32,
                    )
                    places.append(
                        (t, e, 8, hues[0:8, 0:block] + hues[0:8, block:] + hues[8:16, 0:block])
                    )
                heres = []
                for t in lanes:
                    here, behind[t] = behind_of(t, j, e, behind[t])
                    heres.append(here)
                for t in lanes:
                    step_of(t, j, e, heres[t])
                for t in lanes:
                    sums = lax.dot_general(
                        monomials, steps[t][e][0], (((1,), (1,)), ((), ())), preferred_element_type=F32
                    )
                    places.append((t, e, 0, sums[:, 0:block] + sums[:, block:]))
            for t, e, at, value in places:
                moments[e, t, at : at + 8] = value
            return tuple(behind)

        lax.fori_loop(0, turns, backward, (jnp.zeros((8, PIXELS), F32),) * GROUP)

        settle(0)
        return 0

    lax.fori_loop(0, tiles // GROUP, group, 0)

    def pack(o):
        for i in range(cap):
            grad_ref[o, 8 * i : 8 * i + 8] = owed[cap * o + i, 0:8]
            grad_ref[o, 8 * cap + i : 8 * cap + i + 1] = owed[cap * o + i, 8:9]

    stores = [pltpu.make_async_copy(image_ref, image_hbm, sems.at[cuts])]
    stores[0].start()
    for c, span in enumerate(spans):
        each(share * c, share * (c + 1), pack)
        stores.append(pltpu.make_async_copy(grad_ref.at[span], grad_hbm.at[span], sems.at[c]))
        stores[-1].start()
    for store in stores:
        store.wait()


def blend(arrived, cap, target, tile_place, pairs, order):
    channels, tiles, pixels = target.shape
    devices, rows, block = arrived.shape
    slots = devices * cap
    turns = pairs.shape[0] // PAIR
    many = GROUP * PAIR
    basis = jnp.asarray(pixel_basis())
    smem = pl.BlockSpec(memory_space=pltpu.SMEM)
    anywhere = pl.BlockSpec(memory_space=pl.ANY)
    vmem = pl.BlockSpec(memory_space=pltpu.VMEM)
    return pl.pallas_call(
        functools.partial(blend_kernel, cap),
        in_specs=[smem, smem, smem, vmem, vmem, vmem],
        out_specs=[anywhere, anywhere],
        scratch_shapes=[
            pltpu.VMEM(target.shape, F32),
            pltpu.VMEM(arrived.shape, F32),
            pltpu.SemaphoreType.DMA((5,)),
            pltpu.VMEM((slots + 1, 16, block), F32),
            pltpu.VMEM((slots + 1, 16, block), F32),
            pltpu.VMEM((slots + 1, 16, 2 * block), BF16),
            pltpu.VMEM((slots + 1, 32, block), BF16),
            pltpu.VMEM((GROUP, 8, pixels), F32),
            pltpu.VMEM((PAIR, GROUP, 8, block), F32),
            pltpu.VMEM((PAIR, GROUP, 16, block), F32),
        ]
        + [pltpu.VMEM((turns, block, pixels), F32)] * many
        + [pltpu.VMEM((turns, block, pixels), F32)] * many
        + [pltpu.VMEM((turns, 2 * block, pixels), BF16)] * many
        + [pltpu.VMEM((turns, 8, pixels), F32)] * many
        + [pltpu.VMEM((2, block, pixels), F32)] * many
        + [pltpu.VMEM((2, block, pixels), F32)] * many
        + [pltpu.VMEM((2, 2 * block, pixels), BF16)] * many,
        out_shape=[
            jax.ShapeDtypeStruct(target.shape, F32),
            jax.ShapeDtypeStruct((devices, rows, block), F32),
        ],
        name="blend",
        compiler_params=pltpu.CompilerParams(),
    )(pairs, tile_place, order, basis, arrived, target)


def whereabouts(sizes):
    nx, ny = sizes
    me = lax.axis_index("gx") * ny + lax.axis_index("gy")

    def other(n):
        o = lax.rem(me + n, nx * ny)
        return o, (lax.div(o, ny), lax.rem(o, ny))

    return me, nx * ny, other


def each(start, stop, body, width=4):
    whole = (stop - start) // width

    def some(c, _):
        for w in range(width):
            body(start + width * c + w)
        return 0

    lax.fori_loop(0, whole, some, 0)
    for n in range(start + width * whole, stop):
        body(n)


def greet(devices, other):
    barrier = pltpu.get_barrier_semaphore()

    def call(n):
        pl.semaphore_signal(
            barrier, inc=1, device_id=other(n)[1], device_id_type=pl.DeviceIdType.MESH
        )

    each(1, devices, call)
    return barrier


def post(source, target, sems, where):
    return pltpu.make_async_remote_copy(
        src_ref=source,
        dst_ref=target,
        send_sem=sems.at[0],
        recv_sem=sems.at[1],
        device_id=where,
        device_id_type=pl.DeviceIdType.MESH,
    )


def order_rows(pairs, order_ref):
    depth, tiles = pairs.shape
    live = jnp.sum((pairs >= 0).astype(F32), axis=0, keepdims=True)
    across = lax.broadcasted_iota(jnp.int32, (tiles, tiles), 1).astype(F32)
    down = lax.broadcasted_iota(jnp.int32, (tiles, tiles), 0).astype(F32)
    theirs = jnp.broadcast_to(live, (tiles, tiles))
    mine = jnp.sum(jnp.where(across == down, theirs, 0.0), axis=1, keepdims=True)
    before = (theirs > mine) | ((theirs == mine) & (across < down))
    rank = jnp.sum(before.astype(F32), axis=1, keepdims=True)
    order = jnp.sum(jnp.where(rank == across, down, 0.0), axis=0, keepdims=True)
    order_ref[...] = order.astype(jnp.int32)


def fetch_kernel(
    sizes, width, height, splats_ref, fetch_ref, pairs_ref, order_ref,
    arrived_ref, rows_hbm, lists_hbm, asked_hbm,
    rows_ref, lists_ref, asked, raw, wants, lists, mix, own, send, ask, heard,
    ask_sems, hear_sems, sems, local_sems,
):
    me, devices, other = whereabouts(sizes)
    cap = fetch_ref.shape[0]
    _, blocks, block = raw.shape
    used = 9 * cap
    barrier = greet(devices, other)
    loads = [
        pltpu.make_async_copy(source, target, local_sems.at[n])
        for n, (source, target) in enumerate(
            ((fetch_ref, wants), (pairs_ref, lists), (splats_ref, raw), (order_ref, mix))
        )
    ]
    for load in loads:
        load.start()

    loads[0].wait()
    table = jnp.concatenate([wants[...], jnp.zeros((8 - cap, devices), jnp.int32)], axis=0)
    if devices % 128:
        table = jnp.concatenate(
            [table, jnp.zeros((8, 128 - devices % 128), jnp.int32)], axis=1
        )
    table = jnp.transpose(table.astype(F32))[0:devices]
    ask[...] = jnp.zeros_like(ask)
    ask[:, :, 0:8] = table.astype(jnp.int32).reshape(devices, 1, 8)

    pl.semaphore_wait(barrier, devices - 1)

    def inquire(n):
        o, where = other(n)
        post(ask.at[o], asked.at[me], ask_sems, where).start()
        post(ask.at[o], heard.at[me], hear_sems, where).start()

    each(1, devices, inquire)
    keep = pltpu.make_async_copy(ask.at[me], asked.at[me], local_sems.at[0])
    keep.start()
    keep.wait()
    keep = pltpu.make_async_copy(ask.at[me], heard.at[me], local_sems.at[0])
    keep.start()
    keep.wait()
    rest = pl.ds(0, devices - 1)
    bulk = post(ask.at[rest], asked.at[rest], ask_sems, other(1)[1])
    loads[1].wait()
    order_rows(lists[...], rows_ref)
    depth = lists.shape[0]
    lists_ref[...] = jnp.full(lists_ref.shape, -1, jnp.int32)
    lists_ref[0:depth] = lists[...]
    stores = [
        pltpu.make_async_copy(rows_ref, rows_hbm, local_sems.at[0]),
        pltpu.make_async_copy(lists_ref, lists_hbm, local_sems.at[1]),
        pltpu.make_async_copy(asked, asked_hbm, local_sems.at[4]),
    ]
    loads[2].wait()
    loads[3].wait()
    place_x, place_y, place_z = raw[0], raw[1], raw[2]
    inverse_one = jnp.exp(-2.0 * raw[3])
    inverse_two = jnp.exp(-2.0 * raw[4])
    cosine = jnp.cos(raw[5])
    sine = jnp.sin(raw[5])
    length = jnp.sqrt(place_x * place_x + place_y * place_y + place_z * place_z)
    terms = harmonic_terms(place_x / length, place_y / length, place_z / length)
    lines = [
        width * place_x / place_z + 0.5 * width,
        width * place_y / place_z + 0.5 * height,
        cosine * cosine * inverse_one + sine * sine * inverse_two,
        cosine * sine * (inverse_one - inverse_two),
        sine * sine * inverse_one + cosine * cosine * inverse_two,
        jnp.minimum(raw[6], 0.0) - jnp.log1p(jnp.exp(-jnp.abs(raw[6]))),
    ]
    for h in range(3):
        color = jnp.full((blocks, block), 0.5, F32)
        for k in range(16):
            color = color + raw[7 + 16 * h + k] * terms[k]
        lines.append(color)
    order = mix[...].astype(BF16)
    for j, line in enumerate(lines):
        one = rounded(line)
        two = rounded(line - one)
        three = line - one - two
        stack = jnp.concatenate([one, two, three], axis=0).astype(BF16)
        mixed = jnp.dot(stack, order, preferred_element_type=F32)
        mixed = mixed[0:blocks] + mixed[blocks : 2 * blocks] + mixed[2 * blocks :]
        own[:, j, :] = mixed

    bulk.wait_recv()
    for store in stores:
        store.start()
    both = post(ask.at[rest], heard.at[rest], hear_sems, other(1)[1])
    both.wait_recv()
    both.wait_send()

    def pick(o):
        for i in range(cap):
            b = jnp.clip(heard[o, 0, i], 0, blocks - 1)
            send[o, 8 * i : 8 * i + 8] = own[b, 0:8]
            send[o, 8 * cap + i : 8 * cap + i + 1] = own[b, 8:9]

    part = pl.ds(0, used)

    def serve(n):
        o, where = other(n)
        post(send.at[o, part], arrived_ref.at[me, part], sems, where).start()

    lag = 4
    width = 4
    turns = (devices - 1 - lag) // width
    for n in range(1, 1 + lag):
        pick(other(n)[0])

    def run(c, _):
        for w in range(width):
            pick(other(1 + lag + width * c + w)[0])
        for w in range(width):
            serve(1 + width * c + w)
        return 0

    lax.fori_loop(0, turns, run, 0)
    for n in range(1 + lag + width * turns, devices):
        pick(other(n)[0])
    pick(me)
    for n in range(1 + width * turns, devices):
        serve(n)
    keep = pltpu.make_async_copy(send.at[me], arrived_ref.at[me], local_sems.at[3])
    keep.start()
    bulk.wait_send()
    whole = post(send.at[rest, part], arrived_ref.at[rest, part], sems, other(1)[1])
    whole.wait_recv()
    whole.wait_send()
    keep.wait()
    for store in stores:
        store.wait()


def fetch_blocks(splats, fetch, pairs, sizes, width, height):
    _, blocks, block = splats.shape
    cap, devices = fetch.shape
    rows = 8 * pl.cdiv(9 * cap, 8)
    order = jnp.asarray(lane_order(block))
    depth = PAIR * pl.cdiv(pairs.shape[0], PAIR)
    anywhere = pl.BlockSpec(memory_space=pl.ANY)
    return pl.pallas_call(
        functools.partial(fetch_kernel, sizes, width, height),
        in_specs=[anywhere] * 4,
        out_specs=[anywhere] * 4,
        scratch_shapes=[
            pltpu.VMEM((1, pairs.shape[1]), jnp.int32),
            pltpu.VMEM((depth + PAIR, pairs.shape[1]), jnp.int32),
            pltpu.VMEM((devices, 1, 128), jnp.int32),
            pltpu.VMEM(splats.shape, F32),
            pltpu.VMEM(fetch.shape, jnp.int32),
            pltpu.VMEM(pairs.shape, jnp.int32),
            pltpu.VMEM(order.shape, F32),
            pltpu.VMEM((blocks, 16, block), F32),
            pltpu.VMEM((devices, rows, block), F32),
            pltpu.VMEM((devices, 1, 128), jnp.int32),
            pltpu.SMEM((devices, 1, 128), jnp.int32),
            pltpu.SemaphoreType.DMA((2,)),
            pltpu.SemaphoreType.DMA((2,)),
            pltpu.SemaphoreType.DMA((2,)),
            pltpu.SemaphoreType.DMA((5,)),
        ],
        out_shape=[
            jax.ShapeDtypeStruct((devices, rows, block), F32),
            jax.ShapeDtypeStruct((1, pairs.shape[1]), jnp.int32),
            jax.ShapeDtypeStruct((depth + PAIR, pairs.shape[1]), jnp.int32),
            jax.ShapeDtypeStruct((devices, 1, 128), jnp.int32),
        ],
        name="fetch",
        compiler_params=pltpu.CompilerParams(collective_id=0, has_side_effects=True),
    )(splats, fetch, pairs, order)


def thirds(x):
    one = rounded(x)
    two = rounded(x - one)
    return [one, two, x - one - two]


def return_kernel(
    sizes, cap, blocks, grad_ref, asked_ref, order_ref, total_hbm,
    total_ref, returned, asked, mix, sems, local_sems, store_sem,
):
    me, devices, other = whereabouts(sizes)
    barrier = greet(devices, other)
    rows = grad_ref.shape[1]
    used = 9 * cap
    spot = pl.ds(pl.multiple_of(me * rows, 8), rows)
    loads = [
        pltpu.make_async_copy(source, target, local_sems.at[n])
        for n, (source, target) in enumerate(
            ((grad_ref.at[me], returned.at[spot]), (asked_ref, asked), (order_ref, mix))
        )
    ]
    for load in loads:
        load.start()
    for load in loads:
        load.wait()
    lane = lax.broadcasted_iota(jnp.int32, (devices, blocks), 1)
    owners = []
    for i in range(cap):
        column = jnp.broadcast_to(asked[:, 0, i : i + 1], (devices, blocks))
        owners += [(column == lane).astype(F32)] * 3
    owners = jnp.concatenate(owners, axis=0).astype(BF16)
    order = mix[...].astype(BF16)
    pl.semaphore_wait(barrier, devices - 1)
    part = pl.ds(0, used)
    land = pl.ds(pl.multiple_of(me * rows, 8), used)

    def serve(n):
        o, where = other(n)
        post(grad_ref.at[o, part], returned.at[land], sems, where).start()

    each(1, devices, serve)
    rest = pl.ds(0, devices - 1)
    bulk = returned.at[pl.ds(0, (devices - 1) * used)]
    post(bulk, bulk, sems, other(1)[1]).wait_recv()
    for r in range(9):
        terms = []
        for i in range(cap):
            at = 8 * i + r if r < 8 else 8 * cap + i
            terms += thirds(returned[pl.ds(at, devices, stride=rows), :])
        summed = lax.dot_general(
            owners,
            jnp.concatenate(terms, axis=0).astype(BF16),
            (((0,), (0,)), ((), ())),
            preferred_element_type=F32,
        )
        mixed = lax.dot_general(
            jnp.concatenate(thirds(summed), axis=0).astype(BF16),
            order,
            (((1,), (1,)), ((), ())),
            preferred_element_type=F32,
        )
        total_ref[r] = mixed[0:blocks] + mixed[blocks : 2 * blocks] + mixed[2 * blocks :]
        if r % 3 == 2:
            span = pl.ds(r - 2, 3)
            pltpu.make_async_copy(total_ref.at[span], total_hbm.at[span], store_sem).start()
    sent = grad_ref.at[rest, part]
    post(sent, sent, sems, other(1)[1]).wait_send()
    pltpu.make_async_copy(total_ref, total_hbm, store_sem).wait()


def return_grads(grads, asked, cap, blocks, sizes):
    devices, rows, block = grads.shape
    order = jnp.asarray(lane_order(block))
    return pl.pallas_call(
        functools.partial(return_kernel, sizes, cap, blocks),
        in_specs=[pl.BlockSpec(memory_space=pl.ANY)] * 3,
        out_specs=pl.BlockSpec(memory_space=pl.ANY),
        scratch_shapes=[
            pltpu.VMEM((9, blocks, block), F32),
            pltpu.VMEM((devices * rows, block), F32),
            pltpu.VMEM(asked.shape, jnp.int32),
            pltpu.VMEM(order.shape, F32),
            pltpu.SemaphoreType.DMA((2,)),
            pltpu.SemaphoreType.DMA((3,)),
            pltpu.SemaphoreType.DMA,
        ],
        out_shape=jax.ShapeDtypeStruct((9, blocks, block), F32),
        name="give_back",
        compiler_params=pltpu.CompilerParams(collective_id=1, has_side_effects=True),
    )(grads, asked, order)


def outline(width, height, x, y, z, first, second, angle):
    inverse_one = jnp.exp(-2.0 * first)
    inverse_two = jnp.exp(-2.0 * second)
    cosine = jnp.cos(angle)
    sine = jnp.sin(angle)
    return (
        width * x / z + 0.5 * width,
        width * y / z + 0.5 * height,
        cosine * cosine * inverse_one + sine * sine * inverse_two,
        cosine * sine * (inverse_one - inverse_two),
        sine * sine * inverse_one + cosine * cosine * inverse_two,
    )


def directions(x, y, z):
    length = jnp.sqrt(x * x + y * y + z * z)
    return tuple(harmonic_terms(x / length, y / length, z / length))


def adam_kernel(
    width, height, total_hbm, splats_ref, one_ref, two_ref, grad_ref, step_ref,
    total_ref, raw, one, two, grad, step, load_sems, store_sems,
):
    count = raw.shape[0]
    cuts = [0, 7] + [7 + 16 * h for h in range(1, 4)]
    spans = [pl.ds(lo, hi - lo) for lo, hi in zip(cuts, cuts[1:])]
    load = pltpu.make_async_copy(splats_ref, raw, load_sems.at[0])
    load.start()
    sums = pltpu.make_async_copy(total_hbm, total_ref, load_sems.at[9])
    sums.start()
    loads = []
    for n, span in enumerate(spans[1:] + spans[:1]):
        pair = [
            pltpu.make_async_copy(one_ref.at[span], one.at[span], load_sems.at[1 + 2 * n]),
            pltpu.make_async_copy(two_ref.at[span], two.at[span], load_sems.at[2 + 2 * n]),
        ]
        for copy in pair:
            copy.start()
        loads.append(pair)
    load.wait()
    place = (raw[0], raw[1], raw[2])
    terms, turn = jax.vjp(directions, *place)
    sums.wait()
    slants = [jnp.zeros_like(place[0]) for _ in terms]
    stores = []

    def finish(n, span, lo, hi):
        for copy in loads[n]:
            copy.wait()
        for r in range(lo, hi):
            change = grad[r]
            first = 0.9 * one[r] + 0.1 * change
            second = 0.999 * two[r] + 0.001 * change * change
            step[r] = first / (second * lax.rsqrt(second) + 1e-08)
        for m, (source, target) in enumerate(((grad, grad_ref), (step, step_ref))):
            copy = pltpu.make_async_copy(
                source.at[span], target.at[span], store_sems.at[2 * n + m]
            )
            copy.start()
            stores.append(copy)

    for h in range(3):
        hue = total_ref[6 + h]
        for k in range(16):
            r = 7 + 16 * h + k
            grad[r] = hue * terms[k]
            slants[k] = slants[k] + hue * raw[r]
        finish(h, spans[1 + h], cuts[1 + h], cuts[2 + h])
    _, pull = jax.vjp(
        functools.partial(outline, width, height), *place, raw[3], raw[4], raw[5]
    )
    flat = pull(tuple(total_ref[j] for j in range(5)))
    tilt = turn(tuple(slants))
    for j in range(3):
        grad[j] = flat[j] + tilt[j]
    for j in range(3, 6):
        grad[j] = flat[j]
    grad[6] = total_ref[5] / (1.0 + jnp.exp(raw[6]))
    finish(3, spans[0], 0, 7)
    for copy in stores:
        copy.wait()


def adam(total, splats, moment_one, moment_two, width, height):
    anywhere = pl.BlockSpec(memory_space=pl.ANY)
    like = jax.ShapeDtypeStruct(splats.shape, F32)
    return pl.pallas_call(
        functools.partial(adam_kernel, width, height),
        in_specs=[anywhere] * 4,
        out_specs=[anywhere, anywhere],
        scratch_shapes=[pltpu.VMEM(total.shape, F32)]
        + [pltpu.VMEM(splats.shape, F32)] * 5
        + [pltpu.SemaphoreType.DMA((10,)), pltpu.SemaphoreType.DMA((8,))],
        out_shape=[like, like],
        name="adam",
    )(total, splats, moment_one, moment_two)


def local(splats, moment_one, moment_two, target, tile_place, pairs, fetch):
    sizes = (lax.axis_size("gx"), lax.axis_size("gy"))
    devices = sizes[0] * sizes[1]
    tiles_here = target.shape[0]
    cap = fetch.shape[2]
    width = 16.0 * TX
    height = 16.0 * (tiles_here * devices // TX)

    rows_first = jnp.transpose(splats, (1, 0, 2))
    asks = jnp.transpose(fetch[0])
    arrived, rows, lists, asked = fetch_blocks(
        rows_first, asks, jnp.transpose(pairs), sizes, width, height
    )
    image, grads = blend(
        arrived, cap, jnp.transpose(target, (1, 0, 2)), tile_place, lists, rows
    )
    total = return_grads(grads, asked, cap, splats.shape[0], sizes)
    splat_grad, adam_step = adam(
        total,
        rows_first,
        jnp.transpose(moment_one, (1, 0, 2)),
        jnp.transpose(moment_two, (1, 0, 2)),
        width,
        height,
    )
    back = lambda x: jnp.transpose(x, (1, 0, 2))
    return (back(image), back(splat_grad), back(adam_step))


def solution(mesh):
    both = ("gx", "gy")
    return jax.shard_map(
        local,
        mesh=mesh,
        in_specs=(
            P(both, None, None),
            P(both, None, None),
            P(both, None, None),
            P(both, None, None),
            P(both),
            P(both, None),
            P(both, None, None),
        ),
        out_specs=(P(both, None, None), P(both, None, None), P(both, None, None)),
        check_vma=False,
    )
```

```python
import functools

import jax
import jax.numpy as jnp
import numpy as np
from jax import lax
from jax.experimental import pallas as pl
from jax.experimental.pallas import tpu as pltpu
from jax.sharding import PartitionSpec as P

TX = 16
SIDE = 16
PIXELS = SIDE * SIDE
LOG2E = 1.4426950408889634
DEAD = -1.0e4
GROUP = 2
PAIR = 4
F32 = jnp.float32
BF16 = jnp.bfloat16


HARMONIC_ZERO = 0.28209479177387814
HARMONIC_ONE = 0.4886025119029199
HARMONIC_TWO = (
    1.0925484305920792,
    -1.0925484305920792,
    0.31539156525252005,
    -1.0925484305920792,
    0.5462742152960396,
)
HARMONIC_THREE = (
    -0.5900435899266435,
    2.890611442640554,
    -0.4570457994644658,
    0.3731763325901154,
    -0.4570457994644658,
    1.445305721320277,
    -0.5900435899266435,
)


def harmonic_terms(east, north, ahead):
    east_east = east * east
    north_north = north * north
    ahead_ahead = ahead * ahead
    return [
        jnp.full_like(east, HARMONIC_ZERO),
        -HARMONIC_ONE * north,
        HARMONIC_ONE * ahead,
        -HARMONIC_ONE * east,
        HARMONIC_TWO[0] * east * north,
        HARMONIC_TWO[1] * north * ahead,
        HARMONIC_TWO[2] * (2.0 * ahead_ahead - east_east - north_north),
        HARMONIC_TWO[3] * east * ahead,
        HARMONIC_TWO[4] * (east_east - north_north),
        HARMONIC_THREE[0] * north * (3.0 * east_east - north_north),
        HARMONIC_THREE[1] * east * north * ahead,
        HARMONIC_THREE[2] * north * (4.0 * ahead_ahead - east_east - north_north),
        HARMONIC_THREE[3] * ahead * (2.0 * ahead_ahead - 3.0 * east_east - 3.0 * north_north),
        HARMONIC_THREE[4] * east * (4.0 * ahead_ahead - east_east - north_north),
        HARMONIC_THREE[5] * ahead * (east_east - north_north),
        HARMONIC_THREE[6] * east * (east_east - 3.0 * north_north),
    ]


def pixel_basis():
    j = np.arange(PIXELS)
    x = j % SIDE + 0.5 - SIDE / 2
    y = j // SIDE + 0.5 - SIDE / 2
    rows = np.stack([x * x, x * y, y * y, x, y, np.ones_like(x), 0 * x, 0 * x])
    return np.concatenate([rows, rows, rows, 0 * rows]).astype(np.float32)


def lane_order(block):
    row = np.arange(block)
    splat = (row % 8) * (block // 8) + row // 8
    return (np.arange(block)[:, None] == splat[None, :]).astype(np.float32)


def rounded(x):
    return x.astype(BF16).astype(F32)


def shifted(x, shift):
    return pltpu.roll(x, shift % 8, 0)


def blend_kernel(
    cap, pairs_ref, place_ref, order_ref, basis_ref, arrived_ref, target_ref, image_hbm, grad_hbm,
    image_ref, grad_ref, sems, screen, owed, hue_sum, hue_back, resid, parts, moments, *banks,
):
    tiles = target_ref.shape[1]
    depth = pairs_ref.shape[0] - PAIR
    slots = cap * arrived_ref.shape[0]
    block = arrived_ref.shape[2]
    chunks = block // 8
    lanes = range(GROUP)
    spots = [(t, e) for e in range(PAIR) for t in lanes]
    many = GROUP * PAIR
    keeps, weights, halves, ends, alphas, slopes, steps = (
        [banks[many * i + PAIR * t : many * i + PAIR * t + PAIR] for t in lanes] for i in range(7)
    )
    sub = lax.broadcasted_iota(jnp.int32, (8, PIXELS), 0)
    devices = arrived_ref.shape[0]
    cuts = 4 if devices % 4 == 0 else 1
    share = devices // cuts
    spans = [pl.ds(share * c, share) for c in range(cuts)]

    resid[...] = jnp.zeros_like(resid)
    parts[...] = jnp.zeros_like(parts)

    def prepare(o, _):
        for i in range(cap):
            s = cap * o + i
            owed[s] = jnp.zeros((16, block), F32)
            last = arrived_ref[o, 8 * cap + i : 8 * cap + i + 1]
            screen[s, 0:8] = arrived_ref[o, 8 * i : 8 * i + 8]
            screen[s, 8:9] = last
            hue = jnp.concatenate(
                [arrived_ref[o, 8 * i + 6 : 8 * i + 8], last, jnp.zeros((5, block), F32)], axis=0
            )
            hue1 = rounded(hue)
            hue2 = hue - hue1
            zero = jnp.zeros_like(hue)
            hue_sum[s] = jnp.concatenate(
                [
                    jnp.concatenate([hue1, hue1], axis=1),
                    jnp.concatenate([hue2, zero], axis=1),
                ],
                axis=0,
            ).astype(BF16)
            hue_back[s] = jnp.concatenate([hue1, hue2, hue1, zero], axis=0).astype(BF16)
        return 0

    for c in range(cuts):
        lax.fori_loop(share * c, share * (c + 1), prepare, 0)
    owed[slots] = jnp.zeros((16, block), F32)
    screen[slots] = jnp.zeros((16, block), F32)
    screen[slots, 5:6] = jnp.full((1, block), DEAD, F32)
    hue_sum[slots] = jnp.zeros((16, 2 * block), BF16)
    hue_back[slots] = jnp.zeros((32, block), BF16)

    basis = basis_ref[...].astype(BF16)
    monomials = basis_ref[0:8].astype(BF16)
    zero_row = jnp.zeros((8, PIXELS), F32)

    def group(step, _):
        row = [order_ref[0, step * GROUP + t] for t in lanes]
        deepest = jnp.int32(0)
        for k in range(depth):
            deepest = deepest + (pairs_ref[k, row[0]] >= 0).astype(jnp.int32)
        turns = lax.div(deepest + (PAIR - 1), PAIR)
        centre = []
        for t in lanes:
            tile = place_ref[row[t]]
            cx = (lax.rem(tile, TX) * SIDE + SIDE // 2).astype(F32)
            cy = (lax.div(tile, TX) * SIDE + SIDE // 2).astype(F32)
            centre.append((cx, cy))

        def place(t, k):
            slot = pairs_ref[k, row[t]]
            return jnp.where(slot >= 0, slot, slots)

        def shape_up(j):
            for t, e in spots:
                cx, cy = centre[t]
                s = place(t, PAIR * j + e)
                u = screen[s, 0:1] - cx
                v = screen[s, 1:2] - cy
                a, b, c = screen[s, 2:3], screen[s, 3:4], screen[s, 4:5]
                opac = jnp.maximum(screen[s, 5:6], DEAD)
                lin_x = a * u + b * v
                lin_y = b * u + c * v
                const = opac - 0.5 * (lin_x * u + lin_y * v)
                for r, value in enumerate((-0.5 * a, -b, -0.5 * c, lin_x, lin_y, const)):
                    parts[e, t, r : r + 1] = LOG2E * value

        shape_up(0)

        def power_of(t, e):
            c = parts[e, t]
            c1 = rounded(c)
            c2 = rounded(c - c1)
            c3 = c - c1 - c2
            left = jnp.concatenate([c1, c2, c3, jnp.zeros_like(c)], axis=0).astype(BF16)
            return lax.dot_general(
                left, basis, (((0,), (0,)), ((), ())), preferred_element_type=F32
            )

        def draw(t, j, e, power):
            alpha = jnp.exp2(power)
            alphas[t][e][0] = alpha
            keep = 1.0 - alpha
            keeps[t][e][j] = keep
            kept = keep[0:8]
            for i in range(1, chunks):
                kept = kept * keep[8 * i : 8 * i + 8]
            return kept

        def scan_of(t, j, e, kept, trans):
            scan = jnp.where(sub == 0, trans, shifted(kept, 1))
            for d in (1, 2, 4):
                scan = scan * jnp.where(sub < d, 1.0, shifted(scan, d))
            end = scan * kept
            ends[t][e][j] = end
            return scan, jnp.broadcast_to(end[7:8], (8, PIXELS))

        def spread(t, j, e, here):
            for i in range(0, chunks, 2):
                lo, mid, hi = 8 * i, 8 * i + 8, 8 * i + 16
                one = alphas[t][e][0, lo:mid] * here
                here = here * keeps[t][e][j, lo:mid]
                two = alphas[t][e][0, mid:hi] * here
                here = here * keeps[t][e][j, mid:hi]
                pair = jnp.concatenate([one, two], axis=0)
                weights[t][e][j, lo:hi] = pair
                high = pair.astype(BF16)
                halves[t][e][j, lo:hi] = high
                halves[t][e][j, block + lo : block + hi] = (pair - high.astype(F32)).astype(BF16)

        def summed(t, j, e):
            return jnp.dot(
                hue_sum[place(t, PAIR * j + e)], halves[t][e][j], preferred_element_type=F32
            )

        def forward(j, carry):
            trans = [carry[2 * t] for t in lanes]
            totals = [carry[2 * t + 1] for t in lanes]
            powers = [[power_of(t, e) for t in lanes] for e in range(PAIR)]
            kepts = [draw(t, j, 0, powers[0][t]) for t in lanes]
            for e in range(PAIR):
                heres = []
                for t in lanes:
                    here, trans[t] = scan_of(t, j, e, kepts[t], trans[t])
                    heres.append(here)
                for t in lanes:
                    spread(t, j, e, heres[t])
                    if e + 1 < PAIR:
                        kepts[t] = draw(t, j, e + 1, powers[e + 1][t])
                totals = [totals[t] + summed(t, j, e) for t in lanes]
            shape_up(j + 1)
            return tuple(x for t in lanes for x in (trans[t], totals[t]))

        start = (jnp.ones((8, PIXELS), F32), jnp.zeros((16, PIXELS), F32)) * GROUP
        done = lax.fori_loop(0, turns, forward, start)

        pulls = []
        for t in lanes:
            total = done[2 * t + 1]
            image = (total[0:8] + total[8:16])[0:3]
            for h in range(3):
                image_ref[h, pl.ds(row[t], 1)] = image[h : h + 1]
                resid[t, h : h + 1] = (image[h : h + 1] - target_ref[h, pl.ds(row[t], 1)]) * (
                    2.0 / 512.0
                )
            g = resid[t]
            g1 = rounded(g)
            g2 = g - g1
            pulls.append(
                (
                    jnp.concatenate([g1, g1, g2, zero_row], axis=0).astype(BF16),
                    jnp.concatenate([g1, g2], axis=0).astype(BF16),
                )
            )

        def lean(t, j, e):
            slopes[t][e][0] = lax.dot_general(
                hue_back[place(t, PAIR * j + e)],
                pulls[t][0],
                (((0,), (0,)), ((), ())),
                preferred_element_type=F32,
            )

        def behind_of(t, j, e, behind):
            run = weights[t][e][j, 0:8] * slopes[t][e][0, 0:8]
            for i in range(1, chunks):
                lo, hi = 8 * i, 8 * i + 8
                run = run + weights[t][e][j, lo:hi] * slopes[t][e][0, lo:hi]
            scan = jnp.where(sub == 7, behind, shifted(run, -1))
            for d in (1, 2, 4):
                scan = scan + jnp.where(sub < 8 - d, shifted(scan, -d), 0.0)
            return (
                scan / jnp.maximum(ends[t][e][j], 1e-37),
                jnp.broadcast_to((run + scan)[0:1], (8, PIXELS)),
            )

        def step_of(t, j, e, here):
            for i in range(chunks - 2, -1, -2):
                lo, mid, hi = 8 * i, 8 * i + 8, 8 * i + 16
                ahead = slopes[t][e][0, mid:hi]
                gap = ahead - here
                two = weights[t][e][j, mid:hi] * gap
                here = ahead - keeps[t][e][j, mid:hi] * gap
                ahead = slopes[t][e][0, lo:mid]
                gap = ahead - here
                one = weights[t][e][j, lo:mid] * gap
                here = ahead - keeps[t][e][j, lo:mid] * gap
                pair = jnp.concatenate([one, two], axis=0)
                high = pair.astype(BF16)
                steps[t][e][0, lo:hi] = high
                steps[t][e][0, block + lo : block + hi] = (pair - high.astype(F32)).astype(BF16)

        def settle(j):
            for t, e in spots:
                cx, cy = centre[t]
                s = place(t, PAIR * j + e)
                u = screen[s, 0:1] - cx
                v = screen[s, 1:2] - cy
                a, b, c = screen[s, 2:3], screen[s, 3:4], screen[s, 4:5]
                mxx, mxy, myy, mx, my, m = (moments[e, t, r : r + 1] for r in range(6))
                off_x = mx - u * m
                off_y = my - v * m
                changes = (
                    a * off_x + b * off_y,
                    b * off_x + c * off_y,
                    -0.5 * (mxx - u * (mx + off_x)),
                    -(mxy - u * my - v * off_x),
                    -0.5 * (myy - v * (my + off_y)),
                    m,
                    moments[e, t, 8:9],
                    moments[e, t, 9:10],
                    moments[e, t, 10:11],
                )
                for r, change in enumerate(changes):
                    owed[s, r : r + 1] = owed[s, r : r + 1] + change

        def backward(index, carry):
            j = turns - 1 - index
            behind = list(carry)
            settle(j + 1)
            places = []
            for e in reversed(range(PAIR)):
                for t in lanes:
                    lean(t, j, e)
            for e in reversed(range(PAIR)):
                for t in lanes:
                    hues = lax.dot_general(
                        pulls[t][1], halves[t][e][j], (((1,), (1,)), ((), ())),
                        preferred_element_type=F32,
                    )
                    places.append(
                        (t, e, 8, hues[0:8, 0:block] + hues[0:8, block:] + hues[8:16, 0:block])
                    )
                heres = []
                for t in lanes:
                    here, behind[t] = behind_of(t, j, e, behind[t])
                    heres.append(here)
                for t in lanes:
                    step_of(t, j, e, heres[t])
                for t in lanes:
                    sums = lax.dot_general(
                        monomials, steps[t][e][0], (((1,), (1,)), ((), ())), preferred_element_type=F32
                    )
                    places.append((t, e, 0, sums[:, 0:block] + sums[:, block:]))
            for t, e, at, value in places:
                moments[e, t, at : at + 8] = value
            return tuple(behind)

        lax.fori_loop(0, turns, backward, (jnp.zeros((8, PIXELS), F32),) * GROUP)

        settle(0)
        return 0

    lax.fori_loop(0, tiles // GROUP, group, 0)

    def pack(o):
        for i in range(cap):
            grad_ref[o, 8 * i : 8 * i + 8] = owed[cap * o + i, 0:8]
            grad_ref[o, 8 * cap + i : 8 * cap + i + 1] = owed[cap * o + i, 8:9]

    stores = [pltpu.make_async_copy(image_ref, image_hbm, sems.at[cuts])]
    stores[0].start()
    for c, span in enumerate(spans):
        each(share * c, share * (c + 1), pack)
        stores.append(pltpu.make_async_copy(grad_ref.at[span], grad_hbm.at[span], sems.at[c]))
        stores[-1].start()
    for store in stores:
        store.wait()


def blend(arrived, cap, target, tile_place, pairs, order):
    channels, tiles, pixels = target.shape
    devices, rows, block = arrived.shape
    slots = devices * cap
    turns = pairs.shape[0] // PAIR
    many = GROUP * PAIR
    basis = jnp.asarray(pixel_basis())
    smem = pl.BlockSpec(memory_space=pltpu.SMEM)
    anywhere = pl.BlockSpec(memory_space=pl.ANY)
    vmem = pl.BlockSpec(memory_space=pltpu.VMEM)
    return pl.pallas_call(
        functools.partial(blend_kernel, cap),
        in_specs=[smem, smem, smem, vmem, vmem, vmem],
        out_specs=[anywhere, anywhere],
        scratch_shapes=[
            pltpu.VMEM(target.shape, F32),
            pltpu.VMEM(arrived.shape, F32),
            pltpu.SemaphoreType.DMA((5,)),
            pltpu.VMEM((slots + 1, 16, block), F32),
            pltpu.VMEM((slots + 1, 16, block), F32),
            pltpu.VMEM((slots + 1, 16, 2 * block), BF16),
            pltpu.VMEM((slots + 1, 32, block), BF16),
            pltpu.VMEM((GROUP, 8, pixels), F32),
            pltpu.VMEM((PAIR, GROUP, 8, block), F32),
            pltpu.VMEM((PAIR, GROUP, 16, block), F32),
        ]
        + [pltpu.VMEM((turns, block, pixels), F32)] * many
        + [pltpu.VMEM((turns, block, pixels), F32)] * many
        + [pltpu.VMEM((turns, 2 * block, pixels), BF16)] * many
        + [pltpu.VMEM((turns, 8, pixels), F32)] * many
        + [pltpu.VMEM((2, block, pixels), F32)] * many
        + [pltpu.VMEM((2, block, pixels), F32)] * many
        + [pltpu.VMEM((2, 2 * block, pixels), BF16)] * many,
        out_shape=[
            jax.ShapeDtypeStruct(target.shape, F32),
            jax.ShapeDtypeStruct((devices, rows, block), F32),
        ],
        name="blend",
        compiler_params=pltpu.CompilerParams(),
    )(pairs, tile_place, order, basis, arrived, target)


def whereabouts(sizes):
    nx, ny = sizes
    me = lax.axis_index("gx") * ny + lax.axis_index("gy")

    def other(n):
        o = lax.rem(me + n, nx * ny)
        return o, (lax.div(o, ny), lax.rem(o, ny))

    return me, nx * ny, other


def each(start, stop, body, width=4):
    whole = (stop - start) // width

    def some(c, _):
        for w in range(width):
            body(start + width * c + w)
        return 0

    lax.fori_loop(0, whole, some, 0)
    for n in range(start + width * whole, stop):
        body(n)


def greet(devices, other):
    barrier = pltpu.get_barrier_semaphore()

    def call(n):
        pl.semaphore_signal(
            barrier, inc=1, device_id=other(n)[1], device_id_type=pl.DeviceIdType.MESH
        )

    each(1, devices, call)
    return barrier


def post(source, target, sems, where):
    return pltpu.make_async_remote_copy(
        src_ref=source,
        dst_ref=target,
        send_sem=sems.at[0],
        recv_sem=sems.at[1],
        device_id=where,
        device_id_type=pl.DeviceIdType.MESH,
    )


def order_rows(pairs, order_ref):
    depth, tiles = pairs.shape
    live = jnp.sum((pairs >= 0).astype(F32), axis=0, keepdims=True)
    across = lax.broadcasted_iota(jnp.int32, (tiles, tiles), 1).astype(F32)
    down = lax.broadcasted_iota(jnp.int32, (tiles, tiles), 0).astype(F32)
    theirs = jnp.broadcast_to(live, (tiles, tiles))
    mine = jnp.sum(jnp.where(across == down, theirs, 0.0), axis=1, keepdims=True)
    before = (theirs > mine) | ((theirs == mine) & (across < down))
    rank = jnp.sum(before.astype(F32), axis=1, keepdims=True)
    order = jnp.sum(jnp.where(rank == across, down, 0.0), axis=0, keepdims=True)
    order_ref[...] = order.astype(jnp.int32)


def fetch_kernel(
    sizes, width, height, splats_ref, fetch_ref, pairs_ref, order_ref,
    arrived_ref, rows_hbm, lists_hbm, asked_hbm,
    rows_ref, lists_ref, raw, wants, lists, mix, own, send, ask, heard,
    hear_sems, sems, local_sems,
):
    me, devices, other = whereabouts(sizes)
    cap = fetch_ref.shape[0]
    _, blocks, block = raw.shape
    used = 9 * cap
    barrier = greet(devices, other)
    loads = [
        pltpu.make_async_copy(source, target, local_sems.at[n])
        for n, (source, target) in enumerate(
            ((fetch_ref, wants), (pairs_ref, lists), (splats_ref, raw), (order_ref, mix))
        )
    ]
    for load in loads:
        load.start()

    loads[0].wait()
    table = jnp.concatenate([wants[...], jnp.zeros((8 - cap, devices), jnp.int32)], axis=0)
    if devices % 128:
        table = jnp.concatenate(
            [table, jnp.zeros((8, 128 - devices % 128), jnp.int32)], axis=1
        )
    table = jnp.transpose(table.astype(F32))[0:devices]
    ask[...] = jnp.zeros_like(ask)
    ask[:, :, 0:8] = table.astype(jnp.int32).reshape(devices, 1, 8)

    pl.semaphore_wait(barrier, devices - 1)

    def inquire(n):
        o, where = other(n)
        post(ask.at[o], heard.at[me], hear_sems, where).start()

    each(1, devices, inquire)
    keep = pltpu.make_async_copy(ask.at[me], heard.at[me], local_sems.at[0])
    keep.start()
    keep.wait()
    rest = pl.ds(0, devices - 1)
    loads[1].wait()
    order_rows(lists[...], rows_ref)
    depth = lists.shape[0]
    lists_ref[...] = jnp.full(lists_ref.shape, -1, jnp.int32)
    lists_ref[0:depth] = lists[...]
    stores = [
        pltpu.make_async_copy(rows_ref, rows_hbm, local_sems.at[0]),
        pltpu.make_async_copy(lists_ref, lists_hbm, local_sems.at[1]),
        pltpu.make_async_copy(heard, asked_hbm, local_sems.at[4]),
    ]
    loads[2].wait()
    loads[3].wait()
    place_x, place_y, place_z = raw[0], raw[1], raw[2]
    inverse_one = jnp.exp(-2.0 * raw[3])
    inverse_two = jnp.exp(-2.0 * raw[4])
    cosine = jnp.cos(raw[5])
    sine = jnp.sin(raw[5])
    length = jnp.sqrt(place_x * place_x + place_y * place_y + place_z * place_z)
    terms = harmonic_terms(place_x / length, place_y / length, place_z / length)
    lines = [
        width * place_x / place_z + 0.5 * width,
        width * place_y / place_z + 0.5 * height,
        cosine * cosine * inverse_one + sine * sine * inverse_two,
        cosine * sine * (inverse_one - inverse_two),
        sine * sine * inverse_one + cosine * cosine * inverse_two,
        jnp.minimum(raw[6], 0.0) - jnp.log1p(jnp.exp(-jnp.abs(raw[6]))),
    ]
    for h in range(3):
        color = jnp.full((blocks, block), 0.5, F32)
        for k in range(16):
            color = color + raw[7 + 16 * h + k] * terms[k]
        lines.append(color)
    order = mix[...].astype(BF16)
    for j, line in enumerate(lines):
        one = rounded(line)
        two = rounded(line - one)
        three = line - one - two
        stack = jnp.concatenate([one, two, three], axis=0).astype(BF16)
        mixed = jnp.dot(stack, order, preferred_element_type=F32)
        mixed = mixed[0:blocks] + mixed[blocks : 2 * blocks] + mixed[2 * blocks :]
        own[:, j, :] = mixed

    both = post(ask.at[rest], heard.at[rest], hear_sems, other(1)[1])
    both.wait_recv()
    for store in stores:
        store.start()

    def pick(o):
        for i in range(cap):
            b = jnp.clip(heard[o, 0, i], 0, blocks - 1)
            send[o, 8 * i : 8 * i + 8] = own[b, 0:8]
            send[o, 8 * cap + i : 8 * cap + i + 1] = own[b, 8:9]

    part = pl.ds(0, used)

    def serve(n):
        o, where = other(n)
        post(send.at[o, part], arrived_ref.at[me, part], sems, where).start()

    lag = 4
    width = 4
    turns = (devices - 1 - lag) // width
    for n in range(1, 1 + lag):
        pick(other(n)[0])

    def run(c, _):
        for w in range(width):
            pick(other(1 + lag + width * c + w)[0])
        for w in range(width):
            serve(1 + width * c + w)
        return 0

    lax.fori_loop(0, turns, run, 0)
    for n in range(1 + lag + width * turns, devices):
        pick(other(n)[0])
    pick(me)
    for n in range(1 + width * turns, devices):
        serve(n)
    keep = pltpu.make_async_copy(send.at[me], arrived_ref.at[me], local_sems.at[3])
    keep.start()
    both.wait_send()
    whole = post(send.at[rest, part], arrived_ref.at[rest, part], sems, other(1)[1])
    whole.wait_recv()
    whole.wait_send()
    keep.wait()
    for store in stores:
        store.wait()


def fetch_blocks(splats, fetch, pairs, sizes, width, height):
    _, blocks, block = splats.shape
    cap, devices = fetch.shape
    rows = 8 * pl.cdiv(9 * cap, 8)
    order = jnp.asarray(lane_order(block))
    depth = PAIR * pl.cdiv(pairs.shape[0], PAIR)
    anywhere = pl.BlockSpec(memory_space=pl.ANY)
    return pl.pallas_call(
        functools.partial(fetch_kernel, sizes, width, height),
        in_specs=[anywhere] * 4,
        out_specs=[anywhere] * 4,
        scratch_shapes=[
            pltpu.VMEM((1, pairs.shape[1]), jnp.int32),
            pltpu.VMEM((depth + PAIR, pairs.shape[1]), jnp.int32),
            pltpu.VMEM(splats.shape, F32),
            pltpu.VMEM(fetch.shape, jnp.int32),
            pltpu.VMEM(pairs.shape, jnp.int32),
            pltpu.VMEM(order.shape, F32),
            pltpu.VMEM((blocks, 16, block), F32),
            pltpu.VMEM((devices, rows, block), F32),
            pltpu.VMEM((devices, 1, 128), jnp.int32),
            pltpu.SMEM((devices, 1, 128), jnp.int32),
            pltpu.SemaphoreType.DMA((2,)),
            pltpu.SemaphoreType.DMA((2,)),
            pltpu.SemaphoreType.DMA((5,)),
        ],
        out_shape=[
            jax.ShapeDtypeStruct((devices, rows, block), F32),
            jax.ShapeDtypeStruct((1, pairs.shape[1]), jnp.int32),
            jax.ShapeDtypeStruct((depth + PAIR, pairs.shape[1]), jnp.int32),
            jax.ShapeDtypeStruct((devices, 1, 128), jnp.int32),
        ],
        name="fetch",
        compiler_params=pltpu.CompilerParams(collective_id=0, has_side_effects=True),
    )(splats, fetch, pairs, order)


def thirds(x):
    one = rounded(x)
    two = rounded(x - one)
    return [one, two, x - one - two]


def return_kernel(
    sizes, cap, blocks, grad_ref, asked_ref, order_ref, total_hbm,
    total_ref, returned, asked, mix, sems, local_sems, store_sem,
):
    me, devices, other = whereabouts(sizes)
    barrier = greet(devices, other)
    rows = grad_ref.shape[1]
    used = 9 * cap
    spot = pl.ds(pl.multiple_of(me * rows, 8), rows)
    loads = [
        pltpu.make_async_copy(source, target, local_sems.at[n])
        for n, (source, target) in enumerate(
            ((grad_ref.at[me], returned.at[spot]), (asked_ref, asked), (order_ref, mix))
        )
    ]
    for load in loads:
        load.start()
    for load in loads:
        load.wait()
    lane = lax.broadcasted_iota(jnp.int32, (devices, blocks), 1)
    owners = []
    for i in range(cap):
        column = jnp.broadcast_to(asked[:, 0, i : i + 1], (devices, blocks))
        owners += [(column == lane).astype(F32)] * 3
    owners = jnp.concatenate(owners, axis=0).astype(BF16)
    order = mix[...].astype(BF16)
    pl.semaphore_wait(barrier, devices - 1)
    part = pl.ds(0, used)
    land = pl.ds(pl.multiple_of(me * rows, 8), used)

    def serve(n):
        o, where = other(n)
        post(grad_ref.at[o, part], returned.at[land], sems, where).start()

    each(1, devices, serve)
    rest = pl.ds(0, devices - 1)
    bulk = returned.at[pl.ds(0, (devices - 1) * used)]
    post(bulk, bulk, sems, other(1)[1]).wait_recv()
    for r in range(9):
        terms = []
        for i in range(cap):
            at = 8 * i + r if r < 8 else 8 * cap + i
            terms += thirds(returned[pl.ds(at, devices, stride=rows), :])
        summed = lax.dot_general(
            owners,
            jnp.concatenate(terms, axis=0).astype(BF16),
            (((0,), (0,)), ((), ())),
            preferred_element_type=F32,
        )
        mixed = lax.dot_general(
            jnp.concatenate(thirds(summed), axis=0).astype(BF16),
            order,
            (((1,), (1,)), ((), ())),
            preferred_element_type=F32,
        )
        total_ref[r] = mixed[0:blocks] + mixed[blocks : 2 * blocks] + mixed[2 * blocks :]
        if r % 3 == 2:
            span = pl.ds(r - 2, 3)
            pltpu.make_async_copy(total_ref.at[span], total_hbm.at[span], store_sem).start()
    sent = grad_ref.at[rest, part]
    post(sent, sent, sems, other(1)[1]).wait_send()
    pltpu.make_async_copy(total_ref, total_hbm, store_sem).wait()


def return_grads(grads, asked, cap, blocks, sizes):
    devices, rows, block = grads.shape
    order = jnp.asarray(lane_order(block))
    return pl.pallas_call(
        functools.partial(return_kernel, sizes, cap, blocks),
        in_specs=[pl.BlockSpec(memory_space=pl.ANY)] * 3,
        out_specs=pl.BlockSpec(memory_space=pl.ANY),
        scratch_shapes=[
            pltpu.VMEM((9, blocks, block), F32),
            pltpu.VMEM((devices * rows, block), F32),
            pltpu.VMEM(asked.shape, jnp.int32),
            pltpu.VMEM(order.shape, F32),
            pltpu.SemaphoreType.DMA((2,)),
            pltpu.SemaphoreType.DMA((3,)),
            pltpu.SemaphoreType.DMA,
        ],
        out_shape=jax.ShapeDtypeStruct((9, blocks, block), F32),
        name="give_back",
        compiler_params=pltpu.CompilerParams(collective_id=1, has_side_effects=True),
    )(grads, asked, order)


def outline(width, height, x, y, z, first, second, angle):
    inverse_one = jnp.exp(-2.0 * first)
    inverse_two = jnp.exp(-2.0 * second)
    cosine = jnp.cos(angle)
    sine = jnp.sin(angle)
    return (
        width * x / z + 0.5 * width,
        width * y / z + 0.5 * height,
        cosine * cosine * inverse_one + sine * sine * inverse_two,
        cosine * sine * (inverse_one - inverse_two),
        sine * sine * inverse_one + cosine * cosine * inverse_two,
    )


def directions(x, y, z):
    length = jnp.sqrt(x * x + y * y + z * z)
    return tuple(harmonic_terms(x / length, y / length, z / length))


def adam_kernel(
    width, height, total_hbm, splats_ref, one_ref, two_ref, grad_ref, step_ref,
    total_ref, raw, one, two, grad, step, load_sems, store_sems,
):
    count = raw.shape[0]
    cuts = [0, 7] + [7 + 16 * h for h in range(1, 4)]
    spans = [pl.ds(lo, hi - lo) for lo, hi in zip(cuts, cuts[1:])]
    load = pltpu.make_async_copy(splats_ref, raw, load_sems.at[0])
    load.start()
    sums = pltpu.make_async_copy(total_hbm, total_ref, load_sems.at[9])
    sums.start()
    loads = []
    for n, span in enumerate(spans[1:] + spans[:1]):
        pair = [
            pltpu.make_async_copy(one_ref.at[span], one.at[span], load_sems.at[1 + 2 * n]),
            pltpu.make_async_copy(two_ref.at[span], two.at[span], load_sems.at[2 + 2 * n]),
        ]
        for copy in pair:
            copy.start()
        loads.append(pair)
    load.wait()
    place = (raw[0], raw[1], raw[2])
    terms, turn = jax.vjp(directions, *place)
    sums.wait()
    slants = [jnp.zeros_like(place[0]) for _ in terms]
    stores = []

    def finish(n, span, lo, hi):
        for copy in loads[n]:
            copy.wait()
        for r in range(lo, hi):
            change = grad[r]
            first = 0.9 * one[r] + 0.1 * change
            second = 0.999 * two[r] + 0.001 * change * change
            step[r] = first / (second * lax.rsqrt(second) + 1e-08)
        for m, (source, target) in enumerate(((grad, grad_ref), (step, step_ref))):
            copy = pltpu.make_async_copy(
                source.at[span], target.at[span], store_sems.at[2 * n + m]
            )
            copy.start()
            stores.append(copy)

    for h in range(3):
        hue = total_ref[6 + h]
        for k in range(16):
            r = 7 + 16 * h + k
            grad[r] = hue * terms[k]
            slants[k] = slants[k] + hue * raw[r]
        finish(h, spans[1 + h], cuts[1 + h], cuts[2 + h])
    _, pull = jax.vjp(
        functools.partial(outline, width, height), *place, raw[3], raw[4], raw[5]
    )
    flat = pull(tuple(total_ref[j] for j in range(5)))
    tilt = turn(tuple(slants))
    for j in range(3):
        grad[j] = flat[j] + tilt[j]
    for j in range(3, 6):
        grad[j] = flat[j]
    grad[6] = total_ref[5] / (1.0 + jnp.exp(raw[6]))
    finish(3, spans[0], 0, 7)
    for copy in stores:
        copy.wait()


def adam(total, splats, moment_one, moment_two, width, height):
    anywhere = pl.BlockSpec(memory_space=pl.ANY)
    like = jax.ShapeDtypeStruct(splats.shape, F32)
    return pl.pallas_call(
        functools.partial(adam_kernel, width, height),
        in_specs=[anywhere] * 4,
        out_specs=[anywhere, anywhere],
        scratch_shapes=[pltpu.VMEM(total.shape, F32)]
        + [pltpu.VMEM(splats.shape, F32)] * 5
        + [pltpu.SemaphoreType.DMA((10,)), pltpu.SemaphoreType.DMA((8,))],
        out_shape=[like, like],
        name="adam",
    )(total, splats, moment_one, moment_two)


def local(splats, moment_one, moment_two, target, tile_place, pairs, fetch):
    sizes = (lax.axis_size("gx"), lax.axis_size("gy"))
    devices = sizes[0] * sizes[1]
    tiles_here = target.shape[0]
    cap = fetch.shape[2]
    width = 16.0 * TX
    height = 16.0 * (tiles_here * devices // TX)

    rows_first = jnp.transpose(splats, (1, 0, 2))
    asks = jnp.transpose(fetch[0])
    arrived, rows, lists, asked = fetch_blocks(
        rows_first, asks, jnp.transpose(pairs), sizes, width, height
    )
    image, grads = blend(
        arrived, cap, jnp.transpose(target, (1, 0, 2)), tile_place, lists, rows
    )
    total = return_grads(grads, asked, cap, splats.shape[0], sizes)
    splat_grad, adam_step = adam(
        total,
        rows_first,
        jnp.transpose(moment_one, (1, 0, 2)),
        jnp.transpose(moment_two, (1, 0, 2)),
        width,
        height,
    )
    back = lambda x: jnp.transpose(x, (1, 0, 2))
    return (back(image), back(splat_grad), back(adam_step))


def solution(mesh):
    both = ("gx", "gy")
    return jax.shard_map(
        local,
        mesh=mesh,
        in_specs=(
            P(both, None, None),
            P(both, None, None),
            P(both, None, None),
            P(both, None, None),
            P(both),
            P(both, None),
            P(both, None, None),
        ),
        out_specs=(P(both, None, None), P(both, None, None), P(both, None, None)),
        check_vma=False,
    )
```

```python
import functools

import jax
import jax.numpy as jnp
import numpy as np
from jax import lax
from jax.experimental import pallas as pl
from jax.experimental.pallas import tpu as pltpu
from jax.sharding import PartitionSpec as P

TX = 16
SIDE = 16
PIXELS = SIDE * SIDE
LOG2E = 1.4426950408889634
DEAD = -1.0e4
GROUP = 2
PAIR = 4
F32 = jnp.float32
BF16 = jnp.bfloat16


HARMONIC_ZERO = 0.28209479177387814
HARMONIC_ONE = 0.4886025119029199
HARMONIC_TWO = (
    1.0925484305920792,
    -1.0925484305920792,
    0.31539156525252005,
    -1.0925484305920792,
    0.5462742152960396,
)
HARMONIC_THREE = (
    -0.5900435899266435,
    2.890611442640554,
    -0.4570457994644658,
    0.3731763325901154,
    -0.4570457994644658,
    1.445305721320277,
    -0.5900435899266435,
)


def harmonic_terms(east, north, ahead):
    east_east = east * east
    north_north = north * north
    ahead_ahead = ahead * ahead
    return [
        jnp.full_like(east, HARMONIC_ZERO),
        -HARMONIC_ONE * north,
        HARMONIC_ONE * ahead,
        -HARMONIC_ONE * east,
        HARMONIC_TWO[0] * east * north,
        HARMONIC_TWO[1] * north * ahead,
        HARMONIC_TWO[2] * (2.0 * ahead_ahead - east_east - north_north),
        HARMONIC_TWO[3] * east * ahead,
        HARMONIC_TWO[4] * (east_east - north_north),
        HARMONIC_THREE[0] * north * (3.0 * east_east - north_north),
        HARMONIC_THREE[1] * east * north * ahead,
        HARMONIC_THREE[2] * north * (4.0 * ahead_ahead - east_east - north_north),
        HARMONIC_THREE[3] * ahead * (2.0 * ahead_ahead - 3.0 * east_east - 3.0 * north_north),
        HARMONIC_THREE[4] * east * (4.0 * ahead_ahead - east_east - north_north),
        HARMONIC_THREE[5] * ahead * (east_east - north_north),
        HARMONIC_THREE[6] * east * (east_east - 3.0 * north_north),
    ]


def pixel_basis():
    j = np.arange(PIXELS)
    x = j % SIDE + 0.5 - SIDE / 2
    y = j // SIDE + 0.5 - SIDE / 2
    rows = np.stack([x * x, x * y, y * y, x, y, np.ones_like(x), 0 * x, 0 * x])
    return np.concatenate([rows, rows, rows, 0 * rows]).astype(np.float32)


def lane_order(block):
    row = np.arange(block)
    splat = (row % 8) * (block // 8) + row // 8
    return (np.arange(block)[:, None] == splat[None, :]).astype(np.float32)


def rounded(x):
    return x.astype(BF16).astype(F32)


def shifted(x, shift):
    return pltpu.roll(x, shift % 8, 0)


def blend_kernel(
    cap, pairs_ref, place_ref, order_ref, basis_ref, arrived_ref, target_ref, image_hbm, grad_hbm,
    image_ref, grad_ref, sems, screen, owed, hue_sum, hue_back, resid, parts, moments, *banks,
):
    tiles = target_ref.shape[1]
    depth = pairs_ref.shape[0] - PAIR
    slots = cap * arrived_ref.shape[0]
    block = arrived_ref.shape[2]
    chunks = block // 8
    lanes = range(GROUP)
    spots = [(t, e) for e in range(PAIR) for t in lanes]
    many = GROUP * PAIR
    keeps, weights, halves, ends, alphas, slopes, steps = (
        [banks[many * i + PAIR * t : many * i + PAIR * t + PAIR] for t in lanes] for i in range(7)
    )
    sub = lax.broadcasted_iota(jnp.int32, (8, PIXELS), 0)
    devices = arrived_ref.shape[0]
    cuts = 4 if devices % 4 == 0 else 1
    share = devices // cuts
    spans = [pl.ds(share * c, share) for c in range(cuts)]

    resid[...] = jnp.zeros_like(resid)
    parts[...] = jnp.zeros_like(parts)

    def prepare(o):
        for i in range(cap):
            s = cap * o + i
            owed[s] = jnp.zeros((16, block), F32)
            last = arrived_ref[o, 8 * cap + i : 8 * cap + i + 1]
            screen[s, 0:8] = arrived_ref[o, 8 * i : 8 * i + 8]
            screen[s, 8:9] = last
            hue = jnp.concatenate(
                [arrived_ref[o, 8 * i + 6 : 8 * i + 8], last, jnp.zeros((5, block), F32)], axis=0
            )
            hue1 = rounded(hue)
            hue2 = hue - hue1
            zero = jnp.zeros_like(hue)
            hue_sum[s] = jnp.concatenate(
                [
                    jnp.concatenate([hue1, hue1], axis=1),
                    jnp.concatenate([hue2, zero], axis=1),
                ],
                axis=0,
            ).astype(BF16)
            hue_back[s] = jnp.concatenate([hue1, hue2, hue1, zero], axis=0).astype(BF16)

    for c in range(cuts):
        each(share * c, share * (c + 1), prepare, 4)
    owed[slots] = jnp.zeros((16, block), F32)
    screen[slots] = jnp.zeros((16, block), F32)
    screen[slots, 5:6] = jnp.full((1, block), DEAD, F32)
    hue_sum[slots] = jnp.zeros((16, 2 * block), BF16)
    hue_back[slots] = jnp.zeros((32, block), BF16)

    basis = basis_ref[...].astype(BF16)
    monomials = basis_ref[0:8].astype(BF16)
    zero_row = jnp.zeros((8, PIXELS), F32)

    def group(step, _):
        row = [order_ref[0, step * GROUP + t] for t in lanes]
        deepest = jnp.int32(0)
        for k in range(depth):
            deepest = deepest + (pairs_ref[k, row[0]] >= 0).astype(jnp.int32)
        turns = lax.div(deepest + (PAIR - 1), PAIR)
        centre = []
        for t in lanes:
            tile = place_ref[row[t]]
            cx = (lax.rem(tile, TX) * SIDE + SIDE // 2).astype(F32)
            cy = (lax.div(tile, TX) * SIDE + SIDE // 2).astype(F32)
            centre.append((cx, cy))

        def place(t, k):
            slot = pairs_ref[k, row[t]]
            return jnp.where(slot >= 0, slot, slots)

        def shape_up(j):
            for t, e in spots:
                cx, cy = centre[t]
                s = place(t, PAIR * j + e)
                u = screen[s, 0:1] - cx
                v = screen[s, 1:2] - cy
                a, b, c = screen[s, 2:3], screen[s, 3:4], screen[s, 4:5]
                opac = jnp.maximum(screen[s, 5:6], DEAD)
                lin_x = a * u + b * v
                lin_y = b * u + c * v
                const = opac - 0.5 * (lin_x * u + lin_y * v)
                for r, value in enumerate((-0.5 * a, -b, -0.5 * c, lin_x, lin_y, const)):
                    parts[e, t, r : r + 1] = LOG2E * value

        shape_up(0)

        def power_of(t, e):
            c = parts[e, t]
            c1 = rounded(c)
            c2 = rounded(c - c1)
            c3 = c - c1 - c2
            left = jnp.concatenate([c1, c2, c3, jnp.zeros_like(c)], axis=0).astype(BF16)
            return lax.dot_general(
                left, basis, (((0,), (0,)), ((), ())), preferred_element_type=F32
            )

        def draw(t, j, e, power):
            alpha = jnp.exp2(power)
            alphas[t][e][0] = alpha
            keep = 1.0 - alpha
            keeps[t][e][j] = keep
            kept = keep[0:8]
            for i in range(1, chunks):
                kept = kept * keep[8 * i : 8 * i + 8]
            return kept

        def scan_of(t, j, e, kept, trans):
            scan = jnp.where(sub == 0, trans, shifted(kept, 1))
            for d in (1, 2, 4):
                scan = scan * jnp.where(sub < d, 1.0, shifted(scan, d))
            end = scan * kept
            ends[t][e][j] = end
            return scan, jnp.broadcast_to(end[7:8], (8, PIXELS))

        def spread(t, j, e, here):
            for i in range(0, chunks, 2):
                lo, mid, hi = 8 * i, 8 * i + 8, 8 * i + 16
                one = alphas[t][e][0, lo:mid] * here
                here = here * keeps[t][e][j, lo:mid]
                two = alphas[t][e][0, mid:hi] * here
                here = here * keeps[t][e][j, mid:hi]
                pair = jnp.concatenate([one, two], axis=0)
                weights[t][e][j, lo:hi] = pair
                high = pair.astype(BF16)
                halves[t][e][j, lo:hi] = high
                halves[t][e][j, block + lo : block + hi] = (pair - high.astype(F32)).astype(BF16)

        def summed(t, j, e):
            return jnp.dot(
                hue_sum[place(t, PAIR * j + e)], halves[t][e][j], preferred_element_type=F32
            )

        def forward(j, carry):
            trans = [carry[2 * t] for t in lanes]
            totals = [carry[2 * t + 1] for t in lanes]
            powers = [[power_of(t, e) for t in lanes] for e in range(PAIR)]
            kepts = [draw(t, j, 0, powers[0][t]) for t in lanes]
            for e in range(PAIR):
                heres = []
                for t in lanes:
                    here, trans[t] = scan_of(t, j, e, kepts[t], trans[t])
                    heres.append(here)
                for t in lanes:
                    spread(t, j, e, heres[t])
                    if e + 1 < PAIR:
                        kepts[t] = draw(t, j, e + 1, powers[e + 1][t])
                totals = [totals[t] + summed(t, j, e) for t in lanes]
            shape_up(j + 1)
            return tuple(x for t in lanes for x in (trans[t], totals[t]))

        start = (jnp.ones((8, PIXELS), F32), jnp.zeros((16, PIXELS), F32)) * GROUP
        done = lax.fori_loop(0, turns, forward, start)

        pulls = []
        for t in lanes:
            total = done[2 * t + 1]
            image = (total[0:8] + total[8:16])[0:3]
            for h in range(3):
                image_ref[h, pl.ds(row[t], 1)] = image[h : h + 1]
                resid[t, h : h + 1] = (image[h : h + 1] - target_ref[h, pl.ds(row[t], 1)]) * (
                    2.0 / 512.0
                )
            g = resid[t]
            g1 = rounded(g)
            g2 = g - g1
            pulls.append(
                (
                    jnp.concatenate([g1, g1, g2, zero_row], axis=0).astype(BF16),
                    jnp.concatenate([g1, g2], axis=0).astype(BF16),
                )
            )

        def lean(t, j, e):
            slopes[t][e][0] = lax.dot_general(
                hue_back[place(t, PAIR * j + e)],
                pulls[t][0],
                (((0,), (0,)), ((), ())),
                preferred_element_type=F32,
            )

        def behind_of(t, j, e, behind):
            run = weights[t][e][j, 0:8] * slopes[t][e][0, 0:8]
            for i in range(1, chunks):
                lo, hi = 8 * i, 8 * i + 8
                run = run + weights[t][e][j, lo:hi] * slopes[t][e][0, lo:hi]
            scan = jnp.where(sub == 7, behind, shifted(run, -1))
            for d in (1, 2, 4):
                scan = scan + jnp.where(sub < 8 - d, shifted(scan, -d), 0.0)
            return (
                scan / jnp.maximum(ends[t][e][j], 1e-37),
                jnp.broadcast_to((run + scan)[0:1], (8, PIXELS)),
            )

        def step_of(t, j, e, here):
            for i in range(chunks - 2, -1, -2):
                lo, mid, hi = 8 * i, 8 * i + 8, 8 * i + 16
                ahead = slopes[t][e][0, mid:hi]
                gap = ahead - here
                two = weights[t][e][j, mid:hi] * gap
                here = ahead - keeps[t][e][j, mid:hi] * gap
                ahead = slopes[t][e][0, lo:mid]
                gap = ahead - here
                one = weights[t][e][j, lo:mid] * gap
                here = ahead - keeps[t][e][j, lo:mid] * gap
                pair = jnp.concatenate([one, two], axis=0)
                high = pair.astype(BF16)
                steps[t][e][0, lo:hi] = high
                steps[t][e][0, block + lo : block + hi] = (pair - high.astype(F32)).astype(BF16)

        def settle(j):
            for t, e in spots:
                cx, cy = centre[t]
                s = place(t, PAIR * j + e)
                u = screen[s, 0:1] - cx
                v = screen[s, 1:2] - cy
                a, b, c = screen[s, 2:3], screen[s, 3:4], screen[s, 4:5]
                mxx, mxy, myy, mx, my, m = (moments[e, t, r : r + 1] for r in range(6))
                off_x = mx - u * m
                off_y = my - v * m
                changes = (
                    a * off_x + b * off_y,
                    b * off_x + c * off_y,
                    -0.5 * (mxx - u * (mx + off_x)),
                    -(mxy - u * my - v * off_x),
                    -0.5 * (myy - v * (my + off_y)),
                    m,
                    moments[e, t, 8:9],
                    moments[e, t, 9:10],
                    moments[e, t, 10:11],
                )
                for r, change in enumerate(changes):
                    owed[s, r : r + 1] = owed[s, r : r + 1] + change

        def backward(index, carry):
            j = turns - 1 - index
            behind = list(carry)
            settle(j + 1)
            places = []
            for e in reversed(range(PAIR)):
                for t in lanes:
                    lean(t, j, e)
            for e in reversed(range(PAIR)):
                for t in lanes:
                    hues = lax.dot_general(
                        pulls[t][1], halves[t][e][j], (((1,), (1,)), ((), ())),
                        preferred_element_type=F32,
                    )
                    places.append(
                        (t, e, 8, hues[0:8, 0:block] + hues[0:8, block:] + hues[8:16, 0:block])
                    )
                heres = []
                for t in lanes:
                    here, behind[t] = behind_of(t, j, e, behind[t])
                    heres.append(here)
                for t in lanes:
                    step_of(t, j, e, heres[t])
                for t in lanes:
                    sums = lax.dot_general(
                        monomials, steps[t][e][0], (((1,), (1,)), ((), ())), preferred_element_type=F32
                    )
                    places.append((t, e, 0, sums[:, 0:block] + sums[:, block:]))
            for t, e, at, value in places:
                moments[e, t, at : at + 8] = value
            return tuple(behind)

        lax.fori_loop(0, turns, backward, (jnp.zeros((8, PIXELS), F32),) * GROUP)

        settle(0)
        return 0

    lax.fori_loop(0, tiles // GROUP, group, 0)

    def pack(o):
        for i in range(cap):
            grad_ref[o, 8 * i : 8 * i + 8] = owed[cap * o + i, 0:8]
            grad_ref[o, 8 * cap + i : 8 * cap + i + 1] = owed[cap * o + i, 8:9]

    stores = [pltpu.make_async_copy(image_ref, image_hbm, sems.at[cuts])]
    stores[0].start()
    for c, span in enumerate(spans):
        each(share * c, share * (c + 1), pack)
        stores.append(pltpu.make_async_copy(grad_ref.at[span], grad_hbm.at[span], sems.at[c]))
        stores[-1].start()
    for store in stores:
        store.wait()


def blend(arrived, cap, target, tile_place, pairs, order):
    channels, tiles, pixels = target.shape
    devices, rows, block = arrived.shape
    slots = devices * cap
    turns = pairs.shape[0] // PAIR
    many = GROUP * PAIR
    basis = jnp.asarray(pixel_basis())
    smem = pl.BlockSpec(memory_space=pltpu.SMEM)
    anywhere = pl.BlockSpec(memory_space=pl.ANY)
    vmem = pl.BlockSpec(memory_space=pltpu.VMEM)
    return pl.pallas_call(
        functools.partial(blend_kernel, cap),
        in_specs=[smem, smem, smem, vmem, vmem, vmem],
        out_specs=[anywhere, anywhere],
        scratch_shapes=[
            pltpu.VMEM(target.shape, F32),
            pltpu.VMEM(arrived.shape, F32),
            pltpu.SemaphoreType.DMA((5,)),
            pltpu.VMEM((slots + 1, 16, block), F32),
            pltpu.VMEM((slots + 1, 16, block), F32),
            pltpu.VMEM((slots + 1, 16, 2 * block), BF16),
            pltpu.VMEM((slots + 1, 32, block), BF16),
            pltpu.VMEM((GROUP, 8, pixels), F32),
            pltpu.VMEM((PAIR, GROUP, 8, block), F32),
            pltpu.VMEM((PAIR, GROUP, 16, block), F32),
        ]
        + [pltpu.VMEM((turns, block, pixels), F32)] * many
        + [pltpu.VMEM((turns, block, pixels), F32)] * many
        + [pltpu.VMEM((turns, 2 * block, pixels), BF16)] * many
        + [pltpu.VMEM((turns, 8, pixels), F32)] * many
        + [pltpu.VMEM((2, block, pixels), F32)] * many
        + [pltpu.VMEM((2, block, pixels), F32)] * many
        + [pltpu.VMEM((2, 2 * block, pixels), BF16)] * many,
        out_shape=[
            jax.ShapeDtypeStruct(target.shape, F32),
            jax.ShapeDtypeStruct((devices, rows, block), F32),
        ],
        name="blend",
        compiler_params=pltpu.CompilerParams(),
    )(pairs, tile_place, order, basis, arrived, target)


def whereabouts(sizes):
    nx, ny = sizes
    me = lax.axis_index("gx") * ny + lax.axis_index("gy")

    def other(n):
        o = lax.rem(me + n, nx * ny)
        return o, (lax.div(o, ny), lax.rem(o, ny))

    return me, nx * ny, other


def each(start, stop, body, width=8):
    whole = (stop - start) // width

    def some(c, _):
        for w in range(width):
            body(start + width * c + w)
        return 0

    lax.fori_loop(0, whole, some, 0)
    for n in range(start + width * whole, stop):
        body(n)


def greet(devices, other):
    barrier = pltpu.get_barrier_semaphore()

    def call(n):
        pl.semaphore_signal(
            barrier, inc=1, device_id=other(n)[1], device_id_type=pl.DeviceIdType.MESH
        )

    each(1, devices, call)
    return barrier


def post(source, target, sems, where):
    return pltpu.make_async_remote_copy(
        src_ref=source,
        dst_ref=target,
        send_sem=sems.at[0],
        recv_sem=sems.at[1],
        device_id=where,
        device_id_type=pl.DeviceIdType.MESH,
    )


def order_rows(pairs, order_ref):
    depth, tiles = pairs.shape
    live = jnp.sum((pairs >= 0).astype(F32), axis=0, keepdims=True)
    across = lax.broadcasted_iota(jnp.int32, (tiles, tiles), 1).astype(F32)
    down = lax.broadcasted_iota(jnp.int32, (tiles, tiles), 0).astype(F32)
    theirs = jnp.broadcast_to(live, (tiles, tiles))
    mine = jnp.sum(jnp.where(across == down, theirs, 0.0), axis=1, keepdims=True)
    before = (theirs > mine) | ((theirs == mine) & (across < down))
    rank = jnp.sum(before.astype(F32), axis=1, keepdims=True)
    order = jnp.sum(jnp.where(rank == across, down, 0.0), axis=0, keepdims=True)
    order_ref[...] = order.astype(jnp.int32)


def fetch_kernel(
    sizes, width, height, splats_ref, fetch_ref, pairs_ref, order_ref,
    arrived_ref, rows_hbm, lists_hbm, asked_hbm,
    rows_ref, lists_ref, raw, wants, lists, mix, own, send, ask, heard,
    hear_sems, sems, local_sems,
):
    me, devices, other = whereabouts(sizes)
    cap = fetch_ref.shape[0]
    _, blocks, block = raw.shape
    used = 9 * cap
    barrier = greet(devices, other)
    loads = [
        pltpu.make_async_copy(source, target, local_sems.at[n])
        for n, (source, target) in enumerate(
            ((fetch_ref, wants), (pairs_ref, lists), (splats_ref, raw), (order_ref, mix))
        )
    ]
    for load in loads:
        load.start()

    loads[0].wait()
    table = jnp.concatenate([wants[...], jnp.zeros((8 - cap, devices), jnp.int32)], axis=0)
    if devices % 128:
        table = jnp.concatenate(
            [table, jnp.zeros((8, 128 - devices % 128), jnp.int32)], axis=1
        )
    table = jnp.transpose(table.astype(F32))[0:devices]
    ask[...] = jnp.zeros_like(ask)
    ask[:, :, 0:8] = table.astype(jnp.int32).reshape(devices, 1, 8)

    pl.semaphore_wait(barrier, devices - 1)

    def inquire(n):
        o, where = other(n)
        post(ask.at[o], heard.at[me], hear_sems, where).start()

    each(1, devices, inquire)
    keep = pltpu.make_async_copy(ask.at[me], heard.at[me], local_sems.at[0])
    keep.start()
    keep.wait()
    rest = pl.ds(0, devices - 1)
    loads[1].wait()
    order_rows(lists[...], rows_ref)
    depth = lists.shape[0]
    lists_ref[...] = jnp.full(lists_ref.shape, -1, jnp.int32)
    lists_ref[0:depth] = lists[...]
    stores = [
        pltpu.make_async_copy(rows_ref, rows_hbm, local_sems.at[0]),
        pltpu.make_async_copy(lists_ref, lists_hbm, local_sems.at[1]),
        pltpu.make_async_copy(heard, asked_hbm, local_sems.at[4]),
    ]
    loads[2].wait()
    loads[3].wait()
    place_x, place_y, place_z = raw[0], raw[1], raw[2]
    inverse_one = jnp.exp(-2.0 * raw[3])
    inverse_two = jnp.exp(-2.0 * raw[4])
    cosine = jnp.cos(raw[5])
    sine = jnp.sin(raw[5])
    length = jnp.sqrt(place_x * place_x + place_y * place_y + place_z * place_z)
    terms = harmonic_terms(place_x / length, place_y / length, place_z / length)
    lines = [
        width * place_x / place_z + 0.5 * width,
        width * place_y / place_z + 0.5 * height,
        cosine * cosine * inverse_one + sine * sine * inverse_two,
        cosine * sine * (inverse_one - inverse_two),
        sine * sine * inverse_one + cosine * cosine * inverse_two,
        jnp.minimum(raw[6], 0.0) - jnp.log1p(jnp.exp(-jnp.abs(raw[6]))),
    ]
    for h in range(3):
        color = jnp.full((blocks, block), 0.5, F32)
        for k in range(16):
            color = color + raw[7 + 16 * h + k] * terms[k]
        lines.append(color)
    order = mix[...].astype(BF16)
    for j, line in enumerate(lines):
        one = rounded(line)
        two = rounded(line - one)
        three = line - one - two
        stack = jnp.concatenate([one, two, three], axis=0).astype(BF16)
        mixed = jnp.dot(stack, order, preferred_element_type=F32)
        mixed = mixed[0:blocks] + mixed[blocks : 2 * blocks] + mixed[2 * blocks :]
        own[:, j, :] = mixed

    both = post(ask.at[rest], heard.at[rest], hear_sems, other(1)[1])
    both.wait_recv()
    for store in stores:
        store.start()

    def pick(o):
        for i in range(cap):
            b = jnp.clip(heard[o, 0, i], 0, blocks - 1)
            send[o, 8 * i : 8 * i + 8] = own[b, 0:8]
            send[o, 8 * cap + i : 8 * cap + i + 1] = own[b, 8:9]

    part = pl.ds(0, used)

    def serve(n):
        o, where = other(n)
        post(send.at[o, part], arrived_ref.at[me, part], sems, where).start()

    lag = 4
    width = 4
    turns = (devices - 1 - lag) // width
    for n in range(1, 1 + lag):
        pick(other(n)[0])

    def run(c, _):
        for w in range(width):
            pick(other(1 + lag + width * c + w)[0])
        for w in range(width):
            serve(1 + width * c + w)
        return 0

    lax.fori_loop(0, turns, run, 0)
    for n in range(1 + lag + width * turns, devices):
        pick(other(n)[0])
    pick(me)
    for n in range(1 + width * turns, devices):
        serve(n)
    keep = pltpu.make_async_copy(send.at[me], arrived_ref.at[me], local_sems.at[3])
    keep.start()
    both.wait_send()
    whole = post(send.at[rest, part], arrived_ref.at[rest, part], sems, other(1)[1])
    whole.wait_recv()
    whole.wait_send()
    keep.wait()
    for store in stores:
        store.wait()


def fetch_blocks(splats, fetch, pairs, sizes, width, height):
    _, blocks, block = splats.shape
    cap, devices = fetch.shape
    rows = 8 * pl.cdiv(9 * cap, 8)
    order = jnp.asarray(lane_order(block))
    depth = PAIR * pl.cdiv(pairs.shape[0], PAIR)
    anywhere = pl.BlockSpec(memory_space=pl.ANY)
    return pl.pallas_call(
        functools.partial(fetch_kernel, sizes, width, height),
        in_specs=[anywhere] * 4,
        out_specs=[anywhere] * 4,
        scratch_shapes=[
            pltpu.VMEM((1, pairs.shape[1]), jnp.int32),
            pltpu.VMEM((depth + PAIR, pairs.shape[1]), jnp.int32),
            pltpu.VMEM(splats.shape, F32),
            pltpu.VMEM(fetch.shape, jnp.int32),
            pltpu.VMEM(pairs.shape, jnp.int32),
            pltpu.VMEM(order.shape, F32),
            pltpu.VMEM((blocks, 16, block), F32),
            pltpu.VMEM((devices, rows, block), F32),
            pltpu.VMEM((devices, 1, 128), jnp.int32),
            pltpu.SMEM((devices, 1, 128), jnp.int32),
            pltpu.SemaphoreType.DMA((2,)),
            pltpu.SemaphoreType.DMA((2,)),
            pltpu.SemaphoreType.DMA((5,)),
        ],
        out_shape=[
            jax.ShapeDtypeStruct((devices, rows, block), F32),
            jax.ShapeDtypeStruct((1, pairs.shape[1]), jnp.int32),
            jax.ShapeDtypeStruct((depth + PAIR, pairs.shape[1]), jnp.int32),
            jax.ShapeDtypeStruct((devices, 1, 128), jnp.int32),
        ],
        name="fetch",
        compiler_params=pltpu.CompilerParams(collective_id=0, has_side_effects=True),
    )(splats, fetch, pairs, order)


def thirds(x):
    one = rounded(x)
    two = rounded(x - one)
    return [one, two, x - one - two]


def return_kernel(
    sizes, cap, blocks, grad_ref, asked_ref, order_ref, total_hbm,
    total_ref, returned, asked, mix, sems, local_sems, store_sem,
):
    me, devices, other = whereabouts(sizes)
    barrier = greet(devices, other)
    rows = grad_ref.shape[1]
    used = 9 * cap
    spot = pl.ds(pl.multiple_of(me * rows, 8), rows)
    loads = [
        pltpu.make_async_copy(source, target, local_sems.at[n])
        for n, (source, target) in enumerate(
            ((grad_ref.at[me], returned.at[spot]), (asked_ref, asked), (order_ref, mix))
        )
    ]
    for load in loads:
        load.start()
    for load in loads:
        load.wait()
    lane = lax.broadcasted_iota(jnp.int32, (devices, blocks), 1)
    owners = []
    for i in range(cap):
        column = jnp.broadcast_to(asked[:, 0, i : i + 1], (devices, blocks))
        owners += [(column == lane).astype(F32)] * 3
    owners = jnp.concatenate(owners, axis=0).astype(BF16)
    order = mix[...].astype(BF16)
    pl.semaphore_wait(barrier, devices - 1)
    part = pl.ds(0, used)
    land = pl.ds(pl.multiple_of(me * rows, 8), used)

    def serve(n):
        o, where = other(n)
        post(grad_ref.at[o, part], returned.at[land], sems, where).start()

    each(1, devices, serve)
    rest = pl.ds(0, devices - 1)
    bulk = returned.at[pl.ds(0, (devices - 1) * used)]
    post(bulk, bulk, sems, other(1)[1]).wait_recv()
    for r in range(9):
        terms = []
        for i in range(cap):
            at = 8 * i + r if r < 8 else 8 * cap + i
            terms += thirds(returned[pl.ds(at, devices, stride=rows), :])
        summed = lax.dot_general(
            owners,
            jnp.concatenate(terms, axis=0).astype(BF16),
            (((0,), (0,)), ((), ())),
            preferred_element_type=F32,
        )
        mixed = lax.dot_general(
            jnp.concatenate(thirds(summed), axis=0).astype(BF16),
            order,
            (((1,), (1,)), ((), ())),
            preferred_element_type=F32,
        )
        total_ref[r] = mixed[0:blocks] + mixed[blocks : 2 * blocks] + mixed[2 * blocks :]
        if r % 3 == 2:
            span = pl.ds(r - 2, 3)
            pltpu.make_async_copy(total_ref.at[span], total_hbm.at[span], store_sem).start()
    sent = grad_ref.at[rest, part]
    post(sent, sent, sems, other(1)[1]).wait_send()
    pltpu.make_async_copy(total_ref, total_hbm, store_sem).wait()


def return_grads(grads, asked, cap, blocks, sizes):
    devices, rows, block = grads.shape
    order = jnp.asarray(lane_order(block))
    return pl.pallas_call(
        functools.partial(return_kernel, sizes, cap, blocks),
        in_specs=[pl.BlockSpec(memory_space=pl.ANY)] * 3,
        out_specs=pl.BlockSpec(memory_space=pl.ANY),
        scratch_shapes=[
            pltpu.VMEM((9, blocks, block), F32),
            pltpu.VMEM((devices * rows, block), F32),
            pltpu.VMEM(asked.shape, jnp.int32),
            pltpu.VMEM(order.shape, F32),
            pltpu.SemaphoreType.DMA((2,)),
            pltpu.SemaphoreType.DMA((3,)),
            pltpu.SemaphoreType.DMA,
        ],
        out_shape=jax.ShapeDtypeStruct((9, blocks, block), F32),
        name="give_back",
        compiler_params=pltpu.CompilerParams(collective_id=1, has_side_effects=True),
    )(grads, asked, order)


def outline(width, height, x, y, z, first, second, angle):
    inverse_one = jnp.exp(-2.0 * first)
    inverse_two = jnp.exp(-2.0 * second)
    cosine = jnp.cos(angle)
    sine = jnp.sin(angle)
    return (
        width * x / z + 0.5 * width,
        width * y / z + 0.5 * height,
        cosine * cosine * inverse_one + sine * sine * inverse_two,
        cosine * sine * (inverse_one - inverse_two),
        sine * sine * inverse_one + cosine * cosine * inverse_two,
    )


def directions(x, y, z):
    length = jnp.sqrt(x * x + y * y + z * z)
    return tuple(harmonic_terms(x / length, y / length, z / length))


def adam_kernel(
    width, height, total_hbm, splats_ref, one_ref, two_ref, grad_ref, step_ref,
    total_ref, raw, one, two, grad, step, load_sems, store_sems,
):
    count = raw.shape[0]
    cuts = [0, 7] + [7 + 16 * h for h in range(1, 4)]
    spans = [pl.ds(lo, hi - lo) for lo, hi in zip(cuts, cuts[1:])]
    load = pltpu.make_async_copy(splats_ref, raw, load_sems.at[0])
    load.start()
    sums = pltpu.make_async_copy(total_hbm, total_ref, load_sems.at[9])
    sums.start()
    loads = []
    for n, span in enumerate(spans[1:] + spans[:1]):
        pair = [
            pltpu.make_async_copy(one_ref.at[span], one.at[span], load_sems.at[1 + 2 * n]),
            pltpu.make_async_copy(two_ref.at[span], two.at[span], load_sems.at[2 + 2 * n]),
        ]
        for copy in pair:
            copy.start()
        loads.append(pair)
    load.wait()
    place = (raw[0], raw[1], raw[2])
    terms, turn = jax.vjp(directions, *place)
    sums.wait()
    slants = [jnp.zeros_like(place[0]) for _ in terms]
    stores = []

    def finish(n, span, lo, hi):
        for copy in loads[n]:
            copy.wait()
        for r in range(lo, hi):
            change = grad[r]
            first = 0.9 * one[r] + 0.1 * change
            second = 0.999 * two[r] + 0.001 * change * change
            step[r] = first / (second * lax.rsqrt(second) + 1e-08)
        for m, (source, target) in enumerate(((grad, grad_ref), (step, step_ref))):
            copy = pltpu.make_async_copy(
                source.at[span], target.at[span], store_sems.at[2 * n + m]
            )
            copy.start()
            stores.append(copy)

    for h in range(3):
        hue = total_ref[6 + h]
        for k in range(16):
            r = 7 + 16 * h + k
            grad[r] = hue * terms[k]
            slants[k] = slants[k] + hue * raw[r]
        finish(h, spans[1 + h], cuts[1 + h], cuts[2 + h])
    _, pull = jax.vjp(
        functools.partial(outline, width, height), *place, raw[3], raw[4], raw[5]
    )
    flat = pull(tuple(total_ref[j] for j in range(5)))
    tilt = turn(tuple(slants))
    for j in range(3):
        grad[j] = flat[j] + tilt[j]
    for j in range(3, 6):
        grad[j] = flat[j]
    grad[6] = total_ref[5] / (1.0 + jnp.exp(raw[6]))
    finish(3, spans[0], 0, 7)
    for copy in stores:
        copy.wait()


def adam(total, splats, moment_one, moment_two, width, height):
    anywhere = pl.BlockSpec(memory_space=pl.ANY)
    like = jax.ShapeDtypeStruct(splats.shape, F32)
    return pl.pallas_call(
        functools.partial(adam_kernel, width, height),
        in_specs=[anywhere] * 4,
        out_specs=[anywhere, anywhere],
        scratch_shapes=[pltpu.VMEM(total.shape, F32)]
        + [pltpu.VMEM(splats.shape, F32)] * 5
        + [pltpu.SemaphoreType.DMA((10,)), pltpu.SemaphoreType.DMA((8,))],
        out_shape=[like, like],
        name="adam",
    )(total, splats, moment_one, moment_two)


def local(splats, moment_one, moment_two, target, tile_place, pairs, fetch):
    sizes = (lax.axis_size("gx"), lax.axis_size("gy"))
    devices = sizes[0] * sizes[1]
    tiles_here = target.shape[0]
    cap = fetch.shape[2]
    width = 16.0 * TX
    height = 16.0 * (tiles_here * devices // TX)

    rows_first = jnp.transpose(splats, (1, 0, 2))
    asks = jnp.transpose(fetch[0])
    arrived, rows, lists, asked = fetch_blocks(
        rows_first, asks, jnp.transpose(pairs), sizes, width, height
    )
    image, grads = blend(
        arrived, cap, jnp.transpose(target, (1, 0, 2)), tile_place, lists, rows
    )
    total = return_grads(grads, asked, cap, splats.shape[0], sizes)
    splat_grad, adam_step = adam(
        total,
        rows_first,
        jnp.transpose(moment_one, (1, 0, 2)),
        jnp.transpose(moment_two, (1, 0, 2)),
        width,
        height,
    )
    back = lambda x: jnp.transpose(x, (1, 0, 2))
    return (back(image), back(splat_grad), back(adam_step))


def solution(mesh):
    both = ("gx", "gy")
    return jax.shard_map(
        local,
        mesh=mesh,
        in_specs=(
            P(both, None, None),
            P(both, None, None),
            P(both, None, None),
            P(both, None, None),
            P(both),
            P(both, None),
            P(both, None, None),
        ),
        out_specs=(P(both, None, None), P(both, None, None), P(both, None, None)),
        check_vma=False,
    )
```
